64 devices in a mesh: dp: 4 (over x, y), stage: 16 (over z, core).
Axes of the slice: x: 2, y: 2, z: 8, core: 2. Of those that a mesh axis runs over, the one named last changes fastest.
The devices are a block of a 4x4x8 slice.
Arguments:
- tokens: int32 [64, 64], P('dp'), parts along dimension 0
- labels: int32 [64, 64], P('dp'), parts along dimension 0
- emb_table: bfloat16 [30592, 128], replicated
- w_up: bfloat16 [16, 128, 512], P('stage')
- w_down: bfloat16 [16, 512, 128], P('stage')
Outputs:
- output 1: float32 [4], P('dp'), parts along dimension 0
- output 2: float32 [64, 128, 512], P(('dp', 'stage')), parts along dimension 0
- output 3: float32 [64, 512, 128], P(('dp', 'stage')), parts along dimension 0
- output 4: float32 [122368, 128], P('dp'), parts along dimension 0
There are 4 independent parts. The reference program is written for one: setup_inputs(seed, part) draws one part's arguments, and reference() takes and returns one part's arrays. A program takes and returns all parts, laid end to end along the dimension named above; an argument that names none is the same for every part.
All inputs are finite; a program needn't handle non-finite values.
Results may differ from the reference program's by a relative error of at most 0.02.
Values are sent between devices in bfloat16 or wider.
A program may use at most 768 MiB of HBM per device.

```python
import jax
import jax.numpy as jnp
from jax import lax

VOCAB_SIZE = 30592
MODEL_DIM = 128
FFN_DIM = 512
NUM_STAGES = 16
NUM_MICRO = 16
SEQ_TOKENS = 64

LOGIT_SCALE = MODEL_DIM ** -0.5
INV_COUNT = 1.0 / (NUM_MICRO * SEQ_TOKENS)


def setup_inputs(seed: int = 0, part: int = 0) -> dict:
    key_part = jax.random.fold_in(jax.random.key(seed), part)
    key_ids, key_shift = jax.random.split(key_part)
    key_emb, key_up, key_down = jax.random.split(jax.random.key(seed + 1), 3)
    raw_ids = jax.random.randint(key_ids, (NUM_MICRO, SEQ_TOKENS + 1), 0, VOCAB_SIZE)
    shifts = jax.random.randint(key_shift, (NUM_MICRO, SEQ_TOKENS + 1), 0, 9)
    sequence = jnp.right_shift(raw_ids, shifts)
    sequence = sequence.at[0, 0].set(VOCAB_SIZE - 1).at[0, 1].set(0)
    emb_table = jax.random.normal(key_emb, (VOCAB_SIZE, MODEL_DIM), jnp.float32)
    w_up = jax.random.normal(key_up, (NUM_STAGES, MODEL_DIM, FFN_DIM), jnp.float32) * MODEL_DIM ** -0.5
    w_down = jax.random.normal(key_down, (NUM_STAGES, FFN_DIM, MODEL_DIM), jnp.float32) * (2.0 / (FFN_DIM * NUM_STAGES)) ** 0.5
    return {"tokens": sequence[:, :-1], "labels": sequence[:, 1:], "emb_table": emb_table.astype(jnp.bfloat16), "w_up": w_up.astype(jnp.bfloat16), "w_down": w_down.astype(jnp.bfloat16)}


def rms_normalize(x_act):
    x_wide = x_act.astype(jnp.float32)
    inv_rms = lax.rsqrt(jnp.mean(x_wide * x_wide, axis=-1, keepdims=True) + 1e-6)
    return (x_wide * inv_rms).astype(jnp.bfloat16)


def micro_loss(table_f32, up_f32, down_f32, tok_row, lab_row):
    x_act = table_f32[tok_row].astype(jnp.bfloat16)

    def layer_step(x_cur, weights):
        x_wide = x_cur.astype(jnp.float32)
        pre_act = jnp.dot(x_wide, weights[0], preferred_element_type=jnp.float32).astype(jnp.bfloat16)
        hidden = jax.nn.gelu(pre_act.astype(jnp.float32)).astype(jnp.bfloat16)
        branch = jnp.dot(hidden.astype(jnp.float32), weights[1], preferred_element_type=jnp.float32)
        return (x_wide + branch).astype(jnp.bfloat16), None

    x_act, _ = lax.scan(layer_step, x_act, (up_f32, down_f32))
    normed = rms_normalize(x_act)
    logits = (jnp.dot(normed.astype(jnp.float32), table_f32.T, preferred_element_type=jnp.float32) * LOGIT_SCALE).astype(jnp.bfloat16)
    logit_f = logits.astype(jnp.float32)
    log_norm = jax.nn.logsumexp(logit_f, axis=-1)
    picked = jnp.take_along_axis(logit_f, lab_row[:, None], axis=-1)[:, 0]
    return jnp.sum(log_norm - picked) * INV_COUNT


def reference(tokens, labels, emb_table, w_up, w_down):
    table_f32 = emb_table.astype(jnp.float32)
    up_f32 = w_up.astype(jnp.float32)
    down_f32 = w_down.astype(jnp.float32)
    grad_fn = jax.value_and_grad(micro_loss, argnums=(0, 1, 2))

    def micro_step(loop_state, micro_rows):
        loss_sum, grad_emb, grad_up, grad_down = loop_state
        loss_val, grad_all = grad_fn(table_f32, up_f32, down_f32, micro_rows[0], micro_rows[1])
        return (loss_sum + loss_val, grad_emb + grad_all[0], grad_up + grad_all[1], grad_down + grad_all[2]), None

    init_carry = (jnp.zeros((), jnp.float32), jnp.zeros_like(table_f32), jnp.zeros_like(up_f32), jnp.zeros_like(down_f32))
    (loss_sum, grad_emb, grad_up, grad_down), _ = lax.scan(micro_step, init_carry, (tokens, labels))
    return loss_sum.reshape(1), grad_up, grad_down, grad_emb
```

```python
import functools
import math

import jax
import jax.numpy as jnp
from jax import lax
from jax.experimental import pallas as pl
from jax.experimental.pallas import tpu as pltpu
from jax.sharding import PartitionSpec as P

F32 = jnp.float32
BF16 = jnp.bfloat16
MESH = pl.DeviceIdType.MESH
LANES = 128
TILE = 16
HEAD_COLS = 1024
TABLE_ROWS = 512
GELU_C = math.sqrt(2.0 / math.pi)
GELU_K = 0.044715
RMS_EPS = 1e-6


def dot_nn(a, b):
    return lax.dot_general(a, b, (((1,), (0,)), ((), ())), preferred_element_type=F32)


def dot_nt(a, b):
    return lax.dot_general(a, b, (((1,), (1,)), ((), ())), preferred_element_type=F32)


def dot_tn(a, b):
    return lax.dot_general(a, b, (((0,), (0,)), ((), ())), preferred_element_type=F32)


def gelu(a):
    return a * (0.5 * (1.0 + jnp.tanh(GELU_C * (a + GELU_K * (a * a * a)))))


def gelu_grad(a):
    sq = a * a
    t = jnp.tanh(GELU_C * (a + GELU_K * (sq * a)))
    return 0.5 * (1.0 + t) + (0.5 * GELU_C) * a * (1.0 - t * t) * (1.0 + (3.0 * GELU_K) * sq)


def chunks(total, size):
    return size, total // size, total % size


def step_kernel(n_stage, inv_count, tok_ref, lab_ref, table_hbm, w_up_ref, w_down_ref,
                n_out, dx_out, misc_out, gup_out, gdown_out,
                table, up_all, down_all, x_hist, pre_hist, dy_hist, logits,
                n_mine, misc_mine, dx_mine, x_rows, n_all, misc_all, dx_all, x_all, dy_all,
                table_sem, up_recv, down_recv, up_send, down_send,
                x_recv, dy_recv, n_recv, misc_recv, dx_recv,
                x_send, dy_send, n_send, misc_send, dx_send):
    me = lax.axis_index("stage")
    dp = lax.axis_index("dp")
    n_chip = n_stage // 2
    half = n_chip // 2
    chip, core = me // 2, lax.rem(me, 2)
    dim = table.shape[2]
    vocab = table.shape[0] * TILE
    seq = x_hist.shape[1]
    logit_scale = dim ** -0.5

    def slot_at(offset, which):
        return lax.rem(chip + offset + n_chip, n_chip) * 2 + which

    right, left, partner = slot_at(1, core), slot_at(-1, core), chip * 2 + (1 - core)

    table_copy = pltpu.make_async_copy(table_hbm, table, table_sem)
    table_copy.start()

    barrier = pltpu.get_barrier_semaphore()

    def greet(k, carry):
        pl.semaphore_signal(barrier, inc=1, device_id=(dp, lax.rem(me + k, n_stage)), device_id_type=MESH)
        return carry

    lax.fori_loop(1, n_stage, greet, 0)
    pl.semaphore_wait(barrier, n_stage - 1)

    def up_copy(slot, way, target, own=False):
        return pltpu.make_async_remote_copy(
            src_ref=w_up_ref.at[0] if own else up_all.at[slot], dst_ref=up_all.at[slot],
            send_sem=up_send.at[way, slot], recv_sem=up_recv.at[slot],
            device_id=(dp, target), device_id_type=MESH)

    def down_copy(slot, way, target, own=False):
        return pltpu.make_async_remote_copy(
            src_ref=w_down_ref.at[0] if own else down_all.at[slot], dst_ref=down_all.at[slot],
            send_sem=down_send.at[way, slot], recv_sem=down_recv.at[slot],
            device_id=(dp, target), device_id_type=MESH)

    sends = []

    def send(copy):
        copy.start()
        sends.append(copy)

    for way, target in ((0, right), (1, left), (2, partner)):
        send(up_copy(me, way, target, own=True))
        send(down_copy(me, way, target, own=True))
    up_all[me] = w_up_ref[0]
    down_all[me] = w_down_ref[0]

    table_copy.wait()
    row_iota = lax.broadcasted_iota(jnp.int32, (TILE, dim), 0)

    def embed(i, carry):
        tok = tok_ref[me, i]
        tile = table[lax.div(tok, TILE)].astype(F32)
        row = jnp.sum(jnp.where(row_iota == lax.rem(tok, TILE), tile, 0.0), axis=0, keepdims=True)
        x_rows[pl.ds(i, 1), :] = row
        return carry

    lax.fori_loop(0, seq, embed, 0)
    x_now = x_rows[...].astype(BF16)

    for t in range(1, half + 1):
        slot_l, slot_r = slot_at(-t, core), slot_at(t, core)
        up_copy(slot_l, 0, right).wait_recv()
        if t < half:
            send(up_copy(slot_l, 0, right))
        send(up_copy(slot_l, 2, partner))
        down_copy(slot_r, 1, left).wait_recv()
        if t < half:
            send(down_copy(slot_r, 1, left))
        send(down_copy(slot_r, 2, partner))
        if t < half:
            down_copy(slot_l, 0, right).wait_recv()
            if t < half - 1:
                send(down_copy(slot_l, 0, right))
            send(down_copy(slot_l, 2, partner))
            up_copy(slot_r, 1, left).wait_recv()
            if t < half - 1:
                send(up_copy(slot_r, 1, left))
            send(up_copy(slot_r, 2, partner))

    for t in range(n_chip):
        slot = slot_at(t, 1 - core)
        up_copy(slot, 2, partner).wait_recv()
        down_copy(slot, 2, partner).wait_recv()

    def forward(s, x_act):
        x_hist[s] = x_act
        pre = dot_nn(x_act, up_all[s]).astype(BF16)
        pre_hist[s] = pre
        hidden = gelu(pre.astype(F32)).astype(BF16)
        return (x_act.astype(F32) + dot_nn(hidden, down_all[s])).astype(BF16)

    x_last = lax.fori_loop(0, n_stage, forward, x_now)

    def peer_copy(src, dst, send_sem, recv_sem, target):
        return pltpu.make_async_remote_copy(
            src_ref=src, dst_ref=dst.at[me], send_sem=send_sem.at[target], recv_sem=recv_sem.at[me],
            device_id=(dp, target), device_id_type=MESH)

    def x_copy(target):
        return peer_copy(x_hist.at[target], x_all, x_send, x_recv, target)

    def dy_copy(target):
        return peer_copy(dy_hist.at[target], dy_all, dy_send, dy_recv, target)

    def n_copy(target):
        return peer_copy(n_mine, n_all, n_send, n_recv, target)

    def misc_copy(target):
        return peer_copy(misc_mine, misc_all, misc_send, misc_recv, target)

    def dx_copy(target):
        return peer_copy(dx_mine, dx_all, dx_send, dx_recv, target)

    def to_peers(start):
        def one(k, carry):
            start(lax.rem(me + k, n_stage))
            return carry
        lax.fori_loop(1, n_stage, one, 0)

    x_wide = x_last.astype(F32)
    inv_rms = lax.rsqrt(jnp.mean(x_wide * x_wide, axis=-1, keepdims=True) + RMS_EPS)
    normed = (x_wide * inv_rms).astype(BF16)
    n_mine[...] = normed

    cols, n_full, tail = chunks(vocab, HEAD_COLS)

    def table_rows(first, width):
        tile = first // TILE if isinstance(first, int) else lax.div(first, TILE)
        return table[pl.ds(tile, width // TILE)].reshape(width, dim)

    def pass_one(first, width, carry):
        top, total = carry
        z = (dot_nt(normed, table_rows(first, width)) * logit_scale).astype(BF16)
        logits[:, pl.ds(first, width)] = z
        parts = [z[:, j:j + LANES].astype(F32) for j in range(0, width, LANES)]
        new_top = top
        for part in parts:
            new_top = jnp.maximum(new_top, part)
        total = total * jnp.exp(top - new_top)
        for part in parts:
            total = total + jnp.exp(part - new_top)
        return new_top, total

    def head_loop(body, carry):
        carry = lax.fori_loop(0, n_full, lambda i, c: body(pl.multiple_of(i * cols, cols), cols, c), carry)
        if tail:
            carry = body(n_full * cols, tail, carry)
        return carry

    top, total = head_loop(pass_one, (jnp.full((seq, LANES), -1e30, F32), jnp.zeros((seq, LANES), F32)))
    row_top = jnp.max(top, axis=-1, keepdims=True)
    row_sum = jnp.sum(total * jnp.exp(top - row_top), axis=-1, keepdims=True)
    lse = row_top + jnp.log(row_sum)

    to_peers(lambda target: x_copy(target).start())
    x_all[me] = x_hist[me]

    label = lab_ref[...]
    lane_iota = lax.broadcasted_iota(jnp.int32, (seq, LANES), 1)

    def pass_two(first, width, carry):
        picked, grad_n = carry
        base = label - first
        grads = []
        for j in range(0, width, LANES):
            z = logits[:, pl.ds(first + j, LANES)].astype(F32)
            prob = jnp.exp(z - lse)
            hit = lane_iota == base - j
            picked = picked + jnp.where(hit, z, 0.0)
            grads.append((jnp.where(hit, prob - 1.0, prob) * inv_count).astype(BF16))
        grad_z = jnp.concatenate(grads, axis=1)
        return picked, grad_n + dot_nn(grad_z, table_rows(first, width))

    picked, grad_n = head_loop(pass_two, (jnp.zeros((seq, LANES), F32), jnp.zeros((seq, dim), F32)))
    loss = jnp.sum((lse - jnp.sum(picked, axis=-1, keepdims=True)) * inv_count)
    eye = lax.broadcasted_iota(jnp.int32, (seq, LANES), 0) == lane_iota
    lse_row = jnp.sum(jnp.where(eye, lse, 0.0), axis=0, keepdims=True)
    row8 = lax.broadcasted_iota(jnp.int32, (8, LANES), 0)
    misc = jnp.where(row8 == 0, jnp.broadcast_to(lse_row, (8, LANES)), loss)
    misc_mine[...] = misc
    n_all[me] = normed
    misc_all[me] = misc

    grad_n = (grad_n * logit_scale).astype(BF16).astype(F32)
    along = jnp.mean(grad_n * x_wide, axis=-1, keepdims=True)
    grad_x = (inv_rms * grad_n - x_wide * (inv_rms * inv_rms * inv_rms * along)).astype(BF16)

    def backward(k, grad_out):
        s = n_stage - 1 - k
        dy_hist[s] = grad_out
        grad_hidden = dot_nt(grad_out, down_all[s]).astype(BF16).astype(F32)
        grad_pre = (grad_hidden * gelu_grad(pre_hist[s].astype(F32))).astype(BF16)
        result = (grad_out.astype(F32) + dot_nt(grad_pre, up_all[s])).astype(BF16)

        @pl.when(s != me)
        def _():
            dy_copy(s).start()

        return result

    to_peers(lambda target: n_copy(target).start())
    grad_in = lax.fori_loop(0, n_stage, backward, grad_x)
    dx_mine[...] = grad_in
    to_peers(lambda target: misc_copy(target).start())
    dy_all[me] = dy_hist[me]
    dx_all[me] = grad_in

    to_peers(lambda target: x_copy(target).wait_send())

    def wait_from(buf, recv):
        def one(k, carry):
            source = lax.rem(me + k, n_stage)
            pltpu.make_async_remote_copy(
                src_ref=buf.at[source], dst_ref=buf.at[source], send_sem=dx_send.at[source], recv_sem=recv.at[source],
                device_id=(dp, source), device_id_type=MESH).wait_recv()
            return carry
        lax.fori_loop(1, n_stage, one, 0)

    wait_from(x_all, x_recv)
    to_peers(lambda target: dx_copy(target).start())
    wait_from(dy_all, dy_recv)
    up, down = w_up_ref[0], w_down_ref[0]
    gup_out[...] = jnp.zeros_like(gup_out)
    gdown_out[...] = jnp.zeros_like(gdown_out)
    group = max(1, 256 // seq)

    def wgrad(i, carry):
        x_act = x_all[pl.ds(i * group, group)].reshape(group * seq, dim)
        grad_out = dy_all[pl.ds(i * group, group)].reshape(group * seq, dim)
        pre = dot_nn(x_act, up).astype(BF16).astype(F32)
        hidden = gelu(pre).astype(BF16)
        gdown_out[...] += dot_tn(hidden, grad_out)
        grad_hidden = dot_nt(grad_out, down).astype(BF16).astype(F32)
        grad_pre = (grad_hidden * gelu_grad(pre)).astype(BF16)
        gup_out[...] += dot_tn(x_act, grad_pre)
        return carry

    lax.fori_loop(0, n_stage // group, wgrad, 0)

    wait_from(n_all, n_recv)
    wait_from(misc_all, misc_recv)
    wait_from(dx_all, dx_recv)
    n_out[...] = n_all[...]
    misc_out[...] = misc_all[...]
    dx_out[...] = dx_all[...]

    for copy in sends:
        copy.wait_send()
    for make in (dy_copy, n_copy, misc_copy, dx_copy):
        to_peers(lambda target, make=make: make(target).wait_send())


def table_kernel(inv_count, tok_ref, lse_ref, lab_ref, n_ref, dx_ref, table_hbm, out_hbm,
                 table, acc, dx_wide, table_sem, out_sem):
    vocab, dim = table.shape
    count = n_ref.shape[0]
    logit_scale = dim ** -0.5
    table_copy = pltpu.make_async_copy(table_hbm, table, table_sem)
    table_copy.start()
    acc[...] = jnp.zeros_like(acc)
    dx_wide[...] = dx_ref[...].astype(F32)

    def scatter(i, carry):
        tok = tok_ref[0, i]
        acc[pl.ds(tok, 1), :] += dx_wide[pl.ds(i, 1), :]
        return carry

    lax.fori_loop(0, count, scatter, 0, unroll=8)
    table_copy.wait()

    rows, n_full, tail = chunks(vocab, TABLE_ROWS)
    lse = lse_ref[...]
    label = lab_ref[...]

    def out_copy(first, height, index):
        return pltpu.make_async_copy(acc.at[pl.ds(first, height), :], out_hbm.at[pl.ds(first, height), :], out_sem.at[index])

    def part(first, height, index):
        z = (dot_nt(table[pl.ds(first, height), :], n_ref[...]) * logit_scale).astype(BF16).astype(F32)
        prob = jnp.exp(z - lse)
        row_iota = lax.broadcasted_iota(jnp.int32, (height, count), 0)
        hit = row_iota == label - first
        grad_z = (jnp.where(hit, prob - 1.0, prob) * inv_count).astype(BF16)
        acc[pl.ds(first, height), :] += dot_nn(grad_z, n_ref[...]) * logit_scale
        out_copy(first, height, index).start()

    def loop(i, carry):
        part(pl.multiple_of(i * rows, rows), rows, i)
        return carry

    lax.fori_loop(0, n_full, loop, 0)
    if tail:
        part(n_full * rows, tail, n_full)

    def drain(i, carry):
        out_copy(pl.multiple_of(i * rows, rows), rows, i).wait()
        return carry

    lax.fori_loop(0, n_full, drain, 0)
    if tail:
        out_copy(n_full * rows, tail, n_full).wait()


def solution(mesh):
    n_stage = mesh.shape["stage"]

    def device_fn(tokens, labels, emb_table, w_up, w_down):
        n_micro, seq = tokens.shape
        vocab, dim = emb_table.shape
        ffn = w_up.shape[2]
        count = n_micro * seq
        inv_count = 1.0 / count
        stage = lax.axis_index("stage")
        label_col = lax.dynamic_index_in_dim(labels, stage, 0, keepdims=False).reshape(seq, 1)
        vmem = pl.BlockSpec(memory_space=pltpu.VMEM)
        smem = pl.BlockSpec(memory_space=pltpu.SMEM)
        hbm = pl.BlockSpec(memory_space=pl.ANY)
        dma = pltpu.SemaphoreType.DMA

        n_all, dx_all, misc, g_up, g_down = pl.pallas_call(
            functools.partial(step_kernel, n_stage, inv_count),
            name="step",
            out_shape=(
                jax.ShapeDtypeStruct((n_stage, seq, dim), BF16),
                jax.ShapeDtypeStruct((n_stage, seq, dim), BF16),
                jax.ShapeDtypeStruct((n_stage, 8, LANES), F32),
                jax.ShapeDtypeStruct((dim, ffn), F32),
                jax.ShapeDtypeStruct((ffn, dim), F32),
            ),
            in_specs=[smem, vmem, hbm, vmem, vmem],
            out_specs=(vmem,) * 5,
            scratch_shapes=[
                pltpu.VMEM((vocab // TILE, TILE, dim), BF16),
                pltpu.VMEM((n_stage, dim, ffn), BF16),
                pltpu.VMEM((n_stage, ffn, dim), BF16),
                pltpu.VMEM((n_stage, seq, dim), BF16),
                pltpu.VMEM((n_stage, seq, ffn), BF16),
                pltpu.VMEM((n_stage, seq, dim), BF16),
                pltpu.VMEM((seq, vocab), BF16),
                pltpu.VMEM((seq, dim), BF16),
                pltpu.VMEM((8, LANES), F32),
                pltpu.VMEM((seq, dim), BF16),
                pltpu.VMEM((seq, dim), F32),
                pltpu.VMEM((n_stage, seq, dim), BF16),
                pltpu.VMEM((n_stage, 8, LANES), F32),
                pltpu.VMEM((n_stage, seq, dim), BF16),
                pltpu.VMEM((n_stage, seq, dim), BF16),
                pltpu.VMEM((n_stage, seq, dim), BF16),
                dma, dma((n_stage,)), dma((n_stage,)), dma((3, n_stage)), dma((3, n_stage)),
                dma((n_stage,)), dma((n_stage,)), dma((n_stage,)), dma((n_stage,)), dma((n_stage,)),
                dma((n_stage,)), dma((n_stage,)), dma((n_stage,)), dma((n_stage,)), dma((n_stage,)),
            ],
            compiler_params=pltpu.CompilerParams(collective_id=0, has_side_effects=True),
        )(tokens, label_col, emb_table.reshape(vocab // TILE, TILE, dim), w_up, w_down)

        n_parts = -(-vocab // TABLE_ROWS)
        grad_emb = pl.pallas_call(
            functools.partial(table_kernel, inv_count),
            name="table_grad",
            out_shape=jax.ShapeDtypeStruct((vocab, dim), F32),
            in_specs=[smem, vmem, vmem, vmem, vmem, hbm],
            out_specs=hbm,
            scratch_shapes=[
                pltpu.VMEM((vocab, dim), BF16),
                pltpu.VMEM((vocab, dim), F32),
                pltpu.VMEM((count, dim), F32),
                dma, dma((n_parts,)),
            ],
        )(tokens.reshape(1, count), misc[:, 0, :seq].reshape(1, count), labels.reshape(1, count),
          n_all.reshape(count, dim), dx_all.reshape(count, dim), emb_table)
        loss = jnp.sum(misc[:, 1, 0]).reshape(1)
        return loss, g_up[None], g_down[None], grad_emb

    return jax.shard_map(device_fn, mesh=mesh, in_specs=(P("dp", None), P("dp", None), P(None, None), P("stage", None, None), P("stage", None, None)), out_specs=(P("dp"), P(("dp", "stage"), None, None), P(("dp", "stage"), None, None), P("dp", None)), check_vma=False)
```

```python
import functools
import math

import jax
import jax.numpy as jnp
from jax import lax
from jax.experimental import pallas as pl
from jax.experimental.pallas import tpu as pltpu
from jax.sharding import PartitionSpec as P

F32 = jnp.float32
BF16 = jnp.bfloat16
MESH = pl.DeviceIdType.MESH
LANES = 128
TILE = 16
HEAD_COLS = 1024
TABLE_ROWS = 2048
GELU_C = math.sqrt(2.0 / math.pi)
GELU_K = 0.044715
RMS_EPS = 1e-6


def dot_nn(a, b):
    return lax.dot_general(a, b, (((1,), (0,)), ((), ())), preferred_element_type=F32)


def dot_nt(a, b):
    return lax.dot_general(a, b, (((1,), (1,)), ((), ())), preferred_element_type=F32)


def dot_tn(a, b):
    return lax.dot_general(a, b, (((0,), (0,)), ((), ())), preferred_element_type=F32)


def gelu(a):
    return a * (0.5 * (1.0 + jnp.tanh(GELU_C * (a + GELU_K * (a * a * a)))))


def gelu_grad(a):
    sq = a * a
    t = jnp.tanh(GELU_C * (a + GELU_K * (sq * a)))
    return 0.5 * (1.0 + t) + (0.5 * GELU_C) * a * (1.0 - t * t) * (1.0 + (3.0 * GELU_K) * sq)


def chunks(total, size):
    return size, total // size, total % size


def step_kernel(n_stage, inv_count, tok_ref, lab_ref, table_hbm, w_up_ref, w_down_ref,
                n_out, dx_out, x_out, dy_out, misc_out,
                table, up_all, down_all, x_hist, pre_hist, dy_hist, logits,
                n_mine, misc_mine, dx_mine, x_rows, n_all, misc_all, dx_all, x_all, dy_all,
                table_sem, up_recv, down_recv, up_send, down_send,
                x_recv, dy_recv, n_recv, misc_recv, dx_recv,
                x_send, dy_send, n_send, misc_send, dx_send):
    me = lax.axis_index("stage")
    dp = lax.axis_index("dp")
    n_chip = n_stage // 2
    half = n_chip // 2
    chip, core = me // 2, lax.rem(me, 2)
    dim = table.shape[2]
    vocab = table.shape[0] * TILE
    seq = x_hist.shape[1]
    logit_scale = dim ** -0.5

    def slot_at(offset, which):
        return lax.rem(chip + offset + n_chip, n_chip) * 2 + which

    right, left, partner = slot_at(1, core), slot_at(-1, core), chip * 2 + (1 - core)

    table_copy = pltpu.make_async_copy(table_hbm, table, table_sem)
    table_copy.start()

    barrier = pltpu.get_barrier_semaphore()

    def greet(k, carry):
        pl.semaphore_signal(barrier, inc=1, device_id=(dp, lax.rem(me + k, n_stage)), device_id_type=MESH)
        return carry

    lax.fori_loop(1, n_stage, greet, 0)
    pl.semaphore_wait(barrier, n_stage - 1)

    def up_copy(slot, way, target, own=False):
        return pltpu.make_async_remote_copy(
            src_ref=w_up_ref.at[0] if own else up_all.at[slot], dst_ref=up_all.at[slot],
            send_sem=up_send.at[way, slot], recv_sem=up_recv.at[slot],
            device_id=(dp, target), device_id_type=MESH)

    def down_copy(slot, way, target, own=False):
        return pltpu.make_async_remote_copy(
            src_ref=w_down_ref.at[0] if own else down_all.at[slot], dst_ref=down_all.at[slot],
            send_sem=down_send.at[way, slot], recv_sem=down_recv.at[slot],
            device_id=(dp, target), device_id_type=MESH)

    sends = []

    def send(copy):
        copy.start()
        sends.append(copy)

    for way, target in ((0, right), (1, left), (2, partner)):
        send(up_copy(me, way, target, own=True))
        send(down_copy(me, way, target, own=True))
    up_all[me] = w_up_ref[0]
    down_all[me] = w_down_ref[0]

    table_copy.wait()
    row_iota = lax.broadcasted_iota(jnp.int32, (TILE, dim), 0)

    def embed(i, carry):
        tok = tok_ref[me, i]
        tile = table[lax.div(tok, TILE)].astype(F32)
        row = jnp.sum(jnp.where(row_iota == lax.rem(tok, TILE), tile, 0.0), axis=0, keepdims=True)
        x_rows[pl.ds(i, 1), :] = row
        return carry

    lax.fori_loop(0, seq, embed, 0)
    x_now = x_rows[...].astype(BF16)

    for t in range(1, half + 1):
        slot_l, slot_r = slot_at(-t, core), slot_at(t, core)
        up_copy(slot_l, 0, right).wait_recv()
        if t < half:
            send(up_copy(slot_l, 0, right))
        send(up_copy(slot_l, 2, partner))
        down_copy(slot_r, 1, left).wait_recv()
        if t < half:
            send(down_copy(slot_r, 1, left))
        send(down_copy(slot_r, 2, partner))
        if t < half:
            down_copy(slot_l, 0, right).wait_recv()
            if t < half - 1:
                send(down_copy(slot_l, 0, right))
            send(down_copy(slot_l, 2, partner))
            up_copy(slot_r, 1, left).wait_recv()
            if t < half - 1:
                send(up_copy(slot_r, 1, left))
            send(up_copy(slot_r, 2, partner))

    for t in range(n_chip):
        slot = slot_at(t, 1 - core)
        up_copy(slot, 2, partner).wait_recv()
        down_copy(slot, 2, partner).wait_recv()

    def forward(s, x_act):
        x_hist[s] = x_act
        pre = dot_nn(x_act, up_all[s]).astype(BF16)
        pre_hist[s] = pre
        hidden = gelu(pre.astype(F32)).astype(BF16)
        return (x_act.astype(F32) + dot_nn(hidden, down_all[s])).astype(BF16)

    x_last = lax.fori_loop(0, n_stage, forward, x_now)

    def peer_copy(src, dst, send_sem, recv_sem, target):
        return pltpu.make_async_remote_copy(
            src_ref=src, dst_ref=dst.at[me], send_sem=send_sem.at[target], recv_sem=recv_sem.at[me],
            device_id=(dp, target), device_id_type=MESH)

    def x_copy(target):
        return peer_copy(x_hist.at[target], x_all, x_send, x_recv, target)

    def dy_copy(target):
        return peer_copy(dy_hist.at[target], dy_all, dy_send, dy_recv, target)

    def n_copy(target):
        return peer_copy(n_mine, n_all, n_send, n_recv, target)

    def misc_copy(target):
        return peer_copy(misc_mine, misc_all, misc_send, misc_recv, target)

    def dx_copy(target):
        return peer_copy(dx_mine, dx_all, dx_send, dx_recv, target)

    def to_peers(start):
        def one(k, carry):
            start(lax.rem(me + k, n_stage))
            return carry
        lax.fori_loop(1, n_stage, one, 0)

    x_wide = x_last.astype(F32)
    inv_rms = lax.rsqrt(jnp.mean(x_wide * x_wide, axis=-1, keepdims=True) + RMS_EPS)
    normed = (x_wide * inv_rms).astype(BF16)
    n_mine[...] = normed

    cols, n_full, tail = chunks(vocab, HEAD_COLS)

    def table_rows(first, width):
        tile = first // TILE if isinstance(first, int) else lax.div(first, TILE)
        return table[pl.ds(tile, width // TILE)].reshape(width, dim)

    def pass_one(first, width, carry):
        top, total = carry
        z = (dot_nt(normed, table_rows(first, width)) * logit_scale).astype(BF16)
        logits[:, pl.ds(first, width)] = z
        parts = [z[:, j:j + LANES].astype(F32) for j in range(0, width, LANES)]
        new_top = top
        for part in parts:
            new_top = jnp.maximum(new_top, part)
        total = total * jnp.exp(top - new_top)
        for part in parts:
            total = total + jnp.exp(part - new_top)
        return new_top, total

    def head_loop(body, carry):
        carry = lax.fori_loop(0, n_full, lambda i, c: body(pl.multiple_of(i * cols, cols), cols, c), carry)
        if tail:
            carry = body(n_full * cols, tail, carry)
        return carry

    top, total = head_loop(pass_one, (jnp.full((seq, LANES), -1e30, F32), jnp.zeros((seq, LANES), F32)))
    row_top = jnp.max(top, axis=-1, keepdims=True)
    row_sum = jnp.sum(total * jnp.exp(top - row_top), axis=-1, keepdims=True)
    lse = row_top + jnp.log(row_sum)

    to_peers(lambda target: x_copy(target).start())
    x_all[me] = x_hist[me]

    lane_iota = lax.broadcasted_iota(jnp.int32, (seq, LANES), 1)
    lane_wide = lane_iota.astype(F32)
    square = lax.broadcasted_iota(jnp.int32, (seq, seq), 0) == lax.broadcasted_iota(jnp.int32, (seq, seq), 1)
    label = jnp.sum(jnp.where(square, lab_ref[pl.ds(me, 1), :].astype(F32), 0.0), axis=-1, keepdims=True)
    lse_count = lse + math.log(1.0 / inv_count)

    def pass_two(first, width, carry):
        picked, grad_n = carry
        base = label - jnp.asarray(first, jnp.int32).astype(F32)
        grads = []
        for j in range(0, width, LANES):
            z = logits[:, pl.ds(first + j, LANES)].astype(F32)
            prob = jnp.exp(z - lse_count)
            hit = lane_wide == base - float(j)
            picked = picked + jnp.where(hit, z, 0.0)
            grads.append(jnp.where(hit, prob - inv_count, prob).astype(BF16))
        grad_z = jnp.concatenate(grads, axis=1)
        return picked, grad_n + dot_nn(grad_z, table_rows(first, width))

    picked, grad_n = head_loop(pass_two, (jnp.zeros((seq, LANES), F32), jnp.zeros((seq, dim), F32)))
    picked = jnp.sum(picked, axis=-1, keepdims=True)
    loss = jnp.sum((lse - picked) * inv_count)
    label_prob = jnp.exp(picked - lse_count)
    fix = (label_prob - inv_count).astype(BF16).astype(F32) - label_prob.astype(BF16).astype(F32)
    eye = lax.broadcasted_iota(jnp.int32, (seq, LANES), 0) == lane_iota

    def as_row(column):
        return jnp.broadcast_to(jnp.sum(jnp.where(eye, column, 0.0), axis=0, keepdims=True), (8, LANES))

    row8 = lax.broadcasted_iota(jnp.int32, (8, LANES), 0)
    misc = jnp.where(row8 == 0, as_row(lse_count), jnp.where(row8 == 1, as_row(fix), loss))
    misc_mine[...] = misc
    n_all[me] = normed
    misc_all[me] = misc

    grad_n = (grad_n * logit_scale).astype(BF16).astype(F32)
    along = jnp.mean(grad_n * x_wide, axis=-1, keepdims=True)
    grad_x = (inv_rms * grad_n - x_wide * (inv_rms * inv_rms * inv_rms * along)).astype(BF16)

    def backward(k, grad_out):
        s = n_stage - 1 - k
        dy_hist[s] = grad_out
        grad_hidden = dot_nt(grad_out, down_all[s]).astype(BF16).astype(F32)
        grad_pre = (grad_hidden * gelu_grad(pre_hist[s].astype(F32))).astype(BF16)
        result = (grad_out.astype(F32) + dot_nt(grad_pre, up_all[s])).astype(BF16)

        @pl.when(s != me)
        def _():
            dy_copy(s).start()

        return result

    to_peers(lambda target: n_copy(target).start())
    grad_in = lax.fori_loop(0, n_stage, backward, grad_x)
    dx_mine[...] = grad_in
    to_peers(lambda target: misc_copy(target).start())
    dy_all[me] = dy_hist[me]
    dx_all[me] = grad_in

    to_peers(lambda target: x_copy(target).wait_send())

    def wait_from(buf, recv):
        def one(k, carry):
            source = lax.rem(me + k, n_stage)
            pltpu.make_async_remote_copy(
                src_ref=buf.at[source], dst_ref=buf.at[source], send_sem=dx_send.at[source], recv_sem=recv.at[source],
                device_id=(dp, source), device_id_type=MESH).wait_recv()
            return carry
        lax.fori_loop(1, n_stage, one, 0)

    wait_from(x_all, x_recv)
    to_peers(lambda target: dx_copy(target).start())
    wait_from(dy_all, dy_recv)
    wait_from(n_all, n_recv)
    wait_from(misc_all, misc_recv)
    wait_from(dx_all, dx_recv)
    n_out[...] = n_all[...]
    misc_out[...] = misc_all[...]
    dx_out[...] = dx_all[...]
    x_out[...] = x_all[...]
    dy_out[...] = dy_all[...]

    for copy in sends:
        copy.wait_send()
    for make in (dy_copy, n_copy, misc_copy, dx_copy):
        to_peers(lambda target, make=make: make(target).wait_send())


def table_kernel(inv_count, tok_ref, lab_ref, misc_ref, n_ref, dx_ref, x_ref, dy_ref, up_ref, down_ref, table_hbm,
                 out_hbm, loss_out, gup_out, gdown_out, table, acc, dx_wide, fix_rows, lse_row, table_sem, out_sem):
    vocab, dim = table.shape
    n_micro, seq, _ = n_ref.shape
    count = n_micro * seq
    logit_scale = dim ** -0.5
    table_copy = pltpu.make_async_copy(table_hbm, table, table_sem)
    table_copy.start()
    acc[...] = jnp.zeros_like(acc)

    up, down = up_ref[0], down_ref[0]
    gup_out[...] = jnp.zeros_like(gup_out)
    gdown_out[...] = jnp.zeros_like(gdown_out)
    group = max(1, 256 // seq)

    def wgrad(i, carry):
        x_act = x_ref[pl.ds(i * group, group)].reshape(group * seq, dim)
        grad_out = dy_ref[pl.ds(i * group, group)].reshape(group * seq, dim)
        pre = dot_nn(x_act, up).astype(BF16).astype(F32)
        hidden = gelu(pre).astype(BF16)
        gdown_out[...] += dot_tn(hidden, grad_out)
        grad_hidden = dot_nt(grad_out, down).astype(BF16).astype(F32)
        grad_pre = (grad_hidden * gelu_grad(pre)).astype(BF16)
        gup_out[...] += dot_tn(x_act, grad_pre)
        return carry

    lax.fori_loop(0, n_micro // group, wgrad, 0)

    eye = lax.broadcasted_iota(jnp.int32, (seq, LANES), 0) == lax.broadcasted_iota(jnp.int32, (seq, LANES), 1)
    per_row = LANES // seq
    total = jnp.zeros((8, LANES), F32)
    for m in range(n_micro):
        misc = misc_ref[m]
        total = total + misc
        fix = jnp.sum(jnp.where(eye, misc[1:2, :], 0.0), axis=-1, keepdims=True) * logit_scale
        fix_rows[pl.ds(m * seq, seq), :] = n_ref[m].astype(F32) * fix
        dx_wide[pl.ds(m * seq, seq), :] = dx_ref[m].astype(F32)
        if m % per_row == 0:
            row = misc
            for k in range(1, per_row):
                row = row + pltpu.roll(misc_ref[m + k], k * seq, 1)
            lse_row[:, pl.ds(m * seq, LANES)] = row
    loss_out[0] = jnp.max(total[2:3, :])

    def scatter(m, carry):
        def one(i, inner):
            acc[pl.ds(tok_ref[m, i], 1), :] += dx_wide[pl.ds(m * seq + i, 1), :]
            acc[pl.ds(lab_ref[m, i], 1), :] += fix_rows[pl.ds(m * seq + i, 1), :]
            return inner
        return lax.fori_loop(0, seq, one, carry, unroll=8)

    lax.fori_loop(0, n_micro, scatter, 0)
    table_copy.wait()

    rows, n_full, tail = chunks(vocab, TABLE_ROWS)
    lse = lse_row[0:1, :]

    def out_copy(first, height, index):
        return pltpu.make_async_copy(acc.at[pl.ds(first, height), :], out_hbm.at[pl.ds(first, height), :], out_sem.at[index])

    def part(first, height, index):
        normed = n_ref[...].reshape(count, dim)
        z = (dot_nt(table[pl.ds(first, height), :], normed) * logit_scale).astype(BF16).astype(F32)
        grad_z = jnp.exp(z - lse).astype(BF16)
        acc[pl.ds(first, height), :] += dot_nn(grad_z, normed) * logit_scale
        out_copy(first, height, index).start()

    def loop(i, carry):
        part(pl.multiple_of(i * rows, rows), rows, i)
        return carry

    lax.fori_loop(0, n_full, loop, 0)
    if tail:
        part(n_full * rows, tail, n_full)

    def drain(i, carry):
        out_copy(pl.multiple_of(i * rows, rows), rows, i).wait()
        return carry

    lax.fori_loop(0, n_full, drain, 0)
    if tail:
        out_copy(n_full * rows, tail, n_full).wait()


def solution(mesh):
    n_stage = mesh.shape["stage"]

    def device_fn(tokens, labels, emb_table, w_up, w_down):
        n_micro, seq = tokens.shape
        vocab, dim = emb_table.shape
        ffn = w_up.shape[2]
        count = n_micro * seq
        inv_count = 1.0 / count
        vmem = pl.BlockSpec(memory_space=pltpu.VMEM)
        smem = pl.BlockSpec(memory_space=pltpu.SMEM)
        hbm = pl.BlockSpec(memory_space=pl.ANY)
        dma = pltpu.SemaphoreType.DMA

        act = jax.ShapeDtypeStruct((n_stage, seq, dim), BF16)
        n_all, dx_all, x_all, dy_all, misc = pl.pallas_call(
            functools.partial(step_kernel, n_stage, inv_count),
            name="step",
            out_shape=(act, act, act, act, jax.ShapeDtypeStruct((n_stage, 8, LANES), F32)),
            in_specs=[smem, vmem, hbm, vmem, vmem],
            out_specs=(vmem,) * 5,
            scratch_shapes=[
                pltpu.VMEM((vocab // TILE, TILE, dim), BF16),
                pltpu.VMEM((n_stage, dim, ffn), BF16),
                pltpu.VMEM((n_stage, ffn, dim), BF16),
                pltpu.VMEM((n_stage, seq, dim), BF16),
                pltpu.VMEM((n_stage, seq, ffn), BF16),
                pltpu.VMEM((n_stage, seq, dim), BF16),
                pltpu.VMEM((seq, vocab), BF16),
                pltpu.VMEM((seq, dim), BF16),
                pltpu.VMEM((8, LANES), F32),
                pltpu.VMEM((seq, dim), BF16),
                pltpu.VMEM((seq, dim), F32),
                pltpu.VMEM((n_stage, seq, dim), BF16),
                pltpu.VMEM((n_stage, 8, LANES), F32),
                pltpu.VMEM((n_stage, seq, dim), BF16),
                pltpu.VMEM((n_stage, seq, dim), BF16),
                pltpu.VMEM((n_stage, seq, dim), BF16),
                dma, dma((n_stage,)), dma((n_stage,)), dma((3, n_stage)), dma((3, n_stage)),
                dma((n_stage,)), dma((n_stage,)), dma((n_stage,)), dma((n_stage,)), dma((n_stage,)),
                dma((n_stage,)), dma((n_stage,)), dma((n_stage,)), dma((n_stage,)), dma((n_stage,)),
            ],
            compiler_params=pltpu.CompilerParams(collective_id=0, has_side_effects=True),
        )(tokens, labels, emb_table.reshape(vocab // TILE, TILE, dim), w_up, w_down)

        n_parts = -(-vocab // TABLE_ROWS)
        grad_emb, loss, g_up, g_down = pl.pallas_call(
            functools.partial(table_kernel, inv_count),
            name="table_grad",
            out_shape=(
                jax.ShapeDtypeStruct((vocab, dim), F32),
                jax.ShapeDtypeStruct((1,), F32),
                jax.ShapeDtypeStruct((dim, ffn), F32),
                jax.ShapeDtypeStruct((ffn, dim), F32),
            ),
            in_specs=[smem, smem, vmem, vmem, vmem, vmem, vmem, vmem, vmem, hbm],
            out_specs=(hbm, smem, vmem, vmem),
            scratch_shapes=[
                pltpu.VMEM((vocab, dim), BF16),
                pltpu.VMEM((vocab, dim), F32),
                pltpu.VMEM((count, dim), F32),
                pltpu.VMEM((count, dim), F32),
                pltpu.VMEM((8, count), F32),
                dma, dma((n_parts,)),
            ],
        )(tokens, labels, misc, n_all, dx_all, x_all, dy_all, w_up, w_down, emb_table)
        return loss, g_up[None], g_down[None], grad_emb

    return jax.shard_map(device_fn, mesh=mesh, in_specs=(P("dp", None), P("dp", None), P(None, None), P("stage", None, None), P("stage", None, None)), out_specs=(P("dp"), P(("dp", "stage"), None, None), P(("dp", "stage"), None, None), P("dp", None)), check_vma=False)
```

```python
import functools
import math

import jax
import jax.numpy as jnp
from jax import lax
from jax.experimental import pallas as pl
from jax.experimental.pallas import tpu as pltpu
from jax.sharding import PartitionSpec as P

F32 = jnp.float32
BF16 = jnp.bfloat16
MESH = pl.DeviceIdType.MESH
LANES = 128
TILE = 16
HEAD_COLS = 1024
TABLE_ROWS = 2048
OUT_ROWS = 2048
GELU_C = math.sqrt(2.0 / math.pi)
GELU_K = 0.044715
RMS_EPS = 1e-6


def dot_nn(a, b):
    return lax.dot_general(a, b, (((1,), (0,)), ((), ())), preferred_element_type=F32)


def dot_nt(a, b):
    return lax.dot_general(a, b, (((1,), (1,)), ((), ())), preferred_element_type=F32)


def dot_tn(a, b):
    return lax.dot_general(a, b, (((0,), (0,)), ((), ())), preferred_element_type=F32)


def gelu(a):
    return a * (0.5 * (1.0 + jnp.tanh(GELU_C * (a + GELU_K * (a * a * a)))))


def gelu_grad(a):
    sq = a * a
    t = jnp.tanh(GELU_C * (a + GELU_K * (sq * a)))
    return 0.5 * (1.0 + t) + (0.5 * GELU_C) * a * (1.0 - t * t) * (1.0 + (3.0 * GELU_K) * sq)


def chunks(total, size):
    return size, total // size, total % size


def step_kernel(n_stage, inv_count, tok_ref, lab_ref, table_hbm, w_up_ref, w_down_ref,
                n_out, dx_out, x_out, dy_out, misc_out, head_hbm,
                table, up_all, down_all, x_hist, pre_hist, dy_hist, logits,
                n_mine, misc_mine, dx_mine, x_rows, lse_row, head_part, n_all, misc_all, dx_all, x_all, dy_all,
                table_sem, up_recv, down_recv, up_send, down_send,
                x_recv, dy_recv, n_recv, misc_recv, dx_recv,
                x_send, dy_send, n_send, misc_send, dx_send, keep_sem, part_send, part_recv):
    me = lax.axis_index("stage")
    dp = lax.axis_index("dp")
    n_chip = n_stage // 2
    half = n_chip // 2
    chip, core = me // 2, lax.rem(me, 2)
    dim = table.shape[2]
    vocab = table.shape[0] * TILE
    seq = x_hist.shape[1]
    logit_scale = dim ** -0.5

    def slot_at(offset, which):
        return lax.rem(chip + offset + n_chip, n_chip) * 2 + which

    right, left, partner = slot_at(1, core), slot_at(-1, core), chip * 2 + (1 - core)

    table_copy = pltpu.make_async_copy(table_hbm, table, table_sem)
    table_copy.start()

    barrier = pltpu.get_barrier_semaphore()

    def greet(k, carry):
        pl.semaphore_signal(barrier, inc=1, device_id=(dp, lax.rem(me + k, n_stage)), device_id_type=MESH)
        return carry

    lax.fori_loop(1, n_stage, greet, 0)
    pl.semaphore_wait(barrier, n_stage - 1)

    def up_copy(slot, way, target, own=False):
        return pltpu.make_async_remote_copy(
            src_ref=w_up_ref.at[0] if own else up_all.at[slot], dst_ref=up_all.at[slot],
            send_sem=up_send.at[way, slot], recv_sem=up_recv.at[slot],
            device_id=(dp, target), device_id_type=MESH)

    def down_copy(slot, way, target, own=False):
        return pltpu.make_async_remote_copy(
            src_ref=w_down_ref.at[0] if own else down_all.at[slot], dst_ref=down_all.at[slot],
            send_sem=down_send.at[way, slot], recv_sem=down_recv.at[slot],
            device_id=(dp, target), device_id_type=MESH)

    sends = []

    def send(copy):
        copy.start()
        sends.append(copy)

    for way, target in ((0, right), (1, left), (2, partner)):
        send(up_copy(me, way, target, own=True))
        send(down_copy(me, way, target, own=True))
    up_all[me] = w_up_ref[0]
    down_all[me] = w_down_ref[0]

    table_copy.wait()
    row_iota = lax.broadcasted_iota(jnp.int32, (TILE, dim), 0)

    def embed(i, carry):
        tok = tok_ref[me, i]
        tile = table[lax.div(tok, TILE)].astype(F32)
        row = jnp.sum(jnp.where(row_iota == lax.rem(tok, TILE), tile, 0.0), axis=0, keepdims=True)
        x_rows[pl.ds(i, 1), :] = row
        return carry

    lax.fori_loop(0, seq, embed, 0)
    x_now = x_rows[...].astype(BF16)

    for t in range(1, half + 1):
        slot_l, slot_r = slot_at(-t, core), slot_at(t, core)
        up_copy(slot_l, 0, right).wait_recv()
        if t < half:
            send(up_copy(slot_l, 0, right))
        send(up_copy(slot_l, 2, partner))
        down_copy(slot_r, 1, left).wait_recv()
        if t < half:
            send(down_copy(slot_r, 1, left))
        send(down_copy(slot_r, 2, partner))
        if t < half:
            down_copy(slot_l, 0, right).wait_recv()
            if t < half - 1:
                send(down_copy(slot_l, 0, right))
            send(down_copy(slot_l, 2, partner))
            up_copy(slot_r, 1, left).wait_recv()
            if t < half - 1:
                send(up_copy(slot_r, 1, left))
            send(up_copy(slot_r, 2, partner))

    for t in range(n_chip):
        slot = slot_at(t, 1 - core)
        up_copy(slot, 2, partner).wait_recv()
        down_copy(slot, 2, partner).wait_recv()

    def forward(s, x_act):
        x_hist[s] = x_act
        pre = dot_nn(x_act, up_all[s]).astype(BF16)
        pre_hist[s] = pre
        hidden = gelu(pre.astype(F32)).astype(BF16)
        return (x_act.astype(F32) + dot_nn(hidden, down_all[s])).astype(BF16)

    x_last = lax.fori_loop(0, n_stage, forward, x_now)

    def peer_copy(src, dst, send_sem, recv_sem, target):
        return pltpu.make_async_remote_copy(
            src_ref=src, dst_ref=dst.at[me], send_sem=send_sem.at[target], recv_sem=recv_sem.at[me],
            device_id=(dp, target), device_id_type=MESH)

    def x_copy(target):
        return peer_copy(x_hist.at[target], x_all, x_send, x_recv, target)

    def dy_copy(target):
        return peer_copy(dy_hist.at[target], dy_all, dy_send, dy_recv, target)

    def n_copy(target):
        return peer_copy(n_mine, n_all, n_send, n_recv, target)

    def misc_copy(target):
        return peer_copy(misc_mine, misc_all, misc_send, misc_recv, target)

    def dx_copy(target):
        return peer_copy(dx_mine, dx_all, dx_send, dx_recv, target)

    def to_peers(start):
        def one(k, carry):
            start(lax.rem(me + k, n_stage))
            return carry
        lax.fori_loop(1, n_stage, one, 0)

    def wait_from(buf, recv):
        def one(k, carry):
            source = lax.rem(me + k, n_stage)
            pltpu.make_async_remote_copy(
                src_ref=buf.at[source], dst_ref=buf.at[source], send_sem=dx_send.at[source], recv_sem=recv.at[source],
                device_id=(dp, source), device_id_type=MESH).wait_recv()
            return carry
        lax.fori_loop(1, n_stage, one, 0)

    x_wide = x_last.astype(F32)
    inv_rms = lax.rsqrt(jnp.mean(x_wide * x_wide, axis=-1, keepdims=True) + RMS_EPS)
    normed = (x_wide * inv_rms).astype(BF16)
    n_mine[...] = normed
    n_all[me] = normed
    to_peers(lambda target: x_copy(target).start())
    x_all[me] = x_hist[me]
    to_peers(lambda target: n_copy(target).start())

    cols, n_full, tail = chunks(vocab, HEAD_COLS)

    def table_rows(first, width):
        tile = first // TILE if isinstance(first, int) else lax.div(first, TILE)
        return table[pl.ds(tile, width // TILE)].reshape(width, dim)

    def pass_one(first, width, carry):
        top, total = carry
        z = (dot_nt(normed, table_rows(first, width)) * logit_scale).astype(BF16)
        logits[:, pl.ds(first, width)] = z
        parts = [z[:, j:j + LANES].astype(F32) for j in range(0, width, LANES)]
        new_top = top
        for part in parts:
            new_top = jnp.maximum(new_top, part)
        total = total * jnp.exp(top - new_top)
        for part in parts:
            total = total + jnp.exp(part - new_top)
        return new_top, total

    def head_loop(body, carry):
        carry = lax.fori_loop(0, n_full, lambda i, c: body(pl.multiple_of(i * cols, cols), cols, c), carry)
        if tail:
            carry = body(n_full * cols, tail, carry)
        return carry

    top, total = head_loop(pass_one, (jnp.full((seq, LANES), -1e30, F32), jnp.zeros((seq, LANES), F32)))
    row_top = jnp.max(top, axis=-1, keepdims=True)
    row_sum = jnp.sum(total * jnp.exp(top - row_top), axis=-1, keepdims=True)
    lse = row_top + jnp.log(row_sum)

    lane_iota = lax.broadcasted_iota(jnp.int32, (seq, LANES), 1)
    lane_wide = lane_iota.astype(F32)
    square = lax.broadcasted_iota(jnp.int32, (seq, seq), 0) == lax.broadcasted_iota(jnp.int32, (seq, seq), 1)
    label = jnp.sum(jnp.where(square, lab_ref[pl.ds(me, 1), :].astype(F32), 0.0), axis=-1, keepdims=True)
    lse_count = lse + math.log(1.0 / inv_count)

    def pass_two(first, width, carry):
        picked, grad_n = carry
        base = label - jnp.asarray(first, jnp.int32).astype(F32)
        grads = []
        for j in range(0, width, LANES):
            z = logits[:, pl.ds(first + j, LANES)].astype(F32)
            prob = jnp.exp(z - lse_count)
            hit = lane_wide == base - float(j)
            picked = picked + jnp.where(hit, z, 0.0)
            grads.append(jnp.where(hit, prob - inv_count, prob).astype(BF16))
        grad_z = jnp.concatenate(grads, axis=1)
        return picked, grad_n + dot_nn(grad_z, table_rows(first, width))

    picked, grad_n = head_loop(pass_two, (jnp.zeros((seq, LANES), F32), jnp.zeros((seq, dim), F32)))
    picked = jnp.sum(picked, axis=-1, keepdims=True)
    loss = jnp.sum((lse - picked) * inv_count)
    label_prob = jnp.exp(picked - lse_count)
    fix = (label_prob - inv_count).astype(BF16).astype(F32) - label_prob.astype(BF16).astype(F32)
    eye = lax.broadcasted_iota(jnp.int32, (seq, LANES), 0) == lane_iota

    def as_row(column):
        return jnp.broadcast_to(jnp.sum(jnp.where(eye, column, 0.0), axis=0, keepdims=True), (8, LANES))

    row8 = lax.broadcasted_iota(jnp.int32, (8, LANES), 0)
    misc = jnp.where(row8 == 0, as_row(lse_count), jnp.where(row8 == 1, as_row(fix), loss))
    misc_mine[...] = misc
    misc_all[me] = misc

    grad_n = (grad_n * logit_scale).astype(BF16).astype(F32)
    along = jnp.mean(grad_n * x_wide, axis=-1, keepdims=True)
    grad_x = (inv_rms * grad_n - x_wide * (inv_rms * inv_rms * inv_rms * along)).astype(BF16)

    to_peers(lambda target: misc_copy(target).start())

    def backward(k, grad_out):
        s = n_stage - 1 - k
        dy_hist[s] = grad_out
        grad_hidden = dot_nt(grad_out, down_all[s]).astype(BF16).astype(F32)
        grad_pre = (grad_hidden * gelu_grad(pre_hist[s].astype(F32))).astype(BF16)
        result = (grad_out.astype(F32) + dot_nt(grad_pre, up_all[s])).astype(BF16)

        @pl.when(s != me)
        def _():
            dy_copy(s).start()

        return result

    grad_in = lax.fori_loop(0, n_stage, backward, grad_x)
    dx_mine[...] = grad_in
    dy_all[me] = dy_hist[me]
    dx_all[me] = grad_in

    wait_from(n_all, n_recv)
    wait_from(misc_all, misc_recv)
    per_row = LANES // seq
    for m in range(0, n_stage, per_row):
        row = misc_all[m]
        for k in range(1, per_row):
            row = row + pltpu.roll(misc_all[m + k], k * seq, 1)
        lse_row[:, pl.ds(m * seq, LANES)] = row
    to_peers(lambda target: dx_copy(target).start())

    half_rows = vocab // 2
    rows, n_full, tail = chunks(half_rows, TABLE_ROWS)
    count = n_stage * seq

    def keep_copy(first, height, index):
        return pltpu.make_async_copy(
            head_part.at[pl.ds(first, height), :], head_hbm.at[pl.ds(core * half_rows + first, height), :], keep_sem.at[index])

    def part_copy(first, height, index, owner):
        return pltpu.make_async_remote_copy(
            src_ref=head_part.at[pl.ds(first, height), :],
            dst_ref=head_hbm.at[pl.ds(owner * half_rows + first, height), :],
            send_sem=part_send.at[index], recv_sem=part_recv.at[index],
            device_id=(dp, partner), device_id_type=MESH)

    def pass_on(first, height, index):
        keep_copy(first, height, index).start()
        part_copy(first, height, index, core).start()

    def head_rows(first, height):
        every = n_all[...].reshape(count, dim)
        tile = lax.div(core * half_rows + first, TILE)
        z = (dot_nt(table[pl.ds(tile, height // TILE)].reshape(height, dim), every) * logit_scale).astype(BF16).astype(F32)
        grad_z = jnp.exp(z - lse_row[0:1, :]).astype(BF16)
        head_part[pl.ds(first, height), :] = dot_nn(grad_z, every) * logit_scale

    def head_chunk(i, carry):
        @pl.when(i > 0)
        def _():
            pass_on(pl.multiple_of((i - 1) * rows, TILE), rows, i - 1)

        head_rows(pl.multiple_of(i * rows, rows), rows)
        return carry

    lax.fori_loop(0, n_full, head_chunk, 0)
    if tail:
        pass_on((n_full - 1) * rows, rows, n_full - 1)
        head_rows(n_full * rows, tail)

    to_peers(lambda target: x_copy(target).wait_send())
    wait_from(x_all, x_recv)
    wait_from(dy_all, dy_recv)
    wait_from(dx_all, dx_recv)
    if tail:
        pass_on(n_full * rows, tail, n_full)
    else:
        pass_on((n_full - 1) * rows, rows, n_full - 1)
    n_out[...] = n_all[...]
    misc_out[...] = misc_all[...]
    dx_out[...] = dx_all[...]
    x_out[...] = x_all[...]
    dy_out[...] = dy_all[...]

    for copy in sends:
        copy.wait_send()
    for make in (dy_copy, n_copy, misc_copy, dx_copy):
        to_peers(lambda target, make=make: make(target).wait_send())

    def finish(first, height, index):
        keep_copy(first, height, index).wait()
        part_copy(first, height, index, core).wait_send()
        part_copy(first, height, index, 1 - core).wait_recv()

    def finish_chunk(i, carry):
        finish(pl.multiple_of(i * rows, rows), rows, i)
        return carry

    lax.fori_loop(0, n_full, finish_chunk, 0)
    if tail:
        finish(n_full * rows, tail, n_full)


def table_kernel(inv_count, tok_ref, lab_ref, misc_ref, n_ref, dx_ref, x_ref, dy_ref, up_ref, down_ref, head_hbm,
                 out_hbm, loss_out, gup_out, gdown_out, head, acc, acc_lab, dx_wide, fix_rows, head_sem, out_sem):
    vocab, dim = acc.shape
    n_micro, seq, _ = n_ref.shape
    logit_scale = dim ** -0.5
    rows, n_full, tail = chunks(vocab, OUT_ROWS)

    def head_copy(first, height, index):
        return pltpu.make_async_copy(head_hbm.at[pl.ds(first, height), :], head.at[pl.ds(first, height), :], head_sem.at[index])

    def out_copy(first, height, index):
        return pltpu.make_async_copy(acc.at[pl.ds(first, height), :], out_hbm.at[pl.ds(first, height), :], out_sem.at[index])

    def each(body):
        def one(i, carry):
            body(pl.multiple_of(i * rows, rows), rows, i)
            return carry
        lax.fori_loop(0, n_full, one, 0)
        if tail:
            body(n_full * rows, tail, n_full)

    each(lambda *where: head_copy(*where).start())

    def clear(first, height, index):
        acc[pl.ds(first, height), :] = jnp.zeros((height, dim), F32)
        acc_lab[pl.ds(first, height), :] = jnp.zeros((height, dim), F32)

    each(clear)

    eye = lax.broadcasted_iota(jnp.int32, (seq, LANES), 0) == lax.broadcasted_iota(jnp.int32, (seq, LANES), 1)
    total = jnp.zeros((8, LANES), F32)
    for m in range(n_micro):
        misc = misc_ref[m]
        total = total + misc
        fix = jnp.sum(jnp.where(eye, misc[1:2, :], 0.0), axis=-1, keepdims=True) * logit_scale
        fix_rows[pl.ds(m * seq, seq), :] = n_ref[m].astype(F32) * fix
        dx_wide[pl.ds(m * seq, seq), :] = dx_ref[m].astype(F32)
    loss_out[0] = jnp.max(total[2:3, :])

    def scatter(m, carry):
        for i in range(seq):
            acc[pl.ds(tok_ref[m, i], 1), :] += dx_wide[pl.ds(m * seq + i, 1), :]
            acc_lab[pl.ds(lab_ref[m, i], 1), :] += fix_rows[pl.ds(m * seq + i, 1), :]
        return carry

    lax.fori_loop(0, n_micro, scatter, 0)

    def join(first, height, index):
        head_copy(first, height, index).wait()
        where = pl.ds(first, height)
        acc[where, :] = head[where, :] + (acc[where, :] + acc_lab[where, :])
        out_copy(first, height, index).start()

    each(join)

    up, down = up_ref[0], down_ref[0]
    gup_out[...] = jnp.zeros_like(gup_out)
    gdown_out[...] = jnp.zeros_like(gdown_out)
    group = max(1, 256 // seq)

    def wgrad(i, carry):
        x_act = x_ref[pl.ds(i * group, group)].reshape(group * seq, dim)
        grad_out = dy_ref[pl.ds(i * group, group)].reshape(group * seq, dim)
        pre = dot_nn(x_act, up).astype(BF16).astype(F32)
        hidden = gelu(pre).astype(BF16)
        gdown_out[...] += dot_tn(hidden, grad_out)
        grad_hidden = dot_nt(grad_out, down).astype(BF16).astype(F32)
        grad_pre = (grad_hidden * gelu_grad(pre)).astype(BF16)
        gup_out[...] += dot_tn(x_act, grad_pre)
        return carry

    lax.fori_loop(0, n_micro // group, wgrad, 0)
    each(lambda *where: out_copy(*where).wait())


def solution(mesh):
    n_stage = mesh.shape["stage"]

    def device_fn(tokens, labels, emb_table, w_up, w_down):
        n_micro, seq = tokens.shape
        vocab, dim = emb_table.shape
        ffn = w_up.shape[2]
        count = n_micro * seq
        inv_count = 1.0 / count
        vmem = pl.BlockSpec(memory_space=pltpu.VMEM)
        smem = pl.BlockSpec(memory_space=pltpu.SMEM)
        hbm = pl.BlockSpec(memory_space=pl.ANY)
        dma = pltpu.SemaphoreType.DMA

        n_parts = -(-vocab // (2 * TABLE_ROWS))
        act = jax.ShapeDtypeStruct((n_stage, seq, dim), BF16)
        n_all, dx_all, x_all, dy_all, misc, head = pl.pallas_call(
            functools.partial(step_kernel, n_stage, inv_count),
            name="step",
            out_shape=(act, act, act, act, jax.ShapeDtypeStruct((n_stage, 8, LANES), F32), jax.ShapeDtypeStruct((vocab, dim), F32)),
            in_specs=[smem, vmem, hbm, vmem, vmem],
            out_specs=(vmem,) * 5 + (hbm,),
            scratch_shapes=[
                pltpu.VMEM((vocab // TILE, TILE, dim), BF16),
                pltpu.VMEM((n_stage, dim, ffn), BF16),
                pltpu.VMEM((n_stage, ffn, dim), BF16),
                pltpu.VMEM((n_stage, seq, dim), BF16),
                pltpu.VMEM((n_stage, seq, ffn), BF16),
                pltpu.VMEM((n_stage, seq, dim), BF16),
                pltpu.VMEM((seq, vocab), BF16),
                pltpu.VMEM((seq, dim), BF16),
                pltpu.VMEM((8, LANES), F32),
                pltpu.VMEM((seq, dim), BF16),
                pltpu.VMEM((seq, dim), F32),
                pltpu.VMEM((8, count), F32),
                pltpu.VMEM((vocab // 2, dim), F32),
                pltpu.VMEM((n_stage, seq, dim), BF16),
                pltpu.VMEM((n_stage, 8, LANES), F32),
                pltpu.VMEM((n_stage, seq, dim), BF16),
                pltpu.VMEM((n_stage, seq, dim), BF16),
                pltpu.VMEM((n_stage, seq, dim), BF16),
                dma, dma((n_stage,)), dma((n_stage,)), dma((3, n_stage)), dma((3, n_stage)),
                dma((n_stage,)), dma((n_stage,)), dma((n_stage,)), dma((n_stage,)), dma((n_stage,)),
                dma((n_stage,)), dma((n_stage,)), dma((n_stage,)), dma((n_stage,)), dma((n_stage,)),
                dma((n_parts,)), dma((n_parts,)), dma((n_parts,)),
            ],
            compiler_params=pltpu.CompilerParams(collective_id=0, has_side_effects=True),
        )(tokens, labels, emb_table.reshape(vocab // TILE, TILE, dim), w_up, w_down)

        n_outs = -(-vocab // OUT_ROWS)
        grad_emb, loss, g_up, g_down = pl.pallas_call(
            functools.partial(table_kernel, inv_count),
            name="table_grad",
            out_shape=(
                jax.ShapeDtypeStruct((vocab, dim), F32),
                jax.ShapeDtypeStruct((1,), F32),
                jax.ShapeDtypeStruct((dim, ffn), F32),
                jax.ShapeDtypeStruct((ffn, dim), F32),
            ),
            in_specs=[smem, smem, vmem, vmem, vmem, vmem, vmem, vmem, vmem, hbm],
            out_specs=(hbm, smem, vmem, vmem),
            scratch_shapes=[
                pltpu.VMEM((vocab, dim), F32),
                pltpu.VMEM((vocab, dim), F32),
                pltpu.VMEM((vocab, dim), F32),
                pltpu.VMEM((count, dim), F32),
                pltpu.VMEM((count, dim), F32),
                dma((n_outs,)), dma((n_outs,)),
            ],
        )(tokens, labels, misc, n_all, dx_all, x_all, dy_all, w_up, w_down, head)
        return loss, g_up[None], g_down[None], grad_emb

    return jax.shard_map(device_fn, mesh=mesh, in_specs=(P("dp", None), P("dp", None), P(None, None), P("stage", None, None), P("stage", None, None)), out_specs=(P("dp"), P(("dp", "stage"), None, None), P(("dp", "stage"), None, None), P("dp", None)), check_vma=False)
```

```python
import functools
import math

import jax
import jax.numpy as jnp
from jax import lax
from jax.experimental import pallas as pl
from jax.experimental.pallas import tpu as pltpu
from jax.sharding import PartitionSpec as P

F32 = jnp.float32
BF16 = jnp.bfloat16
MESH = pl.DeviceIdType.MESH
LANES = 128
TILE = 16
HEAD_COLS = 4096
TABLE_ROWS = 2048
OUT_ROWS = 2048
GELU_C = math.sqrt(2.0 / math.pi)
GELU_K = 0.044715
RMS_EPS = 1e-6


def dot_nn(a, b):
    return lax.dot_general(a, b, (((1,), (0,)), ((), ())), preferred_element_type=F32)


def dot_nt(a, b):
    return lax.dot_general(a, b, (((1,), (1,)), ((), ())), preferred_element_type=F32)


def dot_tn(a, b):
    return lax.dot_general(a, b, (((0,), (0,)), ((), ())), preferred_element_type=F32)


def gelu(a):
    return a * (0.5 * (1.0 + jnp.tanh(GELU_C * (a + GELU_K * (a * a * a)))))


def gelu_grad(a):
    sq = a * a
    t = jnp.tanh(GELU_C * (a + GELU_K * (sq * a)))
    return 0.5 * (1.0 + t) + (0.5 * GELU_C) * a * (1.0 - t * t) * (1.0 + (3.0 * GELU_K) * sq)


def chunks(total, size):
    return size, total // size, total % size


def step_kernel(n_stage, inv_count, tok_hbm, lab_hbm, table_hbm, w_up_hbm, w_down_hbm,
                n_out, dx_out, x_out, dy_out, misc_out, head_hbm,
                tok_ref, lab_ref, table, up_all, down_all, x_hist, pre_hist, dy_hist, logits,
                n_mine, misc_mine, dx_mine, x_rows, lse_row, head_part, n_all, misc_all, dx_all, x_all, dy_all,
                in_sem, out_sem, table_sem, up_recv, down_recv, up_send, down_send,
                x_recv, dy_recv, n_recv, misc_recv, dx_recv,
                x_send, dy_send, n_send, misc_send, dx_send, keep_sem, part_send, part_recv):
    me = lax.axis_index("stage")
    dp = lax.axis_index("dp")
    n_chip = n_stage // 2
    half = n_chip // 2
    chip, core = me // 2, lax.rem(me, 2)
    dim = table.shape[2]
    vocab = table.shape[0] * TILE
    seq = x_hist.shape[1]
    logit_scale = dim ** -0.5

    def slot_at(offset, which):
        return lax.rem(chip + offset + n_chip, n_chip) * 2 + which

    right, left, partner = slot_at(1, core), slot_at(-1, core), chip * 2 + (1 - core)

    loads = [
        pltpu.make_async_copy(w_up_hbm.at[0], up_all.at[me], in_sem.at[0]),
        pltpu.make_async_copy(w_down_hbm.at[0], down_all.at[me], in_sem.at[1]),
        pltpu.make_async_copy(tok_hbm, tok_ref, in_sem.at[2]),
        pltpu.make_async_copy(lab_hbm, lab_ref, in_sem.at[3]),
    ]
    for load in loads:
        load.start()
    table_copy = pltpu.make_async_copy(table_hbm, table, table_sem)
    table_copy.start()

    barrier = pltpu.get_barrier_semaphore()

    def greet(k, carry):
        pl.semaphore_signal(barrier, inc=1, device_id=(dp, lax.rem(me + k, n_stage)), device_id_type=MESH)
        return carry

    lax.fori_loop(1, n_stage, greet, 0)
    pl.semaphore_wait(barrier, n_stage - 1)
    for load in loads:
        load.wait()

    def up_copy(slot, way, target):
        return pltpu.make_async_remote_copy(
            src_ref=up_all.at[slot], dst_ref=up_all.at[slot],
            send_sem=up_send.at[way, slot], recv_sem=up_recv.at[slot],
            device_id=(dp, target), device_id_type=MESH)

    def down_copy(slot, way, target):
        return pltpu.make_async_remote_copy(
            src_ref=down_all.at[slot], dst_ref=down_all.at[slot],
            send_sem=down_send.at[way, slot], recv_sem=down_recv.at[slot],
            device_id=(dp, target), device_id_type=MESH)

    sends = []

    def send(copy):
        copy.start()
        sends.append(copy)

    for way, target in ((0, right), (1, left), (2, partner)):
        send(up_copy(me, way, target))
        send(down_copy(me, way, target))

    table_copy.wait()
    row_iota = lax.broadcasted_iota(jnp.int32, (TILE, dim), 0)

    def embed(i, carry):
        tok = tok_ref[me, i]
        tile = table[lax.div(tok, TILE)].astype(F32)
        row = jnp.sum(jnp.where(row_iota == lax.rem(tok, TILE), tile, 0.0), axis=0, keepdims=True)
        x_rows[pl.ds(i, 1), :] = row
        return carry

    lax.fori_loop(0, seq, embed, 0)
    x_now = x_rows[...].astype(BF16)

    for t in range(1, half + 1):
        slot_l, slot_r = slot_at(-t, core), slot_at(t, core)
        up_copy(slot_l, 0, right).wait_recv()
        if t < half:
            send(up_copy(slot_l, 0, right))
        send(up_copy(slot_l, 2, partner))
        down_copy(slot_r, 1, left).wait_recv()
        if t < half:
            send(down_copy(slot_r, 1, left))
        send(down_copy(slot_r, 2, partner))
        if t < half:
            down_copy(slot_l, 0, right).wait_recv()
            if t < half - 1:
                send(down_copy(slot_l, 0, right))
            send(down_copy(slot_l, 2, partner))
            up_copy(slot_r, 1, left).wait_recv()
            if t < half - 1:
                send(up_copy(slot_r, 1, left))
            send(up_copy(slot_r, 2, partner))

    for t in range(n_chip):
        slot = slot_at(t, 1 - core)
        up_copy(slot, 2, partner).wait_recv()
        down_copy(slot, 2, partner).wait_recv()

    def forward(s, x_act):
        x_hist[s] = x_act
        pre = dot_nn(x_act, up_all[s]).astype(BF16)
        pre_hist[s] = pre
        hidden = gelu(pre.astype(F32)).astype(BF16)
        return (x_act.astype(F32) + dot_nn(hidden, down_all[s])).astype(BF16)

    x_last = lax.fori_loop(0, n_stage, forward, x_now)

    def peer_copy(src, dst, send_sem, recv_sem, target):
        return pltpu.make_async_remote_copy(
            src_ref=src, dst_ref=dst.at[me], send_sem=send_sem.at[target], recv_sem=recv_sem.at[me],
            device_id=(dp, target), device_id_type=MESH)

    def x_copy(target):
        return peer_copy(x_hist.at[target], x_all, x_send, x_recv, target)

    def dy_copy(target):
        return peer_copy(dy_hist.at[target], dy_all, dy_send, dy_recv, target)

    def n_copy(target):
        return peer_copy(n_mine, n_all, n_send, n_recv, target)

    def misc_copy(target):
        return peer_copy(misc_mine, misc_all, misc_send, misc_recv, target)

    def dx_copy(target):
        return peer_copy(dx_mine, dx_all, dx_send, dx_recv, target)

    def to_peers(start):
        def one(k, carry):
            start(lax.rem(me + k, n_stage))
            return carry
        lax.fori_loop(1, n_stage, one, 0)

    def wait_from(buf, recv):
        def one(k, carry):
            source = lax.rem(me + k, n_stage)
            pltpu.make_async_remote_copy(
                src_ref=buf.at[source], dst_ref=buf.at[source], send_sem=dx_send.at[source], recv_sem=recv.at[source],
                device_id=(dp, source), device_id_type=MESH).wait_recv()
            return carry
        lax.fori_loop(1, n_stage, one, 0)

    x_wide = x_last.astype(F32)
    inv_rms = lax.rsqrt(jnp.mean(x_wide * x_wide, axis=-1, keepdims=True) + RMS_EPS)
    normed = (x_wide * inv_rms).astype(BF16)
    n_mine[...] = normed
    n_all[me] = normed
    to_peers(lambda target: x_copy(target).start())
    x_all[me] = x_hist[me]
    to_peers(lambda target: n_copy(target).start())

    cols, n_full, tail = chunks(vocab, HEAD_COLS)

    def table_rows(first, width):
        tile = first // TILE if isinstance(first, int) else lax.div(first, TILE)
        return table[pl.ds(tile, width // TILE)].reshape(width, dim)

    def pass_one(first, width, carry):
        top, total = carry
        z = (dot_nt(normed, table_rows(first, width)) * logit_scale).astype(BF16)
        logits[:, pl.ds(first, width)] = z
        parts = [z[:, j:j + LANES].astype(F32) for j in range(0, width, LANES)]
        new_top = top
        for part in parts:
            new_top = jnp.maximum(new_top, part)
        total = total * jnp.exp(top - new_top)
        for part in parts:
            total = total + jnp.exp(part - new_top)
        return new_top, total

    def head_loop(body, carry):
        carry = lax.fori_loop(0, n_full, lambda i, c: body(pl.multiple_of(i * cols, cols), cols, c), carry)
        if tail:
            carry = body(n_full * cols, tail, carry)
        return carry

    top, total = head_loop(pass_one, (jnp.full((seq, LANES), -1e30, F32), jnp.zeros((seq, LANES), F32)))
    row_top = jnp.max(top, axis=-1, keepdims=True)
    row_sum = jnp.sum(total * jnp.exp(top - row_top), axis=-1, keepdims=True)
    lse = row_top + jnp.log(row_sum)

    lane_iota = lax.broadcasted_iota(jnp.int32, (seq, LANES), 1)
    lane_wide = lane_iota.astype(F32)
    square = lax.broadcasted_iota(jnp.int32, (seq, seq), 0) == lax.broadcasted_iota(jnp.int32, (seq, seq), 1)
    label = jnp.sum(jnp.where(square, lab_ref[pl.ds(me, 1), :].astype(F32), 0.0), axis=-1, keepdims=True)
    lse_count = lse + math.log(1.0 / inv_count)

    def pass_two(first, width, carry):
        picked, grad_n = carry
        base = label - jnp.asarray(first, jnp.int32).astype(F32)
        grads = []
        for j in range(0, width, LANES):
            z = logits[:, pl.ds(first + j, LANES)].astype(F32)
            prob = jnp.exp(z - lse_count)
            hit = lane_wide == base - float(j)
            picked = picked + jnp.where(hit, z, 0.0)
            grads.append(jnp.where(hit, prob - inv_count, prob).astype(BF16))
        grad_z = jnp.concatenate(grads, axis=1)
        return picked, grad_n + dot_nn(grad_z, table_rows(first, width))

    picked, grad_n = head_loop(pass_two, (jnp.zeros((seq, LANES), F32), jnp.zeros((seq, dim), F32)))
    picked = jnp.sum(picked, axis=-1, keepdims=True)
    loss = jnp.sum((lse - picked) * inv_count)
    label_prob = jnp.exp(picked - lse_count)
    fix = (label_prob - inv_count).astype(BF16).astype(F32) - label_prob.astype(BF16).astype(F32)
    eye = lax.broadcasted_iota(jnp.int32, (seq, LANES), 0) == lane_iota

    def as_row(column):
        return jnp.broadcast_to(jnp.sum(jnp.where(eye, column, 0.0), axis=0, keepdims=True), (8, LANES))

    row8 = lax.broadcasted_iota(jnp.int32, (8, LANES), 0)
    misc = jnp.where(row8 == 0, as_row(lse_count), jnp.where(row8 == 1, as_row(fix), loss))
    misc_mine[...] = misc
    misc_all[me] = misc

    grad_n = (grad_n * logit_scale).astype(BF16).astype(F32)
    along = jnp.mean(grad_n * x_wide, axis=-1, keepdims=True)
    grad_x = (inv_rms * grad_n - x_wide * (inv_rms * inv_rms * inv_rms * along)).astype(BF16)

    to_peers(lambda target: misc_copy(target).start())

    def backward(k, grad_out):
        s = n_stage - 1 - k
        dy_hist[s] = grad_out
        grad_hidden = dot_nt(grad_out, down_all[s]).astype(BF16).astype(F32)
        grad_pre = (grad_hidden * gelu_grad(pre_hist[s].astype(F32))).astype(BF16)
        result = (grad_out.astype(F32) + dot_nt(grad_pre, up_all[s])).astype(BF16)

        @pl.when(s != me)
        def _():
            dy_copy(s).start()

        return result

    grad_in = lax.fori_loop(0, n_stage, backward, grad_x)
    dx_mine[...] = grad_in
    dy_all[me] = dy_hist[me]
    dx_all[me] = grad_in

    wait_from(n_all, n_recv)
    wait_from(misc_all, misc_recv)
    per_row = LANES // seq
    for m in range(0, n_stage, per_row):
        row = misc_all[m]
        for k in range(1, per_row):
            row = row + pltpu.roll(misc_all[m + k], k * seq, 1)
        lse_row[:, pl.ds(m * seq, LANES)] = row
    to_peers(lambda target: dx_copy(target).start())
    results = [pltpu.make_async_copy(src, dst, out_sem.at[i]) for i, (src, dst) in enumerate(
        ((n_all, n_out), (misc_all, misc_out), (x_all, x_out), (dy_all, dy_out), (dx_all, dx_out)))]
    results[0].start()
    results[1].start()

    half_rows = vocab // 2
    rows, n_full, tail = chunks(half_rows, TABLE_ROWS)
    count = n_stage * seq

    def keep_copy(first, height, index):
        return pltpu.make_async_copy(
            head_part.at[pl.ds(first, height), :], head_hbm.at[pl.ds(core * half_rows + first, height), :], keep_sem.at[index])

    def part_copy(first, height, index, owner):
        return pltpu.make_async_remote_copy(
            src_ref=head_part.at[pl.ds(first, height), :],
            dst_ref=head_hbm.at[pl.ds(owner * half_rows + first, height), :],
            send_sem=part_send.at[index], recv_sem=part_recv.at[index],
            device_id=(dp, partner), device_id_type=MESH)

    def pass_on(first, height, index):
        keep_copy(first, height, index).start()
        part_copy(first, height, index, core).start()

    def head_rows(first, height):
        every = n_all[...].reshape(count, dim)
        tile = lax.div(core * half_rows + first, TILE)
        z = (dot_nt(table[pl.ds(tile, height // TILE)].reshape(height, dim), every) * logit_scale).astype(BF16).astype(F32)
        grad_z = jnp.exp(z - lse_row[0:1, :]).astype(BF16)
        head_part[pl.ds(first, height), :] = dot_nn(grad_z, every) * logit_scale

    def head_chunk(i, carry):
        @pl.when(i > 0)
        def _():
            pass_on(pl.multiple_of((i - 1) * rows, TILE), rows, i - 1)

        head_rows(pl.multiple_of(i * rows, rows), rows)
        return carry

    lax.fori_loop(0, n_full, head_chunk, 0)
    pass_on((n_full - 1) * rows, rows, n_full - 1)
    wait_from(x_all, x_recv)
    wait_from(dy_all, dy_recv)
    wait_from(dx_all, dx_recv)
    for result in results[2:]:
        result.start()
    if tail:
        head_rows(n_full * rows, tail)
    to_peers(lambda target: x_copy(target).wait_send())
    for copy in sends:
        copy.wait_send()
    if tail:
        pass_on(n_full * rows, tail, n_full)
    for make in (dy_copy, n_copy, misc_copy, dx_copy):
        to_peers(lambda target, make=make: make(target).wait_send())
    for result in results:
        result.wait()

    def finish(first, height, index):
        keep_copy(first, height, index).wait()
        part_copy(first, height, index, core).wait_send()
        part_copy(first, height, index, 1 - core).wait_recv()

    def finish_chunk(i, carry):
        finish(pl.multiple_of(i * rows, rows), rows, i)
        return carry

    lax.fori_loop(0, n_full, finish_chunk, 0)
    if tail:
        finish(n_full * rows, tail, n_full)


def table_kernel(tok_hbm, lab_hbm, misc_hbm, n_hbm, dx_hbm, x_hbm, dy_hbm, up_hbm, down_hbm, head_hbm,
                 out_hbm, loss_out, gup_hbm, gdown_hbm,
                 tok_ref, lab_ref, misc_ref, n_ref, dx_ref, x_ref, dy_ref, up_ref, down_ref, gup_out, gdown_out,
                 head, acc, acc_lab, dx_wide, fix_rows, in_sem, grad_sem, head_sem, out_sem):
    vocab, dim = acc.shape
    n_micro, seq, _ = n_ref.shape
    logit_scale = dim ** -0.5
    rows, n_full, tail = chunks(vocab, OUT_ROWS)

    def head_copy(first, height, index):
        return pltpu.make_async_copy(head_hbm.at[pl.ds(first, height), :], head.at[pl.ds(first, height), :], head_sem.at[index])

    def out_copy(first, height, index):
        return pltpu.make_async_copy(acc.at[pl.ds(first, height), :], out_hbm.at[pl.ds(first, height), :], out_sem.at[index])

    def each(body):
        def one(i, carry):
            body(pl.multiple_of(i * rows, rows), rows, i)
            return carry
        lax.fori_loop(0, n_full, one, 0)
        if tail:
            body(n_full * rows, tail, n_full)

    loads = [pltpu.make_async_copy(src, dst, in_sem.at[i]) for i, (src, dst) in enumerate((
        (tok_hbm, tok_ref), (lab_hbm, lab_ref), (misc_hbm, misc_ref), (n_hbm, n_ref), (dx_hbm, dx_ref),
        (x_hbm, x_ref), (dy_hbm, dy_ref), (up_hbm.at[0], up_ref), (down_hbm.at[0], down_ref)))]
    for load in loads[:5]:
        load.start()
    each(lambda *where: head_copy(*where).start())
    for load in loads[5:]:
        load.start()

    def clear(first, height, index):
        acc[pl.ds(first, height), :] = jnp.zeros((height, dim), F32)
        acc_lab[pl.ds(first, height), :] = jnp.zeros((height, dim), F32)

    each(clear)
    for load in loads[:5]:
        load.wait()

    eye = lax.broadcasted_iota(jnp.int32, (seq, LANES), 0) == lax.broadcasted_iota(jnp.int32, (seq, LANES), 1)
    total = jnp.zeros((8, LANES), F32)
    for m in range(n_micro):
        misc = misc_ref[m]
        total = total + misc
        fix = jnp.sum(jnp.where(eye, misc[1:2, :], 0.0), axis=-1, keepdims=True) * logit_scale
        fix_rows[pl.ds(m * seq, seq), :] = n_ref[m].astype(F32) * fix
        dx_wide[pl.ds(m * seq, seq), :] = dx_ref[m].astype(F32)
    loss_out[0] = jnp.max(total[2:3, :])

    def scatter(m, carry):
        for i in range(seq):
            acc[pl.ds(tok_ref[m, i], 1), :] += dx_wide[pl.ds(m * seq + i, 1), :]
            acc_lab[pl.ds(lab_ref[m, i], 1), :] += fix_rows[pl.ds(m * seq + i, 1), :]
        return carry

    lax.fori_loop(0, n_micro, scatter, 0)

    def join(first, height, index):
        head_copy(first, height, index).wait()
        where = pl.ds(first, height)
        acc[where, :] = head[where, :] + (acc[where, :] + acc_lab[where, :])
        out_copy(first, height, index).start()

    each(join)

    for load in loads[5:]:
        load.wait()
    up, down = up_ref[...], down_ref[...]
    gup_out[...] = jnp.zeros_like(gup_out)
    gdown_out[...] = jnp.zeros_like(gdown_out)
    group = max(1, 256 // seq)

    def wgrad(i, carry):
        x_act = x_ref[pl.ds(i * group, group)].reshape(group * seq, dim)
        grad_out = dy_ref[pl.ds(i * group, group)].reshape(group * seq, dim)
        pre = dot_nn(x_act, up).astype(BF16).astype(F32)
        hidden = gelu(pre).astype(BF16)
        gdown_out[...] += dot_tn(hidden, grad_out)
        grad_hidden = dot_nt(grad_out, down).astype(BF16).astype(F32)
        grad_pre = (grad_hidden * gelu_grad(pre)).astype(BF16)
        gup_out[...] += dot_tn(x_act, grad_pre)
        return carry

    lax.fori_loop(0, n_micro // group, wgrad, 0)
    grads = [pltpu.make_async_copy(gup_out, gup_hbm, grad_sem.at[0]), pltpu.make_async_copy(gdown_out, gdown_hbm, grad_sem.at[1])]
    for grad in grads:
        grad.start()
    for grad in grads:
        grad.wait()
    each(lambda *where: out_copy(*where).wait())


def solution(mesh):
    n_stage = mesh.shape["stage"]

    def device_fn(tokens, labels, emb_table, w_up, w_down):
        n_micro, seq = tokens.shape
        vocab, dim = emb_table.shape
        ffn = w_up.shape[2]
        count = n_micro * seq
        inv_count = 1.0 / count
        vmem = pl.BlockSpec(memory_space=pltpu.VMEM)
        smem = pl.BlockSpec(memory_space=pltpu.SMEM)
        hbm = pl.BlockSpec(memory_space=pl.ANY)
        dma = pltpu.SemaphoreType.DMA

        n_parts = -(-vocab // (2 * TABLE_ROWS))
        act = jax.ShapeDtypeStruct((n_stage, seq, dim), BF16)
        n_all, dx_all, x_all, dy_all, misc, head = pl.pallas_call(
            functools.partial(step_kernel, n_stage, inv_count),
            name="step",
            out_shape=(act, act, act, act, jax.ShapeDtypeStruct((n_stage, 8, LANES), F32), jax.ShapeDtypeStruct((vocab, dim), F32)),
            in_specs=[hbm] * 5,
            out_specs=(hbm,) * 6,
            scratch_shapes=[
                pltpu.SMEM((n_micro, seq), jnp.int32),
                pltpu.VMEM((n_micro, seq), jnp.int32),
                pltpu.VMEM((vocab // TILE, TILE, dim), BF16),
                pltpu.VMEM((n_stage, dim, ffn), BF16),
                pltpu.VMEM((n_stage, ffn, dim), BF16),
                pltpu.VMEM((n_stage, seq, dim), BF16),
                pltpu.VMEM((n_stage, seq, ffn), BF16),
                pltpu.VMEM((n_stage, seq, dim), BF16),
                pltpu.VMEM((seq, vocab), BF16),
                pltpu.VMEM((seq, dim), BF16),
                pltpu.VMEM((8, LANES), F32),
                pltpu.VMEM((seq, dim), BF16),
                pltpu.VMEM((seq, dim), F32),
                pltpu.VMEM((8, count), F32),
                pltpu.VMEM((vocab // 2, dim), F32),
                pltpu.VMEM((n_stage, seq, dim), BF16),
                pltpu.VMEM((n_stage, 8, LANES), F32),
                pltpu.VMEM((n_stage, seq, dim), BF16),
                pltpu.VMEM((n_stage, seq, dim), BF16),
                pltpu.VMEM((n_stage, seq, dim), BF16),
                dma((4,)), dma((5,)), dma, dma((n_stage,)), dma((n_stage,)), dma((3, n_stage)), dma((3, n_stage)),
                dma((n_stage,)), dma((n_stage,)), dma((n_stage,)), dma((n_stage,)), dma((n_stage,)),
                dma((n_stage,)), dma((n_stage,)), dma((n_stage,)), dma((n_stage,)), dma((n_stage,)),
                dma((n_parts,)), dma((n_parts,)), dma((n_parts,)),
            ],
            compiler_params=pltpu.CompilerParams(collective_id=0, has_side_effects=True),
        )(tokens, labels, emb_table.reshape(vocab // TILE, TILE, dim), w_up, w_down)

        n_outs = -(-vocab // OUT_ROWS)
        grad_emb, loss, g_up, g_down = pl.pallas_call(
            table_kernel,
            name="table_grad",
            out_shape=(
                jax.ShapeDtypeStruct((vocab, dim), F32),
                jax.ShapeDtypeStruct((1,), F32),
                jax.ShapeDtypeStruct((dim, ffn), F32),
                jax.ShapeDtypeStruct((ffn, dim), F32),
            ),
            in_specs=[hbm] * 10,
            out_specs=(hbm, smem, hbm, hbm),
            scratch_shapes=[
                pltpu.SMEM((n_micro, seq), jnp.int32),
                pltpu.SMEM((n_micro, seq), jnp.int32),
                pltpu.VMEM((n_stage, 8, LANES), F32),
                pltpu.VMEM((n_stage, seq, dim), BF16),
                pltpu.VMEM((n_stage, seq, dim), BF16),
                pltpu.VMEM((n_stage, seq, dim), BF16),
                pltpu.VMEM((n_stage, seq, dim), BF16),
                pltpu.VMEM((dim, ffn), BF16),
                pltpu.VMEM((ffn, dim), BF16),
                pltpu.VMEM((dim, ffn), F32),
                pltpu.VMEM((ffn, dim), F32),
                pltpu.VMEM((vocab, dim), F32),
                pltpu.VMEM((vocab, dim), F32),
                pltpu.VMEM((vocab, dim), F32),
                pltpu.VMEM((count, dim), F32),
                pltpu.VMEM((count, dim), F32),
                dma((9,)), dma((2,)), dma((n_outs,)), dma((n_outs,)),
            ],
        )(tokens, labels, misc, n_all, dx_all, x_all, dy_all, w_up, w_down, head)
        return loss, g_up[None], g_down[None], grad_emb

    return jax.shard_map(device_fn, mesh=mesh, in_specs=(P("dp", None), P("dp", None), P(None, None), P("stage", None, None), P("stage", None, None)), out_specs=(P("dp"), P(("dp", "stage"), None, None), P(("dp", "stage"), None, None), P("dp", None)), check_vma=False)
```

```python
import functools
import math

import jax
import jax.numpy as jnp
from jax import lax
from jax.experimental import pallas as pl
from jax.experimental.pallas import tpu as pltpu
from jax.sharding import PartitionSpec as P

F32 = jnp.float32
BF16 = jnp.bfloat16
MESH = pl.DeviceIdType.MESH
LANES = 128
TILE = 16
HEAD_COLS = 4096
TABLE_ROWS = 2048
OUT_ROWS = 2048
GELU_C = math.sqrt(2.0 / math.pi)
GELU_K = 0.044715
RMS_EPS = 1e-6


def dot_nn(a, b):
    return lax.dot_general(a, b, (((1,), (0,)), ((), ())), preferred_element_type=F32)


def dot_nt(a, b):
    return lax.dot_general(a, b, (((1,), (1,)), ((), ())), preferred_element_type=F32)


def dot_tn(a, b):
    return lax.dot_general(a, b, (((0,), (0,)), ((), ())), preferred_element_type=F32)


def gelu(a):
    return a * (0.5 * (1.0 + jnp.tanh(GELU_C * (a + GELU_K * (a * a * a)))))


def gelu_grad(a):
    sq = a * a
    t = jnp.tanh(GELU_C * (a + GELU_K * (sq * a)))
    return 0.5 * (1.0 + t) + (0.5 * GELU_C) * a * (1.0 - t * t) * (1.0 + (3.0 * GELU_K) * sq)


def chunks(total, size):
    return size, total // size, total % size


def step_kernel(n_stage, n_dp, inv_count, tok_hbm, lab_hbm, table_hbm, w_up_hbm, w_down_hbm,
                n_out, dx_out, x_out, dy_out, misc_out, head_hbm,
                tok_ref, lab_ref, table, up_all, down_all, x_hist, pre_hist, dy_hist, logits,
                n_mine, misc_mine, dx_mine, x_rows, lse_row, head_part, n_all, misc_all, dx_all, x_all, dy_all,
                in_sem, out_sem, table_sem, up_recv, down_recv, up_send, down_send, side_recv, side_send,
                x_recv, dy_recv, n_recv, misc_recv, dx_recv,
                x_send, dy_send, n_send, misc_send, dx_send, keep_sem, part_send, part_recv):
    me = lax.axis_index("stage")
    dp = lax.axis_index("dp")
    n_chip = n_stage // 2
    half = n_chip // 2
    chip, core = me // 2, lax.rem(me, 2)
    dim = table.shape[2]
    vocab = table.shape[0] * TILE
    seq = x_hist.shape[1]
    logit_scale = dim ** -0.5

    def slot_at(offset, which):
        return lax.rem(chip + offset + n_chip, n_chip) * 2 + which

    right, left, partner = slot_at(1, core), slot_at(-1, core), chip * 2 + (1 - core)

    loads = [
        pltpu.make_async_copy(w_up_hbm.at[0], up_all.at[me], in_sem.at[0]),
        pltpu.make_async_copy(w_down_hbm.at[0], down_all.at[me], in_sem.at[1]),
        pltpu.make_async_copy(tok_hbm, tok_ref, in_sem.at[2]),
        pltpu.make_async_copy(lab_hbm, lab_ref, in_sem.at[3]),
    ]
    for load in loads:
        load.start()
    table_copy = pltpu.make_async_copy(table_hbm, table, table_sem)
    table_copy.start()

    barrier = pltpu.get_barrier_semaphore()

    def greet(k, carry):
        pl.semaphore_signal(barrier, inc=1, device_id=(dp, lax.rem(me + k, n_stage)), device_id_type=MESH)
        return carry

    lax.fori_loop(1, n_stage, greet, 0)
    paired = n_dp % 2 == 0
    side = dp + 1 - 2 * lax.rem(dp, 2)
    if paired:
        pl.semaphore_signal(barrier, inc=1, device_id=(side, me), device_id_type=MESH)
    pl.semaphore_wait(barrier, n_stage if paired else n_stage - 1)
    for load in loads:
        load.wait()

    parity = lax.rem(dp, 2)
    up_rows, down_rows = up_all.shape[1], down_all.shape[1]

    def up_part(kind):
        left_out = up_rows // 64 * 16
        if kind == "whole" or not paired:
            return pl.ds(0, up_rows)
        if kind == "ring":
            return pl.ds(pl.multiple_of(parity * left_out, 16), up_rows - left_out)
        mine = parity if kind == "give" else 1 - parity
        return pl.ds(pl.multiple_of(mine * (up_rows - left_out), 16), left_out)

    def down_part(kind):
        left_out = down_rows * 5 // 256 * 16
        if kind == "whole" or not paired:
            return pl.ds(0, down_rows)
        if kind == "ring":
            return pl.ds(pl.multiple_of(parity * left_out, 16), down_rows - left_out)
        mine = parity if kind == "give" else 1 - parity
        return pl.ds(pl.multiple_of(mine * (down_rows - left_out), 16), left_out)

    def up_copy(slot, way, target, kind):
        ref = up_all.at[slot, up_part(kind)]
        return pltpu.make_async_remote_copy(
            src_ref=ref, dst_ref=ref, send_sem=up_send.at[way, slot], recv_sem=up_recv.at[slot],
            device_id=(dp, target), device_id_type=MESH)

    def down_copy(slot, way, target, kind):
        ref = down_all.at[slot, down_part(kind)]
        return pltpu.make_async_remote_copy(
            src_ref=ref, dst_ref=ref, send_sem=down_send.at[way, slot], recv_sem=down_recv.at[slot],
            device_id=(dp, target), device_id_type=MESH)

    def side_copy(which, slot, kind):
        ref = up_all.at[slot, up_part(kind)] if which == 0 else down_all.at[slot, down_part(kind)]
        give = kind == "give"
        return pltpu.make_async_remote_copy(
            src_ref=ref, dst_ref=ref, send_sem=side_send.at[0 if give else 1, which, slot], recv_sem=side_recv.at[which, slot],
            device_id=(side, me) if give else (dp, partner), device_id_type=MESH)

    sends = []

    def send(copy):
        copy.start()
        sends.append(copy)

    for way, target, kind in ((0, right, "ring"), (1, left, "ring"), (2, partner, "whole")):
        send(up_copy(me, way, target, kind))
        send(down_copy(me, way, target, kind))

    table_copy.wait()
    row_iota = lax.broadcasted_iota(jnp.int32, (TILE, dim), 0)

    def embed(i, carry):
        tok = tok_ref[me, i]
        tile = table[lax.div(tok, TILE)].astype(F32)
        row = jnp.sum(jnp.where(row_iota == lax.rem(tok, TILE), tile, 0.0), axis=0, keepdims=True)
        x_rows[pl.ds(i, 1), :] = row
        return carry

    lax.fori_loop(0, seq, embed, 0)
    x_now = x_rows[...].astype(BF16)

    def arrived(copy, which, slot, forward):
        copy.wait_recv()
        if forward is not None:
            send(forward)
        if paired:
            send(side_copy(which, slot, "give"))

    for t in range(1, half + 1):
        slot_l, slot_r = slot_at(-t, core), slot_at(t, core)
        whole, onward = t < half, t < half - 1
        up_l, down_r = up_copy(slot_l, 0, right, "ring"), down_copy(slot_r, 1, left, "ring")
        arrived(up_l, 0, slot_l, up_l if whole else None)
        arrived(down_r, 1, slot_r, down_r if whole else None)
        if whole:
            down_l, up_r = down_copy(slot_l, 0, right, "ring"), up_copy(slot_r, 1, left, "ring")
            arrived(down_l, 1, slot_l, down_l if onward else None)
            arrived(up_r, 0, slot_r, up_r if onward else None)
            send(down_copy(slot_l, 2, partner, "ring"))
            send(up_copy(slot_r, 2, partner, "ring"))
        send(up_copy(slot_l, 2, partner, "ring"))
        send(down_copy(slot_r, 2, partner, "ring"))

    if paired:
        for t in [d for k in range(1, half) for d in (-k, k)] + [half]:
            for which in (0, 1):
                taken = side_copy(which, slot_at(t, core), "take")
                taken.wait_recv()
                send(taken)

    for t in range(n_chip):
        slot = slot_at(t, 1 - core)
        kind = "whole" if t == 0 else "ring"
        up_copy(slot, 2, partner, kind).wait_recv()
        down_copy(slot, 2, partner, kind).wait_recv()
        if paired and t > 0:
            side_copy(0, slot, "take").wait_recv()
            side_copy(1, slot, "take").wait_recv()

    def forward(s, x_act):
        x_hist[s] = x_act
        pre = dot_nn(x_act, up_all[s]).astype(BF16)
        pre_hist[s] = pre
        hidden = gelu(pre.astype(F32)).astype(BF16)
        return (x_act.astype(F32) + dot_nn(hidden, down_all[s])).astype(BF16)

    x_last = lax.fori_loop(0, n_stage, forward, x_now)

    def peer_copy(src, dst, send_sem, recv_sem, target):
        return pltpu.make_async_remote_copy(
            src_ref=src, dst_ref=dst.at[me], send_sem=send_sem.at[target], recv_sem=recv_sem.at[me],
            device_id=(dp, target), device_id_type=MESH)

    def x_copy(target):
        return peer_copy(x_hist.at[target], x_all, x_send, x_recv, target)

    def dy_copy(target):
        return peer_copy(dy_hist.at[target], dy_all, dy_send, dy_recv, target)

    def n_copy(target):
        return peer_copy(n_mine, n_all, n_send, n_recv, target)

    def misc_copy(target):
        return peer_copy(misc_mine, misc_all, misc_send, misc_recv, target)

    def dx_copy(target):
        return peer_copy(dx_mine, dx_all, dx_send, dx_recv, target)

    def to_peers(start):
        def one(k, carry):
            start(lax.rem(me + k, n_stage))
            return carry
        lax.fori_loop(1, n_stage, one, 0)

    def wait_from(buf, recv):
        def one(k, carry):
            source = lax.rem(me + k, n_stage)
            pltpu.make_async_remote_copy(
                src_ref=buf.at[source], dst_ref=buf.at[source], send_sem=dx_send.at[source], recv_sem=recv.at[source],
                device_id=(dp, source), device_id_type=MESH).wait_recv()
            return carry
        lax.fori_loop(1, n_stage, one, 0)

    x_wide = x_last.astype(F32)
    inv_rms = lax.rsqrt(jnp.mean(x_wide * x_wide, axis=-1, keepdims=True) + RMS_EPS)
    normed = (x_wide * inv_rms).astype(BF16)
    n_mine[...] = normed
    n_all[me] = normed
    to_peers(lambda target: x_copy(target).start())
    x_all[me] = x_hist[me]
    to_peers(lambda target: n_copy(target).start())

    cols, n_full, tail = chunks(vocab, HEAD_COLS)

    def table_rows(first, width):
        tile = first // TILE if isinstance(first, int) else lax.div(first, TILE)
        return table[pl.ds(tile, width // TILE)].reshape(width, dim)

    def pass_one(first, width, carry):
        top, total = carry
        z = (dot_nt(normed, table_rows(first, width)) * logit_scale).astype(BF16)
        logits[:, pl.ds(first, width)] = z
        parts = [z[:, j:j + LANES].astype(F32) for j in range(0, width, LANES)]
        new_top = top
        for part in parts:
            new_top = jnp.maximum(new_top, part)
        total = total * jnp.exp(top - new_top)
        for part in parts:
            total = total + jnp.exp(part - new_top)
        return new_top, total

    def head_loop(body, carry):
        carry = lax.fori_loop(0, n_full, lambda i, c: body(pl.multiple_of(i * cols, cols), cols, c), carry)
        if tail:
            carry = body(n_full * cols, tail, carry)
        return carry

    top, total = head_loop(pass_one, (jnp.full((seq, LANES), -1e30, F32), jnp.zeros((seq, LANES), F32)))
    row_top = jnp.max(top, axis=-1, keepdims=True)
    row_sum = jnp.sum(total * jnp.exp(top - row_top), axis=-1, keepdims=True)
    lse = row_top + jnp.log(row_sum)

    lane_iota = lax.broadcasted_iota(jnp.int32, (seq, LANES), 1)
    lane_wide = lane_iota.astype(F32)
    square = lax.broadcasted_iota(jnp.int32, (seq, seq), 0) == lax.broadcasted_iota(jnp.int32, (seq, seq), 1)
    label = jnp.sum(jnp.where(square, lab_ref[pl.ds(me, 1), :].astype(F32), 0.0), axis=-1, keepdims=True)
    lse_count = lse + math.log(1.0 / inv_count)

    def pass_two(first, width, carry):
        picked, grad_n = carry
        base = label - jnp.asarray(first, jnp.int32).astype(F32)
        grads = []
        for j in range(0, width, LANES):
            z = logits[:, pl.ds(first + j, LANES)].astype(F32)
            prob = jnp.exp(z - lse_count)
            hit = lane_wide == base - float(j)
            picked = picked + jnp.where(hit, z, 0.0)
            grads.append(jnp.where(hit, prob - inv_count, prob).astype(BF16))
        grad_z = jnp.concatenate(grads, axis=1)
        return picked, grad_n + dot_nn(grad_z, table_rows(first, width))

    picked, grad_n = head_loop(pass_two, (jnp.zeros((seq, LANES), F32), jnp.zeros((seq, dim), F32)))
    picked = jnp.sum(picked, axis=-1, keepdims=True)
    loss = jnp.sum((lse - picked) * inv_count)
    label_prob = jnp.exp(picked - lse_count)
    fix = (label_prob - inv_count).astype(BF16).astype(F32) - label_prob.astype(BF16).astype(F32)
    eye = lax.broadcasted_iota(jnp.int32, (seq, LANES), 0) == lane_iota

    def as_row(column):
        return jnp.broadcast_to(jnp.sum(jnp.where(eye, column, 0.0), axis=0, keepdims=True), (8, LANES))

    row8 = lax.broadcasted_iota(jnp.int32, (8, LANES), 0)
    misc = jnp.where(row8 == 0, as_row(lse_count), jnp.where(row8 == 1, as_row(fix), loss))
    misc_mine[...] = misc
    misc_all[me] = misc

    grad_n = (grad_n * logit_scale).astype(BF16).astype(F32)
    along = jnp.mean(grad_n * x_wide, axis=-1, keepdims=True)
    grad_x = (inv_rms * grad_n - x_wide * (inv_rms * inv_rms * inv_rms * along)).astype(BF16)

    to_peers(lambda target: misc_copy(target).start())

    def backward(k, grad_out):
        s = n_stage - 1 - k
        dy_hist[s] = grad_out
        grad_hidden = dot_nt(grad_out, down_all[s]).astype(BF16).astype(F32)
        grad_pre = (grad_hidden * gelu_grad(pre_hist[s].astype(F32))).astype(BF16)
        result = (grad_out.astype(F32) + dot_nt(grad_pre, up_all[s])).astype(BF16)

        @pl.when(s != me)
        def _():
            dy_copy(s).start()

        return result

    grad_in = lax.fori_loop(0, n_stage, backward, grad_x)
    dx_mine[...] = grad_in
    dy_all[me] = dy_hist[me]
    dx_all[me] = grad_in

    wait_from(n_all, n_recv)
    wait_from(misc_all, misc_recv)
    per_row = LANES // seq
    for m in range(0, n_stage, per_row):
        row = misc_all[m]
        for k in range(1, per_row):
            row = row + pltpu.roll(misc_all[m + k], k * seq, 1)
        lse_row[:, pl.ds(m * seq, LANES)] = row
    to_peers(lambda target: dx_copy(target).start())
    results = [pltpu.make_async_copy(src, dst, out_sem.at[i]) for i, (src, dst) in enumerate(
        ((n_all, n_out), (misc_all, misc_out), (x_all, x_out), (dy_all, dy_out), (dx_all, dx_out)))]
    results[0].start()
    results[1].start()

    half_rows = vocab // 2
    rows, n_full, tail = chunks(half_rows, TABLE_ROWS)
    count = n_stage * seq

    def keep_copy(first, height, index):
        return pltpu.make_async_copy(
            head_part.at[pl.ds(first, height), :], head_hbm.at[pl.ds(core * half_rows + first, height), :], keep_sem.at[index])

    def part_copy(first, height, index, owner):
        return pltpu.make_async_remote_copy(
            src_ref=head_part.at[pl.ds(first, height), :],
            dst_ref=head_hbm.at[pl.ds(owner * half_rows + first, height), :],
            send_sem=part_send.at[index], recv_sem=part_recv.at[index],
            device_id=(dp, partner), device_id_type=MESH)

    def pass_on(first, height, index):
        keep_copy(first, height, index).start()
        part_copy(first, height, index, core).start()

    def head_rows(first, height):
        every = n_all[...].reshape(count, dim)
        tile = lax.div(core * half_rows + first, TILE)
        z = (dot_nt(table[pl.ds(tile, height // TILE)].reshape(height, dim), every) * logit_scale).astype(BF16).astype(F32)
        grad_z = jnp.exp(z - lse_row[0:1, :]).astype(BF16)
        head_part[pl.ds(first, height), :] = dot_nn(grad_z, every) * logit_scale

    def head_chunk(i, carry):
        @pl.when(i > 0)
        def _():
            pass_on(pl.multiple_of((i - 1) * rows, TILE), rows, i - 1)

        head_rows(pl.multiple_of(i * rows, rows), rows)
        return carry

    lax.fori_loop(0, n_full, head_chunk, 0)
    pass_on((n_full - 1) * rows, rows, n_full - 1)
    wait_from(x_all, x_recv)
    wait_from(dy_all, dy_recv)
    wait_from(dx_all, dx_recv)
    for result in results[2:]:
        result.start()
    if tail:
        head_rows(n_full * rows, tail)
    to_peers(lambda target: x_copy(target).wait_send())
    for copy in sends:
        copy.wait_send()
    if tail:
        pass_on(n_full * rows, tail, n_full)
    for make in (dy_copy, n_copy, misc_copy, dx_copy):
        to_peers(lambda target, make=make: make(target).wait_send())
    for result in results:
        result.wait()

    def finish(first, height, index):
        keep_copy(first, height, index).wait()
        part_copy(first, height, index, core).wait_send()
        part_copy(first, height, index, 1 - core).wait_recv()

    def finish_chunk(i, carry):
        finish(pl.multiple_of(i * rows, rows), rows, i)
        return carry

    lax.fori_loop(0, n_full, finish_chunk, 0)
    if tail:
        finish(n_full * rows, tail, n_full)


def table_kernel(tok_hbm, lab_hbm, misc_hbm, n_hbm, dx_hbm, x_hbm, dy_hbm, up_hbm, down_hbm, head_hbm,
                 out_hbm, loss_out, gup_hbm, gdown_hbm,
                 tok_ref, lab_ref, misc_ref, n_ref, dx_ref, x_ref, dy_ref, up_ref, down_ref, gup_out, gdown_out,
                 head, acc, acc_lab, dx_wide, fix_rows, in_sem, grad_sem, head_sem, out_sem):
    vocab, dim = acc.shape
    n_micro, seq, _ = n_ref.shape
    logit_scale = dim ** -0.5
    rows, n_full, tail = chunks(vocab, OUT_ROWS)

    def head_copy(first, height, index):
        return pltpu.make_async_copy(head_hbm.at[pl.ds(first, height), :], head.at[pl.ds(first, height), :], head_sem.at[index])

    def out_copy(first, height, index):
        return pltpu.make_async_copy(acc.at[pl.ds(first, height), :], out_hbm.at[pl.ds(first, height), :], out_sem.at[index])

    def each(body):
        def one(i, carry):
            body(pl.multiple_of(i * rows, rows), rows, i)
            return carry
        lax.fori_loop(0, n_full, one, 0)
        if tail:
            body(n_full * rows, tail, n_full)

    loads = [pltpu.make_async_copy(src, dst, in_sem.at[i]) for i, (src, dst) in enumerate((
        (tok_hbm, tok_ref), (lab_hbm, lab_ref), (misc_hbm, misc_ref), (n_hbm, n_ref), (dx_hbm, dx_ref),
        (x_hbm, x_ref), (dy_hbm, dy_ref), (up_hbm.at[0], up_ref), (down_hbm.at[0], down_ref)))]
    for load in loads[:5]:
        load.start()
    each(lambda *where: head_copy(*where).start())
    for load in loads[5:]:
        load.start()

    def clear(first, height, index):
        acc[pl.ds(first, height), :] = jnp.zeros((height, dim), F32)
        acc_lab[pl.ds(first, height), :] = jnp.zeros((height, dim), F32)

    each(clear)
    for load in loads[:5]:
        load.wait()

    eye = lax.broadcasted_iota(jnp.int32, (seq, LANES), 0) == lax.broadcasted_iota(jnp.int32, (seq, LANES), 1)
    total = jnp.zeros((8, LANES), F32)
    for m in range(n_micro):
        misc = misc_ref[m]
        total = total + misc
        fix = jnp.sum(jnp.where(eye, misc[1:2, :], 0.0), axis=-1, keepdims=True) * logit_scale
        fix_rows[pl.ds(m * seq, seq), :] = n_ref[m].astype(F32) * fix
        dx_wide[pl.ds(m * seq, seq), :] = dx_ref[m].astype(F32)
    loss_out[0] = jnp.max(total[2:3, :])

    def scatter(m, carry):
        for i in range(seq):
            acc[pl.ds(tok_ref[m, i], 1), :] += dx_wide[pl.ds(m * seq + i, 1), :]
            acc_lab[pl.ds(lab_ref[m, i], 1), :] += fix_rows[pl.ds(m * seq + i, 1), :]
        return carry

    lax.fori_loop(0, n_micro, scatter, 0)

    def join(first, height, index):
        head_copy(first, height, index).wait()
        where = pl.ds(first, height)
        acc[where, :] = head[where, :] + (acc[where, :] + acc_lab[where, :])
        out_copy(first, height, index).start()

    each(join)

    for load in loads[5:]:
        load.wait()
    up, down = up_ref[...], down_ref[...]
    gup_out[...] = jnp.zeros_like(gup_out)
    gdown_out[...] = jnp.zeros_like(gdown_out)
    group = max(1, 256 // seq)

    def wgrad(i, carry):
        x_act = x_ref[pl.ds(i * group, group)].reshape(group * seq, dim)
        grad_out = dy_ref[pl.ds(i * group, group)].reshape(group * seq, dim)
        pre = dot_nn(x_act, up).astype(BF16).astype(F32)
        hidden = gelu(pre).astype(BF16)
        gdown_out[...] += dot_tn(hidden, grad_out)
        grad_hidden = dot_nt(grad_out, down).astype(BF16).astype(F32)
        grad_pre = (grad_hidden * gelu_grad(pre)).astype(BF16)
        gup_out[...] += dot_tn(x_act, grad_pre)
        return carry

    lax.fori_loop(0, n_micro // group, wgrad, 0)
    grads = [pltpu.make_async_copy(gup_out, gup_hbm, grad_sem.at[0]), pltpu.make_async_copy(gdown_out, gdown_hbm, grad_sem.at[1])]
    for grad in grads:
        grad.start()
    for grad in grads:
        grad.wait()
    each(lambda *where: out_copy(*where).wait())


def solution(mesh):
    n_stage = mesh.shape["stage"]

    def device_fn(tokens, labels, emb_table, w_up, w_down):
        n_micro, seq = tokens.shape
        vocab, dim = emb_table.shape
        ffn = w_up.shape[2]
        count = n_micro * seq
        inv_count = 1.0 / count
        vmem = pl.BlockSpec(memory_space=pltpu.VMEM)
        smem = pl.BlockSpec(memory_space=pltpu.SMEM)
        hbm = pl.BlockSpec(memory_space=pl.ANY)
        dma = pltpu.SemaphoreType.DMA

        n_parts = -(-vocab // (2 * TABLE_ROWS))
        act = jax.ShapeDtypeStruct((n_stage, seq, dim), BF16)
        n_all, dx_all, x_all, dy_all, misc, head = pl.pallas_call(
            functools.partial(step_kernel, n_stage, mesh.shape["dp"], inv_count),
            name="step",
            out_shape=(act, act, act, act, jax.ShapeDtypeStruct((n_stage, 8, LANES), F32), jax.ShapeDtypeStruct((vocab, dim), F32)),
            in_specs=[hbm] * 5,
            out_specs=(hbm,) * 6,
            scratch_shapes=[
                pltpu.SMEM((n_micro, seq), jnp.int32),
                pltpu.VMEM((n_micro, seq), jnp.int32),
                pltpu.VMEM((vocab // TILE, TILE, dim), BF16),
                pltpu.VMEM((n_stage, dim, ffn), BF16),
                pltpu.VMEM((n_stage, ffn, dim), BF16),
                pltpu.VMEM((n_stage, seq, dim), BF16),
                pltpu.VMEM((n_stage, seq, ffn), BF16),
                pltpu.VMEM((n_stage, seq, dim), BF16),
                pltpu.VMEM((seq, vocab), BF16),
                pltpu.VMEM((seq, dim), BF16),
                pltpu.VMEM((8, LANES), F32),
                pltpu.VMEM((seq, dim), BF16),
                pltpu.VMEM((seq, dim), F32),
                pltpu.VMEM((8, count), F32),
                pltpu.VMEM((vocab // 2, dim), F32),
                pltpu.VMEM((n_stage, seq, dim), BF16),
                pltpu.VMEM((n_stage, 8, LANES), F32),
                pltpu.VMEM((n_stage, seq, dim), BF16),
                pltpu.VMEM((n_stage, seq, dim), BF16),
                pltpu.VMEM((n_stage, seq, dim), BF16),
                dma((4,)), dma((5,)), dma, dma((n_stage,)), dma((n_stage,)), dma((3, n_stage)), dma((3, n_stage)),
                dma((2, n_stage)), dma((2, 2, n_stage)),
                dma((n_stage,)), dma((n_stage,)), dma((n_stage,)), dma((n_stage,)), dma((n_stage,)),
                dma((n_stage,)), dma((n_stage,)), dma((n_stage,)), dma((n_stage,)), dma((n_stage,)),
                dma((n_parts,)), dma((n_parts,)), dma((n_parts,)),
            ],
            compiler_params=pltpu.CompilerParams(collective_id=0, has_side_effects=True),
        )(tokens, labels, emb_table.reshape(vocab // TILE, TILE, dim), w_up, w_down)

        n_outs = -(-vocab // OUT_ROWS)
        grad_emb, loss, g_up, g_down = pl.pallas_call(
            table_kernel,
            name="table_grad",
            out_shape=(
                jax.ShapeDtypeStruct((vocab, dim), F32),
                jax.ShapeDtypeStruct((1,), F32),
                jax.ShapeDtypeStruct((dim, ffn), F32),
                jax.ShapeDtypeStruct((ffn, dim), F32),
            ),
            in_specs=[hbm] * 10,
            out_specs=(hbm, smem, hbm, hbm),
            scratch_shapes=[
                pltpu.SMEM((n_micro, seq), jnp.int32),
                pltpu.SMEM((n_micro, seq), jnp.int32),
                pltpu.VMEM((n_stage, 8, LANES), F32),
                pltpu.VMEM((n_stage, seq, dim), BF16),
                pltpu.VMEM((n_stage, seq, dim), BF16),
                pltpu.VMEM((n_stage, seq, dim), BF16),
                pltpu.VMEM((n_stage, seq, dim), BF16),
                pltpu.VMEM((dim, ffn), BF16),
                pltpu.VMEM((ffn, dim), BF16),
                pltpu.VMEM((dim, ffn), F32),
                pltpu.VMEM((ffn, dim), F32),
                pltpu.VMEM((vocab, dim), F32),
                pltpu.VMEM((vocab, dim), F32),
                pltpu.VMEM((vocab, dim), F32),
                pltpu.VMEM((count, dim), F32),
                pltpu.VMEM((count, dim), F32),
                dma((9,)), dma((2,)), dma((n_outs,)), dma((n_outs,)),
            ],
        )(tokens, labels, misc, n_all, dx_all, x_all, dy_all, w_up, w_down, head)
        return loss, g_up[None], g_down[None], grad_emb

    return jax.shard_map(device_fn, mesh=mesh, in_specs=(P("dp", None), P("dp", None), P(None, None), P("stage", None, None), P("stage", None, None)), out_specs=(P("dp"), P(("dp", "stage"), None, None), P(("dp", "stage"), None, None), P("dp", None)), check_vma=False)
```

```python
import functools
import math

import jax
import jax.numpy as jnp
from jax import lax
from jax.experimental import pallas as pl
from jax.experimental.pallas import tpu as pltpu
from jax.sharding import PartitionSpec as P

F32 = jnp.float32
BF16 = jnp.bfloat16
MESH = pl.DeviceIdType.MESH
LANES = 128
TILE = 16
HEAD_COLS = 4096
TABLE_ROWS = 2048
OUT_ROWS = 2048
GELU_C = math.sqrt(2.0 / math.pi)
GELU_K = 0.044715
RMS_EPS = 1e-6


def dot_nn(a, b):
    return lax.dot_general(a, b, (((1,), (0,)), ((), ())), preferred_element_type=F32)


def dot_nt(a, b):
    return lax.dot_general(a, b, (((1,), (1,)), ((), ())), preferred_element_type=F32)


def dot_tn(a, b):
    return lax.dot_general(a, b, (((0,), (0,)), ((), ())), preferred_element_type=F32)


def gelu(a):
    return a * (0.5 * (1.0 + jnp.tanh(GELU_C * (a + GELU_K * (a * a * a)))))


def gelu_grad(a):
    sq = a * a
    t = jnp.tanh(GELU_C * (a + GELU_K * (sq * a)))
    return 0.5 * (1.0 + t) + (0.5 * GELU_C) * a * (1.0 - t * t) * (1.0 + (3.0 * GELU_K) * sq)


def chunks(total, size):
    return size, total // size, total % size


def step_kernel(n_stage, n_dp, inv_count, tok_hbm, lab_hbm, table_hbm, w_up_hbm, w_down_hbm,
                n_out, dx_out, x_out, dy_out, misc_out, head_hbm,
                tok_ref, lab_ref, table, up_all, down_all, x_hist, pre_hist, dy_hist, logits,
                n_mine, misc_mine, dx_mine, x_rows, lse_row, head_part, n_all, misc_all, dx_all, x_all, dy_all,
                in_sem, out_sem, table_sem, up_recv, down_recv, up_send, down_send, side_recv, side_send,
                x_recv, dy_recv, n_recv, misc_recv, dx_recv,
                x_send, dy_send, n_send, misc_send, dx_send, keep_sem, part_send, part_recv):
    me = lax.axis_index("stage")
    dp = lax.axis_index("dp")
    n_chip = n_stage // 2
    half = n_chip // 2
    chip, core = me // 2, lax.rem(me, 2)
    dim = table.shape[2]
    vocab = table.shape[0] * TILE
    seq = x_hist.shape[1]
    logit_scale = dim ** -0.5

    def slot_at(offset, which):
        return lax.rem(chip + offset + n_chip, n_chip) * 2 + which

    right, left, partner = slot_at(1, core), slot_at(-1, core), chip * 2 + (1 - core)

    loads = [
        pltpu.make_async_copy(w_up_hbm.at[0], up_all.at[me], in_sem.at[0]),
        pltpu.make_async_copy(w_down_hbm.at[0], down_all.at[me], in_sem.at[1]),
        pltpu.make_async_copy(tok_hbm, tok_ref, in_sem.at[2]),
        pltpu.make_async_copy(lab_hbm, lab_ref, in_sem.at[3]),
    ]
    for load in loads:
        load.start()
    table_copy = pltpu.make_async_copy(table_hbm, table, table_sem)
    table_copy.start()

    barrier = pltpu.get_barrier_semaphore()

    paired = n_dp % 2 == 0
    side = dp + 1 - 2 * lax.rem(dp, 2)
    greeted = [(dp, right), (dp, left), (dp, partner)] + ([(side, me)] if paired else [])
    for peer in greeted:
        pl.semaphore_signal(barrier, inc=1, device_id=peer, device_id_type=MESH)
    pl.semaphore_wait(barrier, len(greeted))
    for load in loads:
        load.wait()

    parity = lax.rem(dp, 2)
    up_rows, down_rows = up_all.shape[1], down_all.shape[1]

    def up_part(kind):
        left_out = up_rows // 64 * 16
        if kind == "whole" or not paired:
            return pl.ds(0, up_rows)
        if kind == "ring":
            return pl.ds(pl.multiple_of(parity * left_out, 16), up_rows - left_out)
        mine = parity if kind == "give" else 1 - parity
        return pl.ds(pl.multiple_of(mine * (up_rows - left_out), 16), left_out)

    def down_part(kind):
        left_out = down_rows * 5 // 256 * 16
        if kind == "whole" or not paired:
            return pl.ds(0, down_rows)
        if kind == "ring":
            return pl.ds(pl.multiple_of(parity * left_out, 16), down_rows - left_out)
        mine = parity if kind == "give" else 1 - parity
        return pl.ds(pl.multiple_of(mine * (down_rows - left_out), 16), left_out)

    def up_copy(slot, way, target, kind):
        ref = up_all.at[slot, up_part(kind)]
        return pltpu.make_async_remote_copy(
            src_ref=ref, dst_ref=ref, send_sem=up_send.at[way, slot], recv_sem=up_recv.at[slot],
            device_id=(dp, target), device_id_type=MESH)

    def down_copy(slot, way, target, kind):
        ref = down_all.at[slot, down_part(kind)]
        return pltpu.make_async_remote_copy(
            src_ref=ref, dst_ref=ref, send_sem=down_send.at[way, slot], recv_sem=down_recv.at[slot],
            device_id=(dp, target), device_id_type=MESH)

    def side_copy(which, slot, kind):
        ref = up_all.at[slot, up_part(kind)] if which == 0 else down_all.at[slot, down_part(kind)]
        give = kind == "give"
        return pltpu.make_async_remote_copy(
            src_ref=ref, dst_ref=ref, send_sem=side_send.at[0 if give else 1, which, slot], recv_sem=side_recv.at[which, slot],
            device_id=(side, me) if give else (dp, partner), device_id_type=MESH)

    sends = []

    def send(copy):
        copy.start()
        sends.append(copy)

    for way, target, kind in ((0, right, "ring"), (1, left, "ring"), (2, partner, "whole")):
        for copy in (down_copy, up_copy) if way == 1 else (up_copy, down_copy):
            send(copy(me, way, target, kind))

    table_copy.wait()
    row_iota = lax.broadcasted_iota(jnp.int32, (TILE, dim), 0)

    def embed(i, carry):
        tok = tok_ref[me, i]
        tile = table[lax.div(tok, TILE)].astype(F32)
        row = jnp.sum(jnp.where(row_iota == lax.rem(tok, TILE), tile, 0.0), axis=0, keepdims=True)
        x_rows[pl.ds(i, 1), :] = row
        return carry

    lax.fori_loop(0, seq, embed, 0)
    x_now = x_rows[...].astype(BF16)

    def arrived(copy, which, slot, forward):
        copy.wait_recv()
        if forward is not None:
            send(forward)
        if paired:
            send(side_copy(which, slot, "give"))

    for t in range(1, half + 1):
        slot_l, slot_r = slot_at(-t, core), slot_at(t, core)
        whole, onward = t < half, t < half - 1
        up_l, down_r = up_copy(slot_l, 0, right, "ring"), down_copy(slot_r, 1, left, "ring")
        arrived(up_l, 0, slot_l, up_l if whole else None)
        arrived(down_r, 1, slot_r, down_r if whole else None)
        if whole:
            down_l, up_r = down_copy(slot_l, 0, right, "ring"), up_copy(slot_r, 1, left, "ring")
            arrived(down_l, 1, slot_l, down_l if onward else None)
            arrived(up_r, 0, slot_r, up_r if onward else None)
            send(down_copy(slot_l, 2, partner, "ring"))
            send(up_copy(slot_r, 2, partner, "ring"))
        send(up_copy(slot_l, 2, partner, "ring"))
        send(down_copy(slot_r, 2, partner, "ring"))

    if paired:
        for t in [d for k in range(1, half) for d in (-k, k)] + [half]:
            for which in (0, 1):
                taken = side_copy(which, slot_at(t, core), "take")
                taken.wait_recv()
                send(taken)

    for t in range(n_chip):
        slot = slot_at(t, 1 - core)
        kind = "whole" if t == 0 else "ring"
        up_copy(slot, 2, partner, kind).wait_recv()
        down_copy(slot, 2, partner, kind).wait_recv()
        if paired and t > 0:
            side_copy(0, slot, "take").wait_recv()
            side_copy(1, slot, "take").wait_recv()

    def forward(s, x_act):
        x_hist[s] = x_act
        pre = dot_nn(x_act, up_all[s]).astype(BF16)
        pre_hist[s] = pre
        hidden = gelu(pre.astype(F32)).astype(BF16)
        return (x_act.astype(F32) + dot_nn(hidden, down_all[s])).astype(BF16)

    x_last = lax.fori_loop(0, n_stage, forward, x_now)

    def peer_copy(src, dst, send_sem, recv_sem, target):
        return pltpu.make_async_remote_copy(
            src_ref=src, dst_ref=dst.at[me], send_sem=send_sem.at[target], recv_sem=recv_sem.at[me],
            device_id=(dp, target), device_id_type=MESH)

    def x_copy(target):
        return peer_copy(x_hist.at[target], x_all, x_send, x_recv, target)

    def dy_copy(target):
        return peer_copy(dy_hist.at[target], dy_all, dy_send, dy_recv, target)

    def n_copy(target):
        return peer_copy(n_mine, n_all, n_send, n_recv, target)

    def misc_copy(target):
        return peer_copy(misc_mine, misc_all, misc_send, misc_recv, target)

    def dx_copy(target):
        return peer_copy(dx_mine, dx_all, dx_send, dx_recv, target)

    def to_peers(start):
        def one(k, carry):
            start(lax.rem(me + k, n_stage))
            return carry
        lax.fori_loop(1, n_stage, one, 0)

    def wait_from(buf, recv):
        def one(k, carry):
            source = lax.rem(me + k, n_stage)
            pltpu.make_async_remote_copy(
                src_ref=buf.at[source], dst_ref=buf.at[source], send_sem=dx_send.at[source], recv_sem=recv.at[source],
                device_id=(dp, source), device_id_type=MESH).wait_recv()
            return carry
        lax.fori_loop(1, n_stage, one, 0)

    x_wide = x_last.astype(F32)
    inv_rms = lax.rsqrt(jnp.mean(x_wide * x_wide, axis=-1, keepdims=True) + RMS_EPS)
    normed = (x_wide * inv_rms).astype(BF16)
    n_mine[...] = normed
    n_all[me] = normed
    to_peers(lambda target: x_copy(target).start())
    x_all[me] = x_hist[me]
    to_peers(lambda target: n_copy(target).start())

    cols, n_full, tail = chunks(vocab, HEAD_COLS)

    def table_rows(first, width):
        tile = first // TILE if isinstance(first, int) else lax.div(first, TILE)
        return table[pl.ds(tile, width // TILE)].reshape(width, dim)

    def pass_one(first, width, carry):
        top, total = carry
        z = (dot_nt(normed, table_rows(first, width)) * logit_scale).astype(BF16)
        logits[:, pl.ds(first, width)] = z
        parts = [z[:, j:j + LANES].astype(F32) for j in range(0, width, LANES)]
        new_top = top
        for part in parts:
            new_top = jnp.maximum(new_top, part)
        total = total * jnp.exp(top - new_top)
        for part in parts:
            total = total + jnp.exp(part - new_top)
        return new_top, total

    def head_loop(body, carry):
        carry = lax.fori_loop(0, n_full, lambda i, c: body(pl.multiple_of(i * cols, cols), cols, c), carry)
        if tail:
            carry = body(n_full * cols, tail, carry)
        return carry

    top, total = head_loop(pass_one, (jnp.full((seq, LANES), -1e30, F32), jnp.zeros((seq, LANES), F32)))
    row_top = jnp.max(top, axis=-1, keepdims=True)
    row_sum = jnp.sum(total * jnp.exp(top - row_top), axis=-1, keepdims=True)
    lse = row_top + jnp.log(row_sum)

    lane_iota = lax.broadcasted_iota(jnp.int32, (seq, LANES), 1)
    lane_wide = lane_iota.astype(F32)
    square = lax.broadcasted_iota(jnp.int32, (seq, seq), 0) == lax.broadcasted_iota(jnp.int32, (seq, seq), 1)
    label = jnp.sum(jnp.where(square, lab_ref[pl.ds(me, 1), :].astype(F32), 0.0), axis=-1, keepdims=True)
    lse_count = lse + math.log(1.0 / inv_count)

    def pass_two(first, width, carry):
        picked, grad_n = carry
        base = label - jnp.asarray(first, jnp.int32).astype(F32)
        grads = []
        for j in range(0, width, LANES):
            z = logits[:, pl.ds(first + j, LANES)].astype(F32)
            prob = jnp.exp(z - lse_count)
            hit = lane_wide == base - float(j)
            picked = picked + jnp.where(hit, z, 0.0)
            grads.append(jnp.where(hit, prob - inv_count, prob).astype(BF16))
        grad_z = jnp.concatenate(grads, axis=1)
        return picked, grad_n + dot_nn(grad_z, table_rows(first, width))

    picked, grad_n = head_loop(pass_two, (jnp.zeros((seq, LANES), F32), jnp.zeros((seq, dim), F32)))
    picked = jnp.sum(picked, axis=-1, keepdims=True)
    loss = jnp.sum((lse - picked) * inv_count)
    label_prob = jnp.exp(picked - lse_count)
    fix = (label_prob - inv_count).astype(BF16).astype(F32) - label_prob.astype(BF16).astype(F32)
    eye = lax.broadcasted_iota(jnp.int32, (seq, LANES), 0) == lane_iota

    def as_row(column):
        return jnp.broadcast_to(jnp.sum(jnp.where(eye, column, 0.0), axis=0, keepdims=True), (8, LANES))

    row8 = lax.broadcasted_iota(jnp.int32, (8, LANES), 0)
    misc = jnp.where(row8 == 0, as_row(lse_count), jnp.where(row8 == 1, as_row(fix), loss))
    misc_mine[...] = misc
    misc_all[me] = misc

    grad_n = (grad_n * logit_scale).astype(BF16).astype(F32)
    along = jnp.mean(grad_n * x_wide, axis=-1, keepdims=True)
    grad_x = (inv_rms * grad_n - x_wide * (inv_rms * inv_rms * inv_rms * along)).astype(BF16)

    to_peers(lambda target: misc_copy(target).start())

    def backward(k, grad_out):
        s = n_stage - 1 - k
        dy_hist[s] = grad_out
        grad_hidden = dot_nt(grad_out, down_all[s]).astype(BF16).astype(F32)
        grad_pre = (grad_hidden * gelu_grad(pre_hist[s].astype(F32))).astype(BF16)
        result = (grad_out.astype(F32) + dot_nt(grad_pre, up_all[s])).astype(BF16)

        @pl.when(s != me)
        def _():
            dy_copy(s).start()

        return result

    grad_in = lax.fori_loop(0, n_stage, backward, grad_x)
    dx_mine[...] = grad_in
    dy_all[me] = dy_hist[me]
    dx_all[me] = grad_in

    wait_from(n_all, n_recv)
    wait_from(misc_all, misc_recv)
    per_row = LANES // seq
    for m in range(0, n_stage, per_row):
        row = misc_all[m]
        for k in range(1, per_row):
            row = row + pltpu.roll(misc_all[m + k], k * seq, 1)
        lse_row[:, pl.ds(m * seq, LANES)] = row
    to_peers(lambda target: dx_copy(target).start())
    results = [pltpu.make_async_copy(src, dst, out_sem.at[i]) for i, (src, dst) in enumerate(
        ((n_all, n_out), (misc_all, misc_out), (x_all, x_out), (dy_all, dy_out), (dx_all, dx_out)))]
    results[0].start()
    results[1].start()

    half_rows = vocab // 2
    rows, n_full, tail = chunks(half_rows, TABLE_ROWS)
    count = n_stage * seq

    def keep_copy(first, height, index):
        return pltpu.make_async_copy(
            head_part.at[pl.ds(first, height), :], head_hbm.at[pl.ds(core * half_rows + first, height), :], keep_sem.at[index])

    def part_copy(first, height, index, owner):
        return pltpu.make_async_remote_copy(
            src_ref=head_part.at[pl.ds(first, height), :],
            dst_ref=head_hbm.at[pl.ds(owner * half_rows + first, height), :],
            send_sem=part_send.at[index], recv_sem=part_recv.at[index],
            device_id=(dp, partner), device_id_type=MESH)

    def pass_on(first, height, index):
        keep_copy(first, height, index).start()
        part_copy(first, height, index, core).start()

    def head_rows(first, height):
        every = n_all[...].reshape(count, dim)
        tile = lax.div(core * half_rows + first, TILE)
        z = (dot_nt(table[pl.ds(tile, height // TILE)].reshape(height, dim), every) * logit_scale).astype(BF16).astype(F32)
        grad_z = jnp.exp(z - lse_row[0:1, :]).astype(BF16)
        head_part[pl.ds(first, height), :] = dot_nn(grad_z, every) * logit_scale

    def head_chunk(i, carry):
        @pl.when(i > 0)
        def _():
            pass_on(pl.multiple_of((i - 1) * rows, TILE), rows, i - 1)

        head_rows(pl.multiple_of(i * rows, rows), rows)
        return carry

    lax.fori_loop(0, n_full, head_chunk, 0)
    pass_on((n_full - 1) * rows, rows, n_full - 1)
    wait_from(x_all, x_recv)
    wait_from(dy_all, dy_recv)
    wait_from(dx_all, dx_recv)
    for result in results[2:]:
        result.start()
    if tail:
        head_rows(n_full * rows, tail)
    to_peers(lambda target: x_copy(target).wait_send())
    for copy in sends:
        copy.wait_send()
    if tail:
        pass_on(n_full * rows, tail, n_full)
    for make in (dy_copy, n_copy, misc_copy, dx_copy):
        to_peers(lambda target, make=make: make(target).wait_send())
    for result in results:
        result.wait()

    def finish(first, height, index):
        keep_copy(first, height, index).wait()
        part_copy(first, height, index, core).wait_send()
        part_copy(first, height, index, 1 - core).wait_recv()

    def finish_chunk(i, carry):
        finish(pl.multiple_of(i * rows, rows), rows, i)
        return carry

    lax.fori_loop(0, n_full, finish_chunk, 0)
    if tail:
        finish(n_full * rows, tail, n_full)


def table_kernel(tok_hbm, lab_hbm, misc_hbm, n_hbm, dx_hbm, x_hbm, dy_hbm, up_hbm, down_hbm, head_hbm,
                 out_hbm, loss_out, gup_hbm, gdown_hbm,
                 tok_ref, lab_ref, misc_ref, n_ref, dx_ref, x_ref, dy_ref, up_ref, down_ref, gup_out, gdown_out,
                 head, acc, acc_lab, dx_wide, fix_rows, in_sem, grad_sem, head_sem, out_sem):
    vocab, dim = acc.shape
    n_micro, seq, _ = n_ref.shape
    logit_scale = dim ** -0.5
    rows, n_full, tail = chunks(vocab, OUT_ROWS)

    def head_copy(first, height, index):
        return pltpu.make_async_copy(head_hbm.at[pl.ds(first, height), :], head.at[pl.ds(first, height), :], head_sem.at[index])

    def out_copy(first, height, index):
        return pltpu.make_async_copy(acc.at[pl.ds(first, height), :], out_hbm.at[pl.ds(first, height), :], out_sem.at[index])

    def each(body):
        def one(i, carry):
            body(pl.multiple_of(i * rows, rows), rows, i)
            return carry
        lax.fori_loop(0, n_full, one, 0)
        if tail:
            body(n_full * rows, tail, n_full)

    loads = [pltpu.make_async_copy(src, dst, in_sem.at[i]) for i, (src, dst) in enumerate((
        (tok_hbm, tok_ref), (lab_hbm, lab_ref), (misc_hbm, misc_ref), (n_hbm, n_ref), (dx_hbm, dx_ref),
        (x_hbm, x_ref), (dy_hbm, dy_ref), (up_hbm.at[0], up_ref), (down_hbm.at[0], down_ref)))]
    for load in loads[:5]:
        load.start()
    each(lambda *where: head_copy(*where).start())
    for load in loads[5:]:
        load.start()

    def clear(first, height, index):
        acc[pl.ds(first, height), :] = jnp.zeros((height, dim), F32)
        acc_lab[pl.ds(first, height), :] = jnp.zeros((height, dim), F32)

    each(clear)
    for load in loads[:5]:
        load.wait()

    eye = lax.broadcasted_iota(jnp.int32, (seq, LANES), 0) == lax.broadcasted_iota(jnp.int32, (seq, LANES), 1)
    total = jnp.zeros((8, LANES), F32)
    for m in range(n_micro):
        misc = misc_ref[m]
        total = total + misc
        fix = jnp.sum(jnp.where(eye, misc[1:2, :], 0.0), axis=-1, keepdims=True) * logit_scale
        fix_rows[pl.ds(m * seq, seq), :] = n_ref[m].astype(F32) * fix
        dx_wide[pl.ds(m * seq, seq), :] = dx_ref[m].astype(F32)
    loss_out[0] = jnp.max(total[2:3, :])

    def scatter(m, carry):
        for i in range(seq):
            acc[pl.ds(tok_ref[m, i], 1), :] += dx_wide[pl.ds(m * seq + i, 1), :]
            acc_lab[pl.ds(lab_ref[m, i], 1), :] += fix_rows[pl.ds(m * seq + i, 1), :]
        return carry

    lax.fori_loop(0, n_micro, scatter, 0)

    def join(first, height, index):
        head_copy(first, height, index).wait()
        where = pl.ds(first, height)
        acc[where, :] = head[where, :] + (acc[where, :] + acc_lab[where, :])
        out_copy(first, height, index).start()

    each(join)

    for load in loads[5:]:
        load.wait()
    up, down = up_ref[...], down_ref[...]
    gup_out[...] = jnp.zeros_like(gup_out)
    gdown_out[...] = jnp.zeros_like(gdown_out)
    group = max(1, 256 // seq)

    def wgrad(i, carry):
        x_act = x_ref[pl.ds(i * group, group)].reshape(group * seq, dim)
        grad_out = dy_ref[pl.ds(i * group, group)].reshape(group * seq, dim)
        pre = dot_nn(x_act, up).astype(BF16).astype(F32)
        hidden = gelu(pre).astype(BF16)
        gdown_out[...] += dot_tn(hidden, grad_out)
        grad_hidden = dot_nt(grad_out, down).astype(BF16).astype(F32)
        grad_pre = (grad_hidden * gelu_grad(pre)).astype(BF16)
        gup_out[...] += dot_tn(x_act, grad_pre)
        return carry

    lax.fori_loop(0, n_micro // group, wgrad, 0)
    grads = [pltpu.make_async_copy(gup_out, gup_hbm, grad_sem.at[0]), pltpu.make_async_copy(gdown_out, gdown_hbm, grad_sem.at[1])]
    for grad in grads:
        grad.start()
    for grad in grads:
        grad.wait()
    each(lambda *where: out_copy(*where).wait())


def solution(mesh):
    n_stage = mesh.shape["stage"]

    def device_fn(tokens, labels, emb_table, w_up, w_down):
        n_micro, seq = tokens.shape
        vocab, dim = emb_table.shape
        ffn = w_up.shape[2]
        count = n_micro * seq
        inv_count = 1.0 / count
        vmem = pl.BlockSpec(memory_space=pltpu.VMEM)
        smem = pl.BlockSpec(memory_space=pltpu.SMEM)
        hbm = pl.BlockSpec(memory_space=pl.ANY)
        dma = pltpu.SemaphoreType.DMA

        n_parts = -(-vocab // (2 * TABLE_ROWS))
        act = jax.ShapeDtypeStruct((n_stage, seq, dim), BF16)
        n_all, dx_all, x_all, dy_all, misc, head = pl.pallas_call(
            functools.partial(step_kernel, n_stage, mesh.shape["dp"], inv_count),
            name="step",
            out_shape=(act, act, act, act, jax.ShapeDtypeStruct((n_stage, 8, LANES), F32), jax.ShapeDtypeStruct((vocab, dim), F32)),
            in_specs=[hbm] * 5,
            out_specs=(hbm,) * 6,
            scratch_shapes=[
                pltpu.SMEM((n_micro, seq), jnp.int32),
                pltpu.VMEM((n_micro, seq), jnp.int32),
                pltpu.VMEM((vocab // TILE, TILE, dim), BF16),
                pltpu.VMEM((n_stage, dim, ffn), BF16),
                pltpu.VMEM((n_stage, ffn, dim), BF16),
                pltpu.VMEM((n_stage, seq, dim), BF16),
                pltpu.VMEM((n_stage, seq, ffn), BF16),
                pltpu.VMEM((n_stage, seq, dim), BF16),
                pltpu.VMEM((seq, vocab), BF16),
                pltpu.VMEM((seq, dim), BF16),
                pltpu.VMEM((8, LANES), F32),
                pltpu.VMEM((seq, dim), BF16),
                pltpu.VMEM((seq, dim), F32),
                pltpu.VMEM((8, count), F32),
                pltpu.VMEM((vocab // 2, dim), F32),
                pltpu.VMEM((n_stage, seq, dim), BF16),
                pltpu.VMEM((n_stage, 8, LANES), F32),
                pltpu.VMEM((n_stage, seq, dim), BF16),
                pltpu.VMEM((n_stage, seq, dim), BF16),
                pltpu.VMEM((n_stage, seq, dim), BF16),
                dma((4,)), dma((5,)), dma, dma((n_stage,)), dma((n_stage,)), dma((3, n_stage)), dma((3, n_stage)),
                dma((2, n_stage)), dma((2, 2, n_stage)),
                dma((n_stage,)), dma((n_stage,)), dma((n_stage,)), dma((n_stage,)), dma((n_stage,)),
                dma((n_stage,)), dma((n_stage,)), dma((n_stage,)), dma((n_stage,)), dma((n_stage,)),
                dma((n_parts,)), dma((n_parts,)), dma((n_parts,)),
            ],
            compiler_params=pltpu.CompilerParams(collective_id=0, has_side_effects=True),
        )(tokens, labels, emb_table.reshape(vocab // TILE, TILE, dim), w_up, w_down)

        n_outs = -(-vocab // OUT_ROWS)
        grad_emb, loss, g_up, g_down = pl.pallas_call(
            table_kernel,
            name="table_grad",
            out_shape=(
                jax.ShapeDtypeStruct((vocab, dim), F32),
                jax.ShapeDtypeStruct((1,), F32),
                jax.ShapeDtypeStruct((dim, ffn), F32),
                jax.ShapeDtypeStruct((ffn, dim), F32),
            ),
            in_specs=[hbm] * 10,
            out_specs=(hbm, smem, hbm, hbm),
            scratch_shapes=[
                pltpu.SMEM((n_micro, seq), jnp.int32),
                pltpu.SMEM((n_micro, seq), jnp.int32),
                pltpu.VMEM((n_stage, 8, LANES), F32),
                pltpu.VMEM((n_stage, seq, dim), BF16),
                pltpu.VMEM((n_stage, seq, dim), BF16),
                pltpu.VMEM((n_stage, seq, dim), BF16),
                pltpu.VMEM((n_stage, seq, dim), BF16),
                pltpu.VMEM((dim, ffn), BF16),
                pltpu.VMEM((ffn, dim), BF16),
                pltpu.VMEM((dim, ffn), F32),
                pltpu.VMEM((ffn, dim), F32),
                pltpu.VMEM((vocab, dim), F32),
                pltpu.VMEM((vocab, dim), F32),
                pltpu.VMEM((vocab, dim), F32),
                pltpu.VMEM((count, dim), F32),
                pltpu.VMEM((count, dim), F32),
                dma((9,)), dma((2,)), dma((n_outs,)), dma((n_outs,)),
            ],
        )(tokens, labels, misc, n_all, dx_all, x_all, dy_all, w_up, w_down, head)
        return loss, g_up[None], g_down[None], grad_emb

    return jax.shard_map(device_fn, mesh=mesh, in_specs=(P("dp", None), P("dp", None), P(None, None), P("stage", None, None), P("stage", None, None)), out_specs=(P("dp"), P(("dp", "stage"), None, None), P(("dp", "stage"), None, None), P("dp", None)), check_vma=False)
```

```python
import functools
import math

import jax
import jax.numpy as jnp
from jax import lax
from jax.experimental import pallas as pl
from jax.experimental.pallas import tpu as pltpu
from jax.sharding import PartitionSpec as P

F32 = jnp.float32
BF16 = jnp.bfloat16
MESH = pl.DeviceIdType.MESH
LANES = 128
TILE = 16
HEAD_COLS = 7680
TABLE_ROWS = 2048
OUT_ROWS = 2048
GELU_C = math.sqrt(2.0 / math.pi)
GELU_K = 0.044715
RMS_EPS = 1e-6


def dot_nn(a, b):
    return lax.dot_general(a, b, (((1,), (0,)), ((), ())), preferred_element_type=F32)


def dot_nt(a, b):
    return lax.dot_general(a, b, (((1,), (1,)), ((), ())), preferred_element_type=F32)


def dot_tn(a, b):
    return lax.dot_general(a, b, (((0,), (0,)), ((), ())), preferred_element_type=F32)


def gelu(a):
    return a * (0.5 * (1.0 + jnp.tanh(GELU_C * (a + GELU_K * (a * a * a)))))


def gelu_grad(a):
    sq = a * a
    t = jnp.tanh(GELU_C * (a + GELU_K * (sq * a)))
    return 0.5 * (1.0 + t) + (0.5 * GELU_C) * a * (1.0 - t * t) * (1.0 + (3.0 * GELU_K) * sq)


def chunks(total, size):
    return size, total // size, total % size


def step_kernel(n_stage, n_dp, inv_count, tok_hbm, lab_hbm, table_hbm, w_up_hbm, w_down_hbm,
                n_out, dx_out, x_out, dy_out, misc_out, head_hbm,
                tok_ref, lab_ref, table, up_all, down_all, x_hist, pre_hist, dy_hist, logits,
                n_mine, misc_mine, dx_mine, x_rows, lse_row, head_part, n_all, misc_all, dx_all, x_all, dy_all,
                in_sem, out_sem, table_sem, up_recv, down_recv, up_send, down_send, side_recv, side_send,
                x_recv, dy_recv, n_recv, misc_recv, dx_recv,
                x_send, dy_send, n_send, misc_send, dx_send, keep_sem, part_send, part_recv):
    me = lax.axis_index("stage")
    dp = lax.axis_index("dp")
    n_chip = n_stage // 2
    half = n_chip // 2
    chip, core = me // 2, lax.rem(me, 2)
    dim = table.shape[2]
    vocab = table.shape[0] * TILE
    seq = x_hist.shape[1]
    logit_scale = dim ** -0.5

    def slot_at(offset, which):
        return lax.rem(chip + offset + n_chip, n_chip) * 2 + which

    right, left, partner = slot_at(1, core), slot_at(-1, core), chip * 2 + (1 - core)

    loads = [
        pltpu.make_async_copy(w_up_hbm.at[0], up_all.at[me], in_sem.at[0]),
        pltpu.make_async_copy(w_down_hbm.at[0], down_all.at[me], in_sem.at[1]),
        pltpu.make_async_copy(tok_hbm, tok_ref, in_sem.at[2]),
        pltpu.make_async_copy(lab_hbm, lab_ref, in_sem.at[3]),
    ]
    for load in loads:
        load.start()
    table_copy = pltpu.make_async_copy(table_hbm, table, table_sem)
    table_copy.start()

    barrier = pltpu.get_barrier_semaphore()

    paired = n_dp % 2 == 0
    side = dp + 1 - 2 * lax.rem(dp, 2)
    greeted = [(dp, right), (dp, left), (dp, partner)] + ([(side, me)] if paired else [])
    for peer in greeted:
        pl.semaphore_signal(barrier, inc=1, device_id=peer, device_id_type=MESH)
    pl.semaphore_wait(barrier, len(greeted))
    for load in loads:
        load.wait()

    parity = lax.rem(dp, 2)
    up_rows, down_rows = up_all.shape[1], down_all.shape[1]

    def up_part(kind):
        left_out = up_rows // 64 * 16
        if kind == "whole" or not paired:
            return pl.ds(0, up_rows)
        if kind == "ring":
            return pl.ds(pl.multiple_of(parity * left_out, 16), up_rows - left_out)
        mine = parity if kind == "give" else 1 - parity
        return pl.ds(pl.multiple_of(mine * (up_rows - left_out), 16), left_out)

    def down_part(kind):
        left_out = down_rows * 5 // 256 * 16
        if kind == "whole" or not paired:
            return pl.ds(0, down_rows)
        if kind == "ring":
            return pl.ds(pl.multiple_of(parity * left_out, 16), down_rows - left_out)
        mine = parity if kind == "give" else 1 - parity
        return pl.ds(pl.multiple_of(mine * (down_rows - left_out), 16), left_out)

    def up_copy(slot, way, target, kind):
        ref = up_all.at[slot, up_part(kind)]
        return pltpu.make_async_remote_copy(
            src_ref=ref, dst_ref=ref, send_sem=up_send.at[way, slot], recv_sem=up_recv.at[slot],
            device_id=(dp, target), device_id_type=MESH)

    def down_copy(slot, way, target, kind):
        ref = down_all.at[slot, down_part(kind)]
        return pltpu.make_async_remote_copy(
            src_ref=ref, dst_ref=ref, send_sem=down_send.at[way, slot], recv_sem=down_recv.at[slot],
            device_id=(dp, target), device_id_type=MESH)

    def side_copy(which, slot, kind, across=False):
        ref = up_all.at[slot, up_part(kind)] if which == 0 else down_all.at[slot, down_part(kind)]
        give = kind == "give"
        return pltpu.make_async_remote_copy(
            src_ref=ref, dst_ref=ref, recv_sem=side_recv.at[which, slot],
            send_sem=side_send.at[0 if give and not across else 1, which, slot],
            device_id=(side, partner if across else me) if give else (dp, partner), device_id_type=MESH)

    sends = []

    def send(copy):
        copy.start()
        sends.append(copy)

    for way, target, kind in ((0, right, "ring"), (1, left, "ring"), (2, partner, "whole")):
        for copy in (down_copy, up_copy) if way == 1 else (up_copy, down_copy):
            send(copy(me, way, target, kind))

    table_copy.wait()
    row_iota = lax.broadcasted_iota(jnp.int32, (TILE, dim), 0)

    def embed(i, carry):
        tok = tok_ref[me, i]
        tile = table[lax.div(tok, TILE)].astype(F32)
        row = jnp.sum(jnp.where(row_iota == lax.rem(tok, TILE), tile, 0.0), axis=0, keepdims=True)
        x_rows[pl.ds(i, 1), :] = row
        return carry

    lax.fori_loop(0, seq, embed, 0)
    x_now = x_rows[...].astype(BF16)

    def arrived(copy, which, slot, forward, across=False):
        copy.wait_recv()
        if forward is not None:
            send(forward)
        if paired:
            send(side_copy(which, slot, "give"))
            if across:
                send(side_copy(which, slot, "give", across=True))

    def take(distance, onward=True):
        for which in (0, 1):
            taken = side_copy(which, slot_at(distance, core), "take")
            taken.wait_recv()
            if onward:
                send(taken)

    for t in range(1, half + 1):
        slot_l, slot_r = slot_at(-t, core), slot_at(t, core)
        whole, onward = t < half, t < half - 1
        if paired and t == half:
            for k in range(1, half - 1):
                take(-k)
                take(k)
        up_l, down_r = up_copy(slot_l, 0, right, "ring"), down_copy(slot_r, 1, left, "ring")
        arrived(up_l, 0, slot_l, up_l if whole else None, across=t == half)
        arrived(down_r, 1, slot_r, down_r if whole else None, across=t == half)
        if whole:
            down_l, up_r = down_copy(slot_l, 0, right, "ring"), up_copy(slot_r, 1, left, "ring")
            arrived(down_l, 1, slot_l, down_l if onward else None)
            arrived(up_r, 0, slot_r, up_r if onward else None)
            send(down_copy(slot_l, 2, partner, "ring"))
            send(up_copy(slot_r, 2, partner, "ring"))
        send(up_copy(slot_l, 2, partner, "ring"))
        send(down_copy(slot_r, 2, partner, "ring"))

    if paired:
        take(1 - half)
        take(half - 1)
        take(half, onward=False)

    for t in range(n_chip):
        slot = slot_at(t, 1 - core)
        kind = "whole" if t == 0 else "ring"
        up_copy(slot, 2, partner, kind).wait_recv()
        down_copy(slot, 2, partner, kind).wait_recv()
        if paired and t > 0:
            side_copy(0, slot, "take").wait_recv()
            side_copy(1, slot, "take").wait_recv()

    def forward(s, x_act):
        x_hist[s] = x_act
        pre = dot_nn(x_act, up_all[s]).astype(BF16)
        pre_hist[s] = pre
        hidden = gelu(pre.astype(F32)).astype(BF16)
        return (x_act.astype(F32) + dot_nn(hidden, down_all[s])).astype(BF16)

    x_last = lax.fori_loop(0, n_stage, forward, x_now)

    def peer_copy(src, dst, send_sem, recv_sem, target):
        return pltpu.make_async_remote_copy(
            src_ref=src, dst_ref=dst.at[me], send_sem=send_sem.at[target], recv_sem=recv_sem.at[me],
            device_id=(dp, target), device_id_type=MESH)

    def x_copy(target):
        return peer_copy(x_hist.at[target], x_all, x_send, x_recv, target)

    def dy_copy(target):
        return peer_copy(dy_hist.at[target], dy_all, dy_send, dy_recv, target)

    def n_copy(target):
        return peer_copy(n_mine, n_all, n_send, n_recv, target)

    def misc_copy(target):
        return peer_copy(misc_mine, misc_all, misc_send, misc_recv, target)

    def dx_copy(target):
        return peer_copy(dx_mine, dx_all, dx_send, dx_recv, target)

    def to_peers(start):
        def one(k, carry):
            start(lax.rem(me + k, n_stage))
            return carry
        lax.fori_loop(1, n_stage, one, 0)

    def wait_from(buf, recv):
        def one(k, carry):
            source = lax.rem(me + k, n_stage)
            pltpu.make_async_remote_copy(
                src_ref=buf.at[source], dst_ref=buf.at[source], send_sem=dx_send.at[source], recv_sem=recv.at[source],
                device_id=(dp, source), device_id_type=MESH).wait_recv()
            return carry
        lax.fori_loop(1, n_stage, one, 0)

    x_wide = x_last.astype(F32)
    inv_rms = lax.rsqrt(jnp.mean(x_wide * x_wide, axis=-1, keepdims=True) + RMS_EPS)
    normed = (x_wide * inv_rms).astype(BF16)
    n_mine[...] = normed
    n_all[me] = normed
    to_peers(lambda target: x_copy(target).start())
    x_all[me] = x_hist[me]
    to_peers(lambda target: n_copy(target).start())

    cols, n_full, tail = chunks(vocab, HEAD_COLS)

    def table_rows(first, width):
        tile = first // TILE if isinstance(first, int) else lax.div(first, TILE)
        return table[pl.ds(tile, width // TILE)].reshape(width, dim)

    def pass_one(first, width, carry):
        top, total = carry
        z = (dot_nt(normed, table_rows(first, width)) * logit_scale).astype(BF16)
        logits[:, pl.ds(first, width)] = z
        parts = [z[:, j:j + LANES].astype(F32) for j in range(0, width, LANES)]
        new_top = top
        for part in parts:
            new_top = jnp.maximum(new_top, part)
        total = total * jnp.exp(top - new_top)
        for part in parts:
            total = total + jnp.exp(part - new_top)
        return new_top, total

    def head_loop(body, carry):
        carry = lax.fori_loop(0, n_full, lambda i, c: body(pl.multiple_of(i * cols, cols), cols, c), carry)
        if tail:
            carry = body(n_full * cols, tail, carry)
        return carry

    top, total = head_loop(pass_one, (jnp.full((seq, LANES), -1e30, F32), jnp.zeros((seq, LANES), F32)))
    row_top = jnp.max(top, axis=-1, keepdims=True)
    row_sum = jnp.sum(total * jnp.exp(top - row_top), axis=-1, keepdims=True)
    lse = row_top + jnp.log(row_sum)

    lane_iota = lax.broadcasted_iota(jnp.int32, (seq, LANES), 1)
    lane_wide = lane_iota.astype(F32)
    square = lax.broadcasted_iota(jnp.int32, (seq, seq), 0) == lax.broadcasted_iota(jnp.int32, (seq, seq), 1)
    label = jnp.sum(jnp.where(square, lab_ref[pl.ds(me, 1), :].astype(F32), 0.0), axis=-1, keepdims=True)
    lse_count = lse + math.log(1.0 / inv_count)

    def pass_two(first, width, carry):
        picked, grad_n = carry
        base = label - jnp.asarray(first, jnp.int32).astype(F32)
        grads = []
        for j in range(0, width, LANES):
            z = logits[:, pl.ds(first + j, LANES)].astype(F32)
            prob = jnp.exp(z - lse_count)
            hit = lane_wide == base - float(j)
            picked = picked + jnp.where(hit, z, 0.0)
            grads.append(jnp.where(hit, prob - inv_count, prob).astype(BF16))
        grad_z = jnp.concatenate(grads, axis=1)
        return picked, grad_n + dot_nn(grad_z, table_rows(first, width))

    picked, grad_n = head_loop(pass_two, (jnp.zeros((seq, LANES), F32), jnp.zeros((seq, dim), F32)))
    picked = jnp.sum(picked, axis=-1, keepdims=True)
    loss = jnp.sum((lse - picked) * inv_count)
    label_prob = jnp.exp(picked - lse_count)
    fix = (label_prob - inv_count).astype(BF16).astype(F32) - label_prob.astype(BF16).astype(F32)
    eye = lax.broadcasted_iota(jnp.int32, (seq, LANES), 0) == lane_iota

    def as_row(column):
        return jnp.broadcast_to(jnp.sum(jnp.where(eye, column, 0.0), axis=0, keepdims=True), (8, LANES))

    row8 = lax.broadcasted_iota(jnp.int32, (8, LANES), 0)
    misc = jnp.where(row8 == 0, as_row(lse_count), jnp.where(row8 == 1, as_row(fix), loss))
    misc_mine[...] = misc
    misc_all[me] = misc

    grad_n = (grad_n * logit_scale).astype(BF16).astype(F32)
    along = jnp.mean(grad_n * x_wide, axis=-1, keepdims=True)
    grad_x = (inv_rms * grad_n - x_wide * (inv_rms * inv_rms * inv_rms * along)).astype(BF16)

    to_peers(lambda target: misc_copy(target).start())

    def backward(k, grad_out):
        s = n_stage - 1 - k
        dy_hist[s] = grad_out
        grad_hidden = dot_nt(grad_out, down_all[s]).astype(BF16).astype(F32)
        grad_pre = (grad_hidden * gelu_grad(pre_hist[s].astype(F32))).astype(BF16)
        result = (grad_out.astype(F32) + dot_nt(grad_pre, up_all[s])).astype(BF16)

        @pl.when(s != me)
        def _():
            dy_copy(s).start()

        return result

    grad_in = lax.fori_loop(0, n_stage, backward, grad_x)
    dx_mine[...] = grad_in
    dy_all[me] = dy_hist[me]
    dx_all[me] = grad_in

    wait_from(n_all, n_recv)
    wait_from(misc_all, misc_recv)
    per_row = LANES // seq
    for m in range(0, n_stage, per_row):
        row = misc_all[m]
        for k in range(1, per_row):
            row = row + pltpu.roll(misc_all[m + k], k * seq, 1)
        lse_row[:, pl.ds(m * seq, LANES)] = row
    to_peers(lambda target: dx_copy(target).start())
    results = [pltpu.make_async_copy(src, dst, out_sem.at[i]) for i, (src, dst) in enumerate(
        ((n_all, n_out), (misc_all, misc_out), (x_all, x_out), (dy_all, dy_out), (dx_all, dx_out)))]
    results[0].start()
    results[1].start()

    half_rows = vocab // 2
    rows, n_full, tail = chunks(half_rows, TABLE_ROWS)
    count = n_stage * seq

    def keep_copy(first, height, index):
        return pltpu.make_async_copy(
            head_part.at[pl.ds(first, height), :], head_hbm.at[pl.ds(core * half_rows + first, height), :], keep_sem.at[index])

    def part_copy(first, height, index, owner):
        return pltpu.make_async_remote_copy(
            src_ref=head_part.at[pl.ds(first, height), :],
            dst_ref=head_hbm.at[pl.ds(owner * half_rows + first, height), :],
            send_sem=part_send.at[index], recv_sem=part_recv.at[index],
            device_id=(dp, partner), device_id_type=MESH)

    def pass_on(first, height, index):
        keep_copy(first, height, index).start()
        part_copy(first, height, index, core).start()

    def head_rows(first, height):
        every = n_all[...].reshape(count, dim)
        tile = lax.div(core * half_rows + first, TILE)
        z = (dot_nt(table[pl.ds(tile, height // TILE)].reshape(height, dim), every) * logit_scale).astype(BF16).astype(F32)
        grad_z = jnp.exp(z - lse_row[0:1, :]).astype(BF16)
        head_part[pl.ds(first, height), :] = dot_nn(grad_z, every) * logit_scale

    def head_chunk(i, carry):
        @pl.when(i > 0)
        def _():
            pass_on(pl.multiple_of((i - 1) * rows, TILE), rows, i - 1)

        head_rows(pl.multiple_of(i * rows, rows), rows)
        return carry

    lax.fori_loop(0, n_full, head_chunk, 0)
    pass_on((n_full - 1) * rows, rows, n_full - 1)
    wait_from(x_all, x_recv)
    wait_from(dy_all, dy_recv)
    wait_from(dx_all, dx_recv)
    for result in results[2:]:
        result.start()
    if tail:
        head_rows(n_full * rows, tail)
    to_peers(lambda target: x_copy(target).wait_send())
    for copy in sends:
        copy.wait_send()
    if tail:
        pass_on(n_full * rows, tail, n_full)
    for make in (dy_copy, n_copy, misc_copy, dx_copy):
        to_peers(lambda target, make=make: make(target).wait_send())
    for result in results:
        result.wait()

    def finish(first, height, index):
        keep_copy(first, height, index).wait()
        part_copy(first, height, index, core).wait_send()
        part_copy(first, height, index, 1 - core).wait_recv()

    def finish_chunk(i, carry):
        finish(pl.multiple_of(i * rows, rows), rows, i)
        return carry

    lax.fori_loop(0, n_full, finish_chunk, 0)
    if tail:
        finish(n_full * rows, tail, n_full)


def table_kernel(tok_hbm, lab_hbm, misc_hbm, n_hbm, dx_hbm, x_hbm, dy_hbm, up_hbm, down_hbm, head_hbm,
                 out_hbm, loss_out, gup_hbm, gdown_hbm,
                 tok_ref, lab_ref, misc_ref, n_ref, dx_ref, x_ref, dy_ref, up_ref, down_ref, gup_out, gdown_out,
                 head, acc, acc_lab, dx_wide, fix_rows, in_sem, grad_sem, head_sem, out_sem):
    vocab, dim = acc.shape
    n_micro, seq, _ = n_ref.shape
    logit_scale = dim ** -0.5
    rows, n_full, tail = chunks(vocab, OUT_ROWS)

    def head_copy(first, height, index):
        return pltpu.make_async_copy(head_hbm.at[pl.ds(first, height), :], head.at[pl.ds(first, height), :], head_sem.at[index])

    def out_copy(first, height, index):
        return pltpu.make_async_copy(acc.at[pl.ds(first, height), :], out_hbm.at[pl.ds(first, height), :], out_sem.at[index])

    def each(body):
        def one(i, carry):
            body(pl.multiple_of(i * rows, rows), rows, i)
            return carry
        lax.fori_loop(0, n_full, one, 0)
        if tail:
            body(n_full * rows, tail, n_full)

    loads = [pltpu.make_async_copy(src, dst, in_sem.at[i]) for i, (src, dst) in enumerate((
        (tok_hbm, tok_ref), (lab_hbm, lab_ref), (misc_hbm, misc_ref), (n_hbm, n_ref), (dx_hbm, dx_ref),
        (x_hbm, x_ref), (dy_hbm, dy_ref), (up_hbm.at[0], up_ref), (down_hbm.at[0], down_ref)))]
    for load in loads[:5]:
        load.start()
    each(lambda *where: head_copy(*where).start())
    for load in loads[5:]:
        load.start()

    def clear(first, height, index):
        acc[pl.ds(first, height), :] = jnp.zeros((height, dim), F32)
        acc_lab[pl.ds(first, height), :] = jnp.zeros((height, dim), F32)

    each(clear)
    for load in loads[:5]:
        load.wait()

    eye = lax.broadcasted_iota(jnp.int32, (seq, LANES), 0) == lax.broadcasted_iota(jnp.int32, (seq, LANES), 1)
    total = jnp.zeros((8, LANES), F32)
    for m in range(n_micro):
        misc = misc_ref[m]
        total = total + misc
        fix = jnp.sum(jnp.where(eye, misc[1:2, :], 0.0), axis=-1, keepdims=True) * logit_scale
        fix_rows[pl.ds(m * seq, seq), :] = n_ref[m].astype(F32) * fix
        dx_wide[pl.ds(m * seq, seq), :] = dx_ref[m].astype(F32)
    loss_out[0] = jnp.max(total[2:3, :])

    def scatter(m, carry):
        for i in range(seq):
            acc[pl.ds(tok_ref[m, i], 1), :] += dx_wide[pl.ds(m * seq + i, 1), :]
            acc_lab[pl.ds(lab_ref[m, i], 1), :] += fix_rows[pl.ds(m * seq + i, 1), :]
        return carry

    lax.fori_loop(0, n_micro, scatter, 0)

    def join(first, height, index):
        head_copy(first, height, index).wait()
        where = pl.ds(first, height)
        acc[where, :] = head[where, :] + (acc[where, :] + acc_lab[where, :])
        out_copy(first, height, index).start()

    each(join)

    for load in loads[5:]:
        load.wait()
    up, down = up_ref[...], down_ref[...]
    gup_out[...] = jnp.zeros_like(gup_out)
    gdown_out[...] = jnp.zeros_like(gdown_out)
    group = max(1, 256 // seq)

    def wgrad(i, carry):
        x_act = x_ref[pl.ds(i * group, group)].reshape(group * seq, dim)
        grad_out = dy_ref[pl.ds(i * group, group)].reshape(group * seq, dim)
        pre = dot_nn(x_act, up).astype(BF16).astype(F32)
        hidden = gelu(pre).astype(BF16)
        gdown_out[...] += dot_tn(hidden, grad_out)
        grad_hidden = dot_nt(grad_out, down).astype(BF16).astype(F32)
        grad_pre = (grad_hidden * gelu_grad(pre)).astype(BF16)
        gup_out[...] += dot_tn(x_act, grad_pre)
        return carry

    lax.fori_loop(0, n_micro // group, wgrad, 0)
    grads = [pltpu.make_async_copy(gup_out, gup_hbm, grad_sem.at[0]), pltpu.make_async_copy(gdown_out, gdown_hbm, grad_sem.at[1])]
    for grad in grads:
        grad.start()
    for grad in grads:
        grad.wait()
    each(lambda *where: out_copy(*where).wait())


def solution(mesh):
    n_stage = mesh.shape["stage"]

    def device_fn(tokens, labels, emb_table, w_up, w_down):
        n_micro, seq = tokens.shape
        vocab, dim = emb_table.shape
        ffn = w_up.shape[2]
        count = n_micro * seq
        inv_count = 1.0 / count
        vmem = pl.BlockSpec(memory_space=pltpu.VMEM)
        smem = pl.BlockSpec(memory_space=pltpu.SMEM)
        hbm = pl.BlockSpec(memory_space=pl.ANY)
        dma = pltpu.SemaphoreType.DMA

        n_parts = -(-vocab // (2 * TABLE_ROWS))
        act = jax.ShapeDtypeStruct((n_stage, seq, dim), BF16)
        n_all, dx_all, x_all, dy_all, misc, head = pl.pallas_call(
            functools.partial(step_kernel, n_stage, mesh.shape["dp"], inv_count),
            name="step",
            out_shape=(act, act, act, act, jax.ShapeDtypeStruct((n_stage, 8, LANES), F32), jax.ShapeDtypeStruct((vocab, dim), F32)),
            in_specs=[hbm] * 5,
            out_specs=(hbm,) * 6,
            scratch_shapes=[
                pltpu.SMEM((n_micro, seq), jnp.int32),
                pltpu.VMEM((n_micro, seq), jnp.int32),
                pltpu.VMEM((vocab // TILE, TILE, dim), BF16),
                pltpu.VMEM((n_stage, dim, ffn), BF16),
                pltpu.VMEM((n_stage, ffn, dim), BF16),
                pltpu.VMEM((n_stage, seq, dim), BF16),
                pltpu.VMEM((n_stage, seq, ffn), BF16),
                pltpu.VMEM((n_stage, seq, dim), BF16),
                pltpu.VMEM((seq, vocab), BF16),
                pltpu.VMEM((seq, dim), BF16),
                pltpu.VMEM((8, LANES), F32),
                pltpu.VMEM((seq, dim), BF16),
                pltpu.VMEM((seq, dim), F32),
                pltpu.VMEM((8, count), F32),
                pltpu.VMEM((vocab // 2, dim), F32),
                pltpu.VMEM((n_stage, seq, dim), BF16),
                pltpu.VMEM((n_stage, 8, LANES), F32),
                pltpu.VMEM((n_stage, seq, dim), BF16),
                pltpu.VMEM((n_stage, seq, dim), BF16),
                pltpu.VMEM((n_stage, seq, dim), BF16),
                dma((4,)), dma((5,)), dma, dma((n_stage,)), dma((n_stage,)), dma((3, n_stage)), dma((3, n_stage)),
                dma((2, n_stage)), dma((2, 2, n_stage)),
                dma((n_stage,)), dma((n_stage,)), dma((n_stage,)), dma((n_stage,)), dma((n_stage,)),
                dma((n_stage,)), dma((n_stage,)), dma((n_stage,)), dma((n_stage,)), dma((n_stage,)),
                dma((n_parts,)), dma((n_parts,)), dma((n_parts,)),
            ],
            compiler_params=pltpu.CompilerParams(collective_id=0, has_side_effects=True),
        )(tokens, labels, emb_table.reshape(vocab // TILE, TILE, dim), w_up, w_down)

        n_outs = -(-vocab // OUT_ROWS)
        grad_emb, loss, g_up, g_down = pl.pallas_call(
            table_kernel,
            name="table_grad",
            out_shape=(
                jax.ShapeDtypeStruct((vocab, dim), F32),
                jax.ShapeDtypeStruct((1,), F32),
                jax.ShapeDtypeStruct((dim, ffn), F32),
                jax.ShapeDtypeStruct((ffn, dim), F32),
            ),
            in_specs=[hbm] * 10,
            out_specs=(hbm, smem, hbm, hbm),
            scratch_shapes=[
                pltpu.SMEM((n_micro, seq), jnp.int32),
                pltpu.SMEM((n_micro, seq), jnp.int32),
                pltpu.VMEM((n_stage, 8, LANES), F32),
                pltpu.VMEM((n_stage, seq, dim), BF16),
                pltpu.VMEM((n_stage, seq, dim), BF16),
                pltpu.VMEM((n_stage, seq, dim), BF16),
                pltpu.VMEM((n_stage, seq, dim), BF16),
                pltpu.VMEM((dim, ffn), BF16),
                pltpu.VMEM((ffn, dim), BF16),
                pltpu.VMEM((dim, ffn), F32),
                pltpu.VMEM((ffn, dim), F32),
                pltpu.VMEM((vocab, dim), F32),
                pltpu.VMEM((vocab, dim), F32),
                pltpu.VMEM((vocab, dim), F32),
                pltpu.VMEM((count, dim), F32),
                pltpu.VMEM((count, dim), F32),
                dma((9,)), dma((2,)), dma((n_outs,)), dma((n_outs,)),
            ],
        )(tokens, labels, misc, n_all, dx_all, x_all, dy_all, w_up, w_down, head)
        return loss, g_up[None], g_down[None], grad_emb

    return jax.shard_map(device_fn, mesh=mesh, in_specs=(P("dp", None), P("dp", None), P(None, None), P("stage", None, None), P("stage", None, None)), out_specs=(P("dp"), P(("dp", "stage"), None, None), P(("dp", "stage"), None, None), P("dp", None)), check_vma=False)
```

```python
import functools
import math

import jax
import jax.numpy as jnp
from jax import lax
from jax.experimental import pallas as pl
from jax.experimental.pallas import tpu as pltpu
from jax.sharding import PartitionSpec as P

F32 = jnp.float32
BF16 = jnp.bfloat16
MESH = pl.DeviceIdType.MESH
LANES = 128
TILE = 16
HEAD_COLS = 7680
TABLE_ROWS = 2048
OUT_ROWS = 2048
GELU_C = math.sqrt(2.0 / math.pi)
GELU_K = 0.044715
RMS_EPS = 1e-6


def dot_nn(a, b):
    return lax.dot_general(a, b, (((1,), (0,)), ((), ())), preferred_element_type=F32)


def dot_nt(a, b):
    return lax.dot_general(a, b, (((1,), (1,)), ((), ())), preferred_element_type=F32)


def dot_tn(a, b):
    return lax.dot_general(a, b, (((0,), (0,)), ((), ())), preferred_element_type=F32)


def gelu(a):
    return a * (0.5 * (1.0 + jnp.tanh(GELU_C * (a + GELU_K * (a * a * a)))))


def gelu_grad(a):
    sq = a * a
    t = jnp.tanh(GELU_C * (a + GELU_K * (sq * a)))
    return 0.5 * (1.0 + t) + (0.5 * GELU_C) * a * (1.0 - t * t) * (1.0 + (3.0 * GELU_K) * sq)


def chunks(total, size):
    return size, total // size, total % size


def step_kernel(n_stage, n_dp, inv_count, tok_hbm, lab_hbm, table_hbm, w_up_hbm, w_down_hbm,
                n_out, dx_out, x_out, dy_out, misc_out, head_hbm,
                tok_ref, lab_ref, table, up_all, down_all, x_hist, pre_hist, dy_hist, logits,
                n_mine, misc_mine, dx_mine, x_rows, lse_row, head_part, n_all, misc_all, dx_all, x_all, dy_all,
                in_sem, out_sem, table_sem, up_recv, down_recv, up_send, down_send, side_recv, side_send,
                x_recv, dy_recv, n_recv, misc_recv, dx_recv,
                x_send, dy_send, n_send, misc_send, dx_send, keep_sem, part_send, part_recv):
    me = lax.axis_index("stage")
    dp = lax.axis_index("dp")
    n_chip = n_stage // 2
    half = n_chip // 2
    chip, core = me // 2, lax.rem(me, 2)
    dim = table.shape[2]
    vocab = table.shape[0] * TILE
    seq = x_hist.shape[1]
    logit_scale = dim ** -0.5

    def slot_at(offset, which):
        return lax.rem(chip + offset + n_chip, n_chip) * 2 + which

    right, left, partner = slot_at(1, core), slot_at(-1, core), chip * 2 + (1 - core)

    loads = [
        pltpu.make_async_copy(w_up_hbm.at[0], up_all.at[me], in_sem.at[0]),
        pltpu.make_async_copy(w_down_hbm.at[0], down_all.at[me], in_sem.at[1]),
        pltpu.make_async_copy(tok_hbm, tok_ref, in_sem.at[2]),
        pltpu.make_async_copy(lab_hbm, lab_ref, in_sem.at[3]),
    ]
    for load in loads:
        load.start()
    table_copy = pltpu.make_async_copy(table_hbm, table, table_sem)
    table_copy.start()

    barrier = pltpu.get_barrier_semaphore()

    paired = n_dp % 2 == 0
    side = dp + 1 - 2 * lax.rem(dp, 2)
    greeted = [(dp, right), (dp, left), (dp, partner)] + ([(side, me)] if paired else [])
    for peer in greeted:
        pl.semaphore_signal(barrier, inc=1, device_id=peer, device_id_type=MESH)
    pl.semaphore_wait(barrier, len(greeted))
    for load in loads:
        load.wait()

    parity = lax.rem(dp, 2)
    up_rows, down_rows = up_all.shape[1], down_all.shape[1]

    def part(height, left_out, kind, piece):
        first, size = 0, height
        if paired and kind == "ring":
            first, size = parity * left_out, height - left_out
        elif paired and kind != "whole":
            first, size = (parity if kind == "give" else 1 - parity) * (height - left_out), left_out
        return pl.ds(pl.multiple_of(first + piece * (size // 2), 16), size // 2)

    def up_part(kind, piece):
        return part(up_rows, up_rows // 64 * 16, kind, piece)

    def down_part(kind, piece):
        return part(down_rows, down_rows * 5 // 256 * 16, kind, piece)

    def up_copy(slot, way, target, kind, piece):
        ref = up_all.at[slot, up_part(kind, piece)]
        return pltpu.make_async_remote_copy(
            src_ref=ref, dst_ref=ref, send_sem=up_send.at[way, piece, slot], recv_sem=up_recv.at[piece, slot],
            device_id=(dp, target), device_id_type=MESH)

    def down_copy(slot, way, target, kind, piece):
        ref = down_all.at[slot, down_part(kind, piece)]
        return pltpu.make_async_remote_copy(
            src_ref=ref, dst_ref=ref, send_sem=down_send.at[way, piece, slot], recv_sem=down_recv.at[piece, slot],
            device_id=(dp, target), device_id_type=MESH)

    def side_copy(which, slot, kind, piece, across=False):
        ref = up_all.at[slot, up_part(kind, piece)] if which == 0 else down_all.at[slot, down_part(kind, piece)]
        give = kind == "give"
        return pltpu.make_async_remote_copy(
            src_ref=ref, dst_ref=ref, recv_sem=side_recv.at[which, piece, slot],
            send_sem=side_send.at[0 if give and not across else 1, which, piece, slot],
            device_id=(side, partner if across else me) if give else (dp, partner), device_id_type=MESH)

    sends = []

    def send(copy):
        copy.start()
        sends.append(copy)

    for way, target, kind in ((0, right, "ring"), (1, left, "ring"), (2, partner, "whole")):
        for copy in (down_copy, up_copy) if way == 1 else (up_copy, down_copy):
            for piece in (0, 1):
                send(copy(me, way, target, kind, piece))

    table_copy.wait()
    row_iota = lax.broadcasted_iota(jnp.int32, (TILE, dim), 0)

    def embed(i, carry):
        tok = tok_ref[me, i]
        tile = table[lax.div(tok, TILE)].astype(F32)
        row = jnp.sum(jnp.where(row_iota == lax.rem(tok, TILE), tile, 0.0), axis=0, keepdims=True)
        x_rows[pl.ds(i, 1), :] = row
        return carry

    lax.fori_loop(0, seq, embed, 0)
    x_now = x_rows[...].astype(BF16)

    def arrived(which, slot, way, onward, piece, across=False):
        target = (right, left)[way]
        copy = (up_copy, down_copy)[which](slot, way, target, "ring", piece)
        copy.wait_recv()
        if onward:
            send(copy)
        for given in (0, 1) if paired and piece == 1 else ():
            send(side_copy(which, slot, "give", given))
            if across:
                send(side_copy(which, slot, "give", given, across=True))
        send((up_copy, down_copy)[which](slot, 2, partner, "ring", piece))

    def take(distance, onward=True):
        for which in (0, 1):
            for piece in (0, 1):
                taken = side_copy(which, slot_at(distance, core), "take", piece)
                taken.wait_recv()
                if onward:
                    send(taken)

    for t in range(1, half + 1):
        slot_l, slot_r = slot_at(-t, core), slot_at(t, core)
        if paired and t == half:
            for k in range(1, half - 1):
                take(-k)
                take(k)
        for piece in (0, 1):
            arrived(0, slot_l, 0, t < half, piece, across=t == half)
            arrived(1, slot_r, 1, t < half, piece, across=t == half)
        if t < half:
            for piece in (0, 1):
                arrived(1, slot_l, 0, t < half - 1, piece)
                arrived(0, slot_r, 1, t < half - 1, piece)

    if paired:
        take(1 - half)
        take(half - 1)
        take(half, onward=False)

    for t in range(n_chip):
        slot = slot_at(t, 1 - core)
        kind = "whole" if t == 0 else "ring"
        for piece in (0, 1):
            up_copy(slot, 2, partner, kind, piece).wait_recv()
            down_copy(slot, 2, partner, kind, piece).wait_recv()
            if paired and t > 0:
                side_copy(0, slot, "take", piece).wait_recv()
                side_copy(1, slot, "take", piece).wait_recv()

    def forward(s, x_act):
        x_hist[s] = x_act
        pre = dot_nn(x_act, up_all[s]).astype(BF16)
        pre_hist[s] = pre
        hidden = gelu(pre.astype(F32)).astype(BF16)
        return (x_act.astype(F32) + dot_nn(hidden, down_all[s])).astype(BF16)

    x_last = lax.fori_loop(0, n_stage, forward, x_now)

    def peer_copy(src, dst, send_sem, recv_sem, target):
        return pltpu.make_async_remote_copy(
            src_ref=src, dst_ref=dst.at[me], send_sem=send_sem.at[target], recv_sem=recv_sem.at[me],
            device_id=(dp, target), device_id_type=MESH)

    def x_copy(target):
        return peer_copy(x_hist.at[target], x_all, x_send, x_recv, target)

    def dy_copy(target):
        return peer_copy(dy_hist.at[target], dy_all, dy_send, dy_recv, target)

    def n_copy(target):
        return peer_copy(n_mine, n_all, n_send, n_recv, target)

    def misc_copy(target):
        return peer_copy(misc_mine, misc_all, misc_send, misc_recv, target)

    def dx_copy(target):
        return peer_copy(dx_mine, dx_all, dx_send, dx_recv, target)

    def to_peers(start):
        def one(k, carry):
            start(lax.rem(me + k, n_stage))
            return carry
        lax.fori_loop(1, n_stage, one, 0)

    def wait_from(buf, recv):
        def one(k, carry):
            source = lax.rem(me + k, n_stage)
            pltpu.make_async_remote_copy(
                src_ref=buf.at[source], dst_ref=buf.at[source], send_sem=dx_send.at[source], recv_sem=recv.at[source],
                device_id=(dp, source), device_id_type=MESH).wait_recv()
            return carry
        lax.fori_loop(1, n_stage, one, 0)

    x_wide = x_last.astype(F32)
    inv_rms = lax.rsqrt(jnp.mean(x_wide * x_wide, axis=-1, keepdims=True) + RMS_EPS)
    normed = (x_wide * inv_rms).astype(BF16)
    n_mine[...] = normed
    n_all[me] = normed
    to_peers(lambda target: x_copy(target).start())
    x_all[me] = x_hist[me]
    to_peers(lambda target: n_copy(target).start())

    cols, n_full, tail = chunks(vocab, HEAD_COLS)

    def table_rows(first, width):
        tile = first // TILE if isinstance(first, int) else lax.div(first, TILE)
        return table[pl.ds(tile, width // TILE)].reshape(width, dim)

    def pass_one(first, width, carry):
        top, total = carry
        z = (dot_nt(normed, table_rows(first, width)) * logit_scale).astype(BF16)
        logits[:, pl.ds(first, width)] = z
        parts = [z[:, j:j + LANES].astype(F32) for j in range(0, width, LANES)]
        new_top = top
        for part in parts:
            new_top = jnp.maximum(new_top, part)
        total = total * jnp.exp(top - new_top)
        for part in parts:
            total = total + jnp.exp(part - new_top)
        return new_top, total

    def head_loop(body, carry):
        carry = lax.fori_loop(0, n_full, lambda i, c: body(pl.multiple_of(i * cols, cols), cols, c), carry)
        if tail:
            carry = body(n_full * cols, tail, carry)
        return carry

    top, total = head_loop(pass_one, (jnp.full((seq, LANES), -1e30, F32), jnp.zeros((seq, LANES), F32)))
    row_top = jnp.max(top, axis=-1, keepdims=True)
    row_sum = jnp.sum(total * jnp.exp(top - row_top), axis=-1, keepdims=True)
    lse = row_top + jnp.log(row_sum)

    lane_iota = lax.broadcasted_iota(jnp.int32, (seq, LANES), 1)
    lane_wide = lane_iota.astype(F32)
    square = lax.broadcasted_iota(jnp.int32, (seq, seq), 0) == lax.broadcasted_iota(jnp.int32, (seq, seq), 1)
    label = jnp.sum(jnp.where(square, lab_ref[pl.ds(me, 1), :].astype(F32), 0.0), axis=-1, keepdims=True)
    lse_count = lse + math.log(1.0 / inv_count)

    def pass_two(first, width, carry):
        picked, grad_n = carry
        base = label - jnp.asarray(first, jnp.int32).astype(F32)
        grads = []
        for j in range(0, width, LANES):
            z = logits[:, pl.ds(first + j, LANES)].astype(F32)
            prob = jnp.exp(z - lse_count)
            hit = lane_wide == base - float(j)
            picked = picked + jnp.where(hit, z, 0.0)
            grads.append(jnp.where(hit, prob - inv_count, prob).astype(BF16))
        grad_z = jnp.concatenate(grads, axis=1)
        return picked, grad_n + dot_nn(grad_z, table_rows(first, width))

    picked, grad_n = head_loop(pass_two, (jnp.zeros((seq, LANES), F32), jnp.zeros((seq, dim), F32)))
    picked = jnp.sum(picked, axis=-1, keepdims=True)
    loss = jnp.sum((lse - picked) * inv_count)
    label_prob = jnp.exp(picked - lse_count)
    fix = (label_prob - inv_count).astype(BF16).astype(F32) - label_prob.astype(BF16).astype(F32)
    eye = lax.broadcasted_iota(jnp.int32, (seq, LANES), 0) == lane_iota

    def as_row(column):
        return jnp.broadcast_to(jnp.sum(jnp.where(eye, column, 0.0), axis=0, keepdims=True), (8, LANES))

    row8 = lax.broadcasted_iota(jnp.int32, (8, LANES), 0)
    misc = jnp.where(row8 == 0, as_row(lse_count), jnp.where(row8 == 1, as_row(fix), loss))
    misc_mine[...] = misc
    misc_all[me] = misc

    grad_n = (grad_n * logit_scale).astype(BF16).astype(F32)
    along = jnp.mean(grad_n * x_wide, axis=-1, keepdims=True)
    grad_x = (inv_rms * grad_n - x_wide * (inv_rms * inv_rms * inv_rms * along)).astype(BF16)

    to_peers(lambda target: misc_copy(target).start())

    def backward(k, grad_out):
        s = n_stage - 1 - k
        dy_hist[s] = grad_out
        grad_hidden = dot_nt(grad_out, down_all[s]).astype(BF16).astype(F32)
        grad_pre = (grad_hidden * gelu_grad(pre_hist[s].astype(F32))).astype(BF16)
        result = (grad_out.astype(F32) + dot_nt(grad_pre, up_all[s])).astype(BF16)

        @pl.when(s != me)
        def _():
            dy_copy(s).start()

        return result

    grad_in = lax.fori_loop(0, n_stage, backward, grad_x)
    dx_mine[...] = grad_in
    dy_all[me] = dy_hist[me]
    dx_all[me] = grad_in

    wait_from(n_all, n_recv)
    wait_from(misc_all, misc_recv)
    per_row = LANES // seq
    for m in range(0, n_stage, per_row):
        row = misc_all[m]
        for k in range(1, per_row):
            row = row + pltpu.roll(misc_all[m + k], k * seq, 1)
        lse_row[:, pl.ds(m * seq, LANES)] = row
    to_peers(lambda target: dx_copy(target).start())
    results = [pltpu.make_async_copy(src, dst, out_sem.at[i]) for i, (src, dst) in enumerate(
        ((n_all, n_out), (misc_all, misc_out), (x_all, x_out), (dy_all, dy_out), (dx_all, dx_out)))]
    results[0].start()
    results[1].start()

    half_rows = vocab // 2
    rows, n_full, tail = chunks(half_rows, TABLE_ROWS)
    count = n_stage * seq

    def keep_copy(first, height, index):
        return pltpu.make_async_copy(
            head_part.at[pl.ds(first, height), :], head_hbm.at[pl.ds(core * half_rows + first, height), :], keep_sem.at[index])

    def part_copy(first, height, index, owner):
        return pltpu.make_async_remote_copy(
            src_ref=head_part.at[pl.ds(first, height), :],
            dst_ref=head_hbm.at[pl.ds(owner * half_rows + first, height), :],
            send_sem=part_send.at[index], recv_sem=part_recv.at[index],
            device_id=(dp, partner), device_id_type=MESH)

    def pass_on(first, height, index):
        keep_copy(first, height, index).start()
        part_copy(first, height, index, core).start()

    def head_rows(first, height):
        every = n_all[...].reshape(count, dim)
        tile = lax.div(core * half_rows + first, TILE)
        z = (dot_nt(table[pl.ds(tile, height // TILE)].reshape(height, dim), every) * logit_scale).astype(BF16).astype(F32)
        grad_z = jnp.exp(z - lse_row[0:1, :]).astype(BF16)
        head_part[pl.ds(first, height), :] = dot_nn(grad_z, every) * logit_scale

    def head_chunk(i, carry):
        @pl.when(i > 0)
        def _():
            pass_on(pl.multiple_of((i - 1) * rows, TILE), rows, i - 1)

        head_rows(pl.multiple_of(i * rows, rows), rows)
        return carry

    lax.fori_loop(0, n_full, head_chunk, 0)
    pass_on((n_full - 1) * rows, rows, n_full - 1)
    wait_from(x_all, x_recv)
    wait_from(dy_all, dy_recv)
    wait_from(dx_all, dx_recv)
    for result in results[2:]:
        result.start()
    if tail:
        head_rows(n_full * rows, tail)
    to_peers(lambda target: x_copy(target).wait_send())
    for copy in sends:
        copy.wait_send()
    if tail:
        pass_on(n_full * rows, tail, n_full)
    for make in (dy_copy, n_copy, misc_copy, dx_copy):
        to_peers(lambda target, make=make: make(target).wait_send())
    for result in results:
        result.wait()

    def finish(first, height, index):
        keep_copy(first, height, index).wait()
        part_copy(first, height, index, core).wait_send()
        part_copy(first, height, index, 1 - core).wait_recv()

    def finish_chunk(i, carry):
        finish(pl.multiple_of(i * rows, rows), rows, i)
        return carry

    lax.fori_loop(0, n_full, finish_chunk, 0)
    if tail:
        finish(n_full * rows, tail, n_full)


def table_kernel(tok_hbm, lab_hbm, misc_hbm, n_hbm, dx_hbm, x_hbm, dy_hbm, up_hbm, down_hbm, head_hbm,
                 out_hbm, loss_out, gup_hbm, gdown_hbm,
                 tok_ref, lab_ref, misc_ref, n_ref, dx_ref, x_ref, dy_ref, up_ref, down_ref, gup_out, gdown_out,
                 head, acc, acc_lab, dx_wide, fix_rows, in_sem, grad_sem, head_sem, out_sem):
    vocab, dim = acc.shape
    n_micro, seq, _ = n_ref.shape
    logit_scale = dim ** -0.5
    rows, n_full, tail = chunks(vocab, OUT_ROWS)

    def head_copy(first, height, index):
        return pltpu.make_async_copy(head_hbm.at[pl.ds(first, height), :], head.at[pl.ds(first, height), :], head_sem.at[index])

    def out_copy(first, height, index):
        return pltpu.make_async_copy(acc.at[pl.ds(first, height), :], out_hbm.at[pl.ds(first, height), :], out_sem.at[index])

    def each(body):
        def one(i, carry):
            body(pl.multiple_of(i * rows, rows), rows, i)
            return carry
        lax.fori_loop(0, n_full, one, 0)
        if tail:
            body(n_full * rows, tail, n_full)

    loads = [pltpu.make_async_copy(src, dst, in_sem.at[i]) for i, (src, dst) in enumerate((
        (tok_hbm, tok_ref), (lab_hbm, lab_ref), (misc_hbm, misc_ref), (n_hbm, n_ref), (dx_hbm, dx_ref),
        (x_hbm, x_ref), (dy_hbm, dy_ref), (up_hbm.at[0], up_ref), (down_hbm.at[0], down_ref)))]
    for load in loads[:5]:
        load.start()
    each(lambda *where: head_copy(*where).start())
    for load in loads[5:]:
        load.start()

    def clear(first, height, index):
        acc[pl.ds(first, height), :] = jnp.zeros((height, dim), F32)
        acc_lab[pl.ds(first, height), :] = jnp.zeros((height, dim), F32)

    each(clear)
    for load in loads[:5]:
        load.wait()

    eye = lax.broadcasted_iota(jnp.int32, (seq, LANES), 0) == lax.broadcasted_iota(jnp.int32, (seq, LANES), 1)
    total = jnp.zeros((8, LANES), F32)
    for m in range(n_micro):
        misc = misc_ref[m]
        total = total + misc
        fix = jnp.sum(jnp.where(eye, misc[1:2, :], 0.0), axis=-1, keepdims=True) * logit_scale
        fix_rows[pl.ds(m * seq, seq), :] = n_ref[m].astype(F32) * fix
        dx_wide[pl.ds(m * seq, seq), :] = dx_ref[m].astype(F32)
    loss_out[0] = jnp.max(total[2:3, :])

    def scatter(m, carry):
        for i in range(seq):
            acc[pl.ds(tok_ref[m, i], 1), :] += dx_wide[pl.ds(m * seq + i, 1), :]
            acc_lab[pl.ds(lab_ref[m, i], 1), :] += fix_rows[pl.ds(m * seq + i, 1), :]
        return carry

    lax.fori_loop(0, n_micro, scatter, 0)

    def join(first, height, index):
        head_copy(first, height, index).wait()
        where = pl.ds(first, height)
        acc[where, :] = head[where, :] + (acc[where, :] + acc_lab[where, :])
        out_copy(first, height, index).start()

    each(join)

    for load in loads[5:]:
        load.wait()
    up, down = up_ref[...], down_ref[...]
    gup_out[...] = jnp.zeros_like(gup_out)
    gdown_out[...] = jnp.zeros_like(gdown_out)
    group = max(1, 256 // seq)

    def wgrad(i, carry):
        x_act = x_ref[pl.ds(i * group, group)].reshape(group * seq, dim)
        grad_out = dy_ref[pl.ds(i * group, group)].reshape(group * seq, dim)
        pre = dot_nn(x_act, up).astype(BF16).astype(F32)
        hidden = gelu(pre).astype(BF16)
        gdown_out[...] += dot_tn(hidden, grad_out)
        grad_hidden = dot_nt(grad_out, down).astype(BF16).astype(F32)
        grad_pre = (grad_hidden * gelu_grad(pre)).astype(BF16)
        gup_out[...] += dot_tn(x_act, grad_pre)
        return carry

    lax.fori_loop(0, n_micro // group, wgrad, 0)
    grads = [pltpu.make_async_copy(gup_out, gup_hbm, grad_sem.at[0]), pltpu.make_async_copy(gdown_out, gdown_hbm, grad_sem.at[1])]
    for grad in grads:
        grad.start()
    for grad in grads:
        grad.wait()
    each(lambda *where: out_copy(*where).wait())


def solution(mesh):
    n_stage = mesh.shape["stage"]

    def device_fn(tokens, labels, emb_table, w_up, w_down):
        n_micro, seq = tokens.shape
        vocab, dim = emb_table.shape
        ffn = w_up.shape[2]
        count = n_micro * seq
        inv_count = 1.0 / count
        vmem = pl.BlockSpec(memory_space=pltpu.VMEM)
        smem = pl.BlockSpec(memory_space=pltpu.SMEM)
        hbm = pl.BlockSpec(memory_space=pl.ANY)
        dma = pltpu.SemaphoreType.DMA

        n_parts = -(-vocab // (2 * TABLE_ROWS))
        act = jax.ShapeDtypeStruct((n_stage, seq, dim), BF16)
        n_all, dx_all, x_all, dy_all, misc, head = pl.pallas_call(
            functools.partial(step_kernel, n_stage, mesh.shape["dp"], inv_count),
            name="step",
            out_shape=(act, act, act, act, jax.ShapeDtypeStruct((n_stage, 8, LANES), F32), jax.ShapeDtypeStruct((vocab, dim), F32)),
            in_specs=[hbm] * 5,
            out_specs=(hbm,) * 6,
            scratch_shapes=[
                pltpu.SMEM((n_micro, seq), jnp.int32),
                pltpu.VMEM((n_micro, seq), jnp.int32),
                pltpu.VMEM((vocab // TILE, TILE, dim), BF16),
                pltpu.VMEM((n_stage, dim, ffn), BF16),
                pltpu.VMEM((n_stage, ffn, dim), BF16),
                pltpu.VMEM((n_stage, seq, dim), BF16),
                pltpu.VMEM((n_stage, seq, ffn), BF16),
                pltpu.VMEM((n_stage, seq, dim), BF16),
                pltpu.VMEM((seq, vocab), BF16),
                pltpu.VMEM((seq, dim), BF16),
                pltpu.VMEM((8, LANES), F32),
                pltpu.VMEM((seq, dim), BF16),
                pltpu.VMEM((seq, dim), F32),
                pltpu.VMEM((8, count), F32),
                pltpu.VMEM((vocab // 2, dim), F32),
                pltpu.VMEM((n_stage, seq, dim), BF16),
                pltpu.VMEM((n_stage, 8, LANES), F32),
                pltpu.VMEM((n_stage, seq, dim), BF16),
                pltpu.VMEM((n_stage, seq, dim), BF16),
                pltpu.VMEM((n_stage, seq, dim), BF16),
                dma((4,)), dma((5,)), dma, dma((2, n_stage)), dma((2, n_stage)), dma((3, 2, n_stage)), dma((3, 2, n_stage)),
                dma((2, 2, n_stage)), dma((2, 2, 2, n_stage)),
                dma((n_stage,)), dma((n_stage,)), dma((n_stage,)), dma((n_stage,)), dma((n_stage,)),
                dma((n_stage,)), dma((n_stage,)), dma((n_stage,)), dma((n_stage,)), dma((n_stage,)),
                dma((n_parts,)), dma((n_parts,)), dma((n_parts,)),
            ],
            compiler_params=pltpu.CompilerParams(collective_id=0, has_side_effects=True),
        )(tokens, labels, emb_table.reshape(vocab // TILE, TILE, dim), w_up, w_down)

        n_outs = -(-vocab // OUT_ROWS)
        grad_emb, loss, g_up, g_down = pl.pallas_call(
            table_kernel,
            name="table_grad",
            out_shape=(
                jax.ShapeDtypeStruct((vocab, dim), F32),
                jax.ShapeDtypeStruct((1,), F32),
                jax.ShapeDtypeStruct((dim, ffn), F32),
                jax.ShapeDtypeStruct((ffn, dim), F32),
            ),
            in_specs=[hbm] * 10,
            out_specs=(hbm, smem, hbm, hbm),
            scratch_shapes=[
                pltpu.SMEM((n_micro, seq), jnp.int32),
                pltpu.SMEM((n_micro, seq), jnp.int32),
                pltpu.VMEM((n_stage, 8, LANES), F32),
                pltpu.VMEM((n_stage, seq, dim), BF16),
                pltpu.VMEM((n_stage, seq, dim), BF16),
                pltpu.VMEM((n_stage, seq, dim), BF16),
                pltpu.VMEM((n_stage, seq, dim), BF16),
                pltpu.VMEM((dim, ffn), BF16),
                pltpu.VMEM((ffn, dim), BF16),
                pltpu.VMEM((dim, ffn), F32),
                pltpu.VMEM((ffn, dim), F32),
                pltpu.VMEM((vocab, dim), F32),
                pltpu.VMEM((vocab, dim), F32),
                pltpu.VMEM((vocab, dim), F32),
                pltpu.VMEM((count, dim), F32),
                pltpu.VMEM((count, dim), F32),
                dma((9,)), dma((2,)), dma((n_outs,)), dma((n_outs,)),
            ],
        )(tokens, labels, misc, n_all, dx_all, x_all, dy_all, w_up, w_down, head)
        return loss, g_up[None], g_down[None], grad_emb

    return jax.shard_map(device_fn, mesh=mesh, in_specs=(P("dp", None), P("dp", None), P(None, None), P("stage", None, None), P("stage", None, None)), out_specs=(P("dp"), P(("dp", "stage"), None, None), P(("dp", "stage"), None, None), P("dp", None)), check_vma=False)
```
